128 devices in a mesh: lat: 32 (over z, x, core), fld: 4 (over y).
Axes of the slice: x: 4, y: 4, z: 4, core: 2. Of those that a mesh axis runs over, the one named last changes fastest.
Arguments:
- grid_in: bfloat16 [32, 2560, 2688], P('fld', 'lat'), may hold values from -6 to 6
- legendre: bfloat16 [768, 1280, 768], P(('lat', 'fld')), may hold values from -0.15625 to 0.15625
- wave_slot: int32 [768], replicated, may hold values from 512 to 1279, as said below
- lat_modes: int32 [2560], P('lat'), may hold values from 10 to 1280
- gauss_weight: float32 [1280], replicated, may hold values from 0.5 to 2
- diffusion: float32 [32], replicated, may hold values from 0.5 to 8
Outputs:
- grid_out: float32 [32, 2560, 2688], P('fld', 'lat')
- spectra: float32 [2, 768, 32, 768], P(None, 'lat', 'fld')
The draws below stay inside these ranges and needn't reach their ends.
Inputs may be any that keep to these rules, and one draw needn't show every extreme that they name: `wave_slot`: every wavenumber from 512 to 1279 stands in exactly one slot; slots 2 t and 2 t + 1 hold two wavenumbers that sum to 1791, the smaller one in the even slot.
All inputs are finite; a program needn't handle non-finite values.
Results may differ from the reference program's by a relative error of at most 0.0071.
Values may be sent and summed in bfloat16 or wider, within the bound.
A program may use at most 192 MiB of HBM per device.

```python
import math
import jax
import jax.numpy as jnp
from jax import lax

LMAX = 1279
NLAT = 2560
NLON = 2688
MW = 768
FIELDS = 32


def draw_wave_slot(key, part):
    pair_count = MW // 2
    shuffled = jax.random.permutation(key, pair_count).astype(jnp.int32)
    low_waves = LMAX + 1 - MW + shuffled
    high_waves = LMAX - shuffled
    return jnp.stack([low_waves, high_waves], 1).reshape(MW).astype(jnp.int32)


def draw_lat_modes(key, part):
    rows_index = jnp.arange(NLAT, dtype=jnp.int32)
    polar_rows = jnp.minimum(rows_index, NLAT - 1 - rows_index)
    jitter = jax.random.randint(key, (NLAT,), 0, 32, dtype=jnp.int32)
    modes_grown = 10 + 2 * polar_rows * (LMAX + 1) // (NLAT // 2) + jitter
    return jnp.minimum(modes_grown, LMAX + 1).astype(jnp.int32)


def block_levels(stream_key, shape, split, smallest, largest):
    loudness, own = 1.0, jax.random.fold_in(stream_key, 6)
    for dim, blocks in split:
        steps = jnp.exp(jax.random.uniform(jax.random.fold_in(own, dim), (blocks,), jnp.float32, smallest / len(split), largest / len(split)))
        loudness = loudness * jnp.repeat(steps, shape[dim] // blocks).reshape([-1 if axis == dim else 1 for axis in range(len(shape))])
    return loudness


def scatter_about(key, shape, scale, bound, cuts=(), kind=jnp.bfloat16):
    result = scale * jax.random.normal(key, shape, jnp.float32)
    if cuts:
        result = result * block_levels(key, shape, cuts, -0.22, 0.18)
    return jnp.clip(result, -bound, bound).astype(kind)


def setup_inputs(seed: int = 0) -> dict:
    streams_of = jax.random.split(jax.random.key(seed), 7)
    grid_in = scatter_about(streams_of[0], (FIELDS, NLAT, NLON), 1.0, 6.0, ((0, 4), (1, 32)))
    legendre = scatter_about(streams_of[1], (MW, NLAT // 2, MW), (NLAT // 2) ** -0.5, 0.15625, ((0, 128),))
    wave_slot = draw_wave_slot(jax.random.fold_in(streams_of[6], 71), 0)
    lat_modes = draw_lat_modes(jax.random.fold_in(streams_of[6], 71), 0)
    gauss_weight = jnp.clip(jnp.exp(jax.random.uniform(streams_of[4], (NLAT // 2,), jnp.float32, math.log(0.5), math.log(2.0))), 0.5, 2.0)
    diffusion = jnp.clip(jnp.exp(jax.random.uniform(streams_of[5], (FIELDS,), jnp.float32, math.log(0.5), math.log(8.0))), 0.5, 8.0)
    return {"grid_in": grid_in, "legendre": legendre, "wave_slot": wave_slot, "lat_modes": lat_modes, "gauss_weight": gauss_weight, "diffusion": diffusion}


def angle_table(waves, lon_count):
    points = jnp.arange(lon_count, dtype=jnp.int32)
    phase_index = points[:, None] * waves[None, :] % lon_count
    radians = phase_index.astype(jnp.float32) * (2.0 * math.pi / lon_count)
    norm_scale = 1.0 / math.sqrt(lon_count)
    return jnp.stack([jnp.cos(radians) * norm_scale, -jnp.sin(radians) * norm_scale], 1).astype(jnp.bfloat16)

def damping(waves, damp_rates, columns):
    half_cols = columns // 2
    col_index = jnp.arange(columns, dtype=jnp.int32)
    offset = jnp.where(col_index < half_cols, 2 * col_index, 2 * col_index - columns + 1)
    degree = waves[:, None] + offset[None, :]
    degree_ratio = (degree * (degree + 1)).astype(jnp.float32) / float(LMAX * (LMAX + 1))
    factor = 1.0 / (1.0 + damp_rates[None, :, None] * (degree_ratio ** 4)[:, None, :])
    return jnp.where((degree <= LMAX)[:, None, :], factor, 0.0)

def reference(grid_in, legendre, wave_slot, lat_modes, gauss_weight, diffusion):
    highest = lax.Precision.HIGHEST
    angles = angle_table(wave_slot, NLON)
    keep_mask = (wave_slot[:, None] < lat_modes[None, :]).astype(jnp.float32)
    fourier = jnp.einsum('fjx,xrs->rsfj', grid_in.astype(jnp.float32), angles.astype(jnp.float32), precision=highest)
    fourier = (fourier * keep_mask[None, :, None, :]).astype(jnp.bfloat16)
    half_cols = MW // 2
    half_lats = NLAT // 2

    def per_slot(slot_items):
        slot_data, tables, slot_wave = slot_items
        north_half = slot_data[..., :half_lats].astype(jnp.float32)
        south_half = jnp.flip(slot_data[..., half_lats:], -1).astype(jnp.float32)
        even_part = ((north_half + south_half) * gauss_weight).astype(jnp.bfloat16)
        odd_part = ((north_half - south_half) * gauss_weight).astype(jnp.bfloat16)
        table_wide = tables.astype(jnp.float32)
        even_cols = jnp.einsum('rfj,jq->rfq', even_part.astype(jnp.float32), table_wide[:, :half_cols], precision=highest)
        odd_cols = jnp.einsum('rfj,jq->rfq', odd_part.astype(jnp.float32), table_wide[:, half_cols:], precision=highest)
        raw_coeff = jnp.concatenate([even_cols, odd_cols], -1)
        spectra = raw_coeff * damping(slot_wave[None], diffusion, MW)[0][None]
        rounded = spectra.astype(jnp.bfloat16).astype(jnp.float32)
        sym_part = jnp.einsum('rfq,jq->rfj', rounded[..., :half_cols], table_wide[:, :half_cols], precision=highest)
        anti_part = jnp.einsum('rfq,jq->rfj', rounded[..., half_cols:], table_wide[:, half_cols:], precision=highest)
        synthesized = jnp.concatenate([(sym_part + anti_part).astype(jnp.bfloat16), jnp.flip((sym_part - anti_part).astype(jnp.bfloat16), -1)], -1)
        return (spectra, synthesized)
    spectra, synthesized = lax.map(per_slot, (jnp.moveaxis(fourier, 1, 0), legendre, wave_slot))
    spectra = jnp.moveaxis(spectra, 0, 1)
    masked = synthesized.astype(jnp.float32) * keep_mask[:, None, None, :]
    grid_out = 2.0 * jnp.einsum('srfj,xrs->fjx', masked, angles.astype(jnp.float32), precision=highest)
    return (grid_out, spectra)
```

```python
import functools
import math

import jax
import jax.numpy as jnp
from jax import lax
from jax.experimental import pallas as pl
from jax.experimental.pallas import tpu as pltpu
from jax.sharding import PartitionSpec as P

LMAX = 1279
MESH = pl.DeviceIdType.MESH
F32 = jnp.float32
BF16 = jnp.bfloat16

LON = 2688
ROW_A, ROW_B, ROW_C = 14, 12, 16
GROUPS = 16
TRIG_ROWS = 48
NT = (((1,), (1,)), ((), ()))

ORDER = (
    (1, 1), (3, 3), (1, 3), (3, 1), (1, 0), (3, 0), (0, 1), (0, 3),
    (2, 1), (2, 3), (1, 2), (3, 2), (2, 0), (0, 2), (2, 2), (0, 0),
)


def position():
    lat = lax.axis_index("lat")
    return lat // 8, lax.rem(lat // 2, 4), lat, lax.axis_index("fld")


def group_at(step):
    z, x, _, _ = position()
    dz, dx = jnp.int32(0), jnp.int32(0)
    for n, (a, b) in enumerate(ORDER):
        dz = jnp.where(step == n, a, dz)
        dx = jnp.where(step == n, b, dx)
    return lax.rem(z + dz, 4) * 4 + lax.rem(x + dx, 4)


def greet():
    barrier = pltpu.get_barrier_semaphore()
    _, _, lat, fld = position()
    me = lat * 4 + fld

    def signal(n, carry):
        peer = lax.rem(me + n, 128)
        pl.semaphore_signal(
            barrier, inc=1, device_id=(peer // 4, lax.rem(peer, 4)), device_id_type=MESH
        )
        return carry

    lax.fori_loop(1, 128, signal, 0)


def greeted():
    pl.semaphore_wait(pltpu.get_barrier_semaphore(), 127)


def send_group(group, source, target, send_sem, recv_sem, own_sem):
    _, _, lat, fld = position()
    me = lat * 4 + fld

    def send(n, carry):
        to = group * 8 + n
        @pl.when(to != me)
        def _():
            pltpu.make_async_remote_copy(
                src_ref=source.at[to],
                dst_ref=target.at[me],
                send_sem=send_sem,
                recv_sem=recv_sem,
                device_id=(to // 4, lax.rem(to, 4)),
                device_id_type=MESH,
            ).start()

        @pl.when(to == me)
        def _():
            pltpu.make_async_copy(source.at[me], target.at[me], own_sem).start()

        return carry

    lax.fori_loop(0, 8, send, 0)


def wait_all(source, target, send_sem, recv_sem, own_sem):
    _, _, lat, fld = position()
    pltpu.make_async_copy(source.at[0], target.at[0], own_sem).wait()
    pltpu.make_async_remote_copy(
        src_ref=source.at[pl.ds(0, 127)],
        dst_ref=target.at[pl.ds(0, 127)],
        send_sem=send_sem,
        recv_sem=recv_sem,
        device_id=(lat, fld),
        device_id_type=MESH,
    ).wait()


def lanes(rows=16):
    return lax.broadcasted_iota(jnp.int32, (rows, 128), 1)


def swap_blocks(parts):
    block = lanes() // 16
    turned = [p if i == 0 else pltpu.roll(p, 16 * i, 1) for i, p in enumerate(parts)]
    row = [turned[(-i) % 8] for i in range(8)]
    for bit in (1, 2, 4):
        mask = (block & bit) != 0
        row = [jnp.where(mask, row[(i - bit) % 8], row[i]) for i in range(8)]
    return [p if d == 0 else pltpu.roll(p, 128 - 16 * d, 1) for d, p in enumerate(row)]


def make_table(trig_cos, trig_sin, group, half, uv, table):
    cos_b = trig_cos.at[group]
    sin_b = trig_sin.at[group]
    cos_c = cos_b[ROW_A + ROW_B : ROW_A + ROW_B + ROW_C]
    sin_c = sin_b[ROW_A + ROW_B : ROW_A + ROW_B + ROW_C]
    for b in range(ROW_B):
        cb, sb = cos_b[ROW_A + b : ROW_A + b + 1], sin_b[ROW_A + b : ROW_A + b + 1]
        uv[0, 16 * b : 16 * b + 16] = cb * cos_c - sb * sin_c
        uv[1, 16 * b : 16 * b + 16] = sb * cos_c + cb * sin_c
    for a in range(ROW_A):
        ca, sa = cos_b[a : a + 1], sin_b[a : a + 1]
        table[192 * a : 192 * a + 192, 128 * half : 128 * half + 128] = (
            ca * uv[0] - sa * uv[1]
        ).astype(BF16)


def forward_kernel(
    grid_ref, cos_ref, sin_ref, waves_ref, modes_ref, recv_ref, angles_ref,
    uv, table, result, last_rows, outbox, send_sem, recv_sem, own_sem, table_sem,
):
    greet()
    lane16 = lax.rem(lanes(), 16)

    def step_body(step, carry):
        groups = (group_at(2 * step), group_at(2 * step + 1))
        for half in range(2):
            make_table(cos_ref, sin_ref, groups[half], half, uv, table)
        copies = [
            pltpu.make_async_copy(
                table.at[:, pl.ds(128 * half, 128)],
                angles_ref.at[:, pl.ds(pl.multiple_of(groups[half] * 128, 128), 128)],
                table_sem.at[half],
            )
            for half in range(2)
        ]
        for copy in copies:
            copy.start()
        result[...] = jnp.dot(grid_ref[...], table[...], preferred_element_type=F32)
        for half in range(2):
            waves = waves_ref[groups[half]]
            for q in (4, 0, 1, 2, 3):
                keep = waves < modes_ref[16 * q : 16 * q + 16]
                parts = [
                    jnp.where(
                        keep,
                        result[80 * f + 16 * q : 80 * f + 16 * q + 16, 128 * half : 128 * half + 128],
                        0.0,
                    )
                    for f in range(8)
                ]
                for d, part in enumerate(swap_blocks(parts)):
                    if q == 4:
                        last_rows[d] = part
                        continue
                    if q < 3:
                        moved = pltpu.roll(last_rows[d], 12 - 4 * q, 1)
                        part = jnp.where(lane16 >= 12, moved, part)
                    outbox[groups[half] * 8 + d, 16 * q : 16 * q + 16] = part.astype(BF16)
        for copy in copies:
            copy.wait()

        @pl.when(step == 0)
        def _():
            greeted()

        for half in range(2):
            send_group(groups[half], outbox, recv_ref, send_sem, recv_sem, own_sem)
        return carry

    lax.fori_loop(0, GROUPS // 2, step_body, 0)
    wait_all(outbox, recv_ref, send_sem, recv_sem, own_sem)


def unpack_last(read):
    lane16 = lax.rem(lanes(), 16)
    last = jnp.zeros((16, 128), F32)
    for c in range(3):
        piece = pltpu.roll(read(c).astype(F32), 128 - (12 - 4 * c), 1)
        last = jnp.where((lane16 >= 4 * c) & (lane16 < 4 * c + 4), piece, last)
    return last


def flip_matrix():
    row = lax.broadcasted_iota(jnp.int32, (128, 128), 0)
    col = lax.broadcasted_iota(jnp.int32, (128, 128), 1)
    return jnp.where(row + col == 127, 1.0, 0.0).astype(BF16), jnp.where(
        row == col, 1.0, 0.0
    ).astype(BF16)


def project_kernel(
    waves_ref, inbox, table_ref, weight_ref, pick_ref, rate_ref, coeff_ref, folded, even, odd
):
    slot = pl.program_id(0)

    @pl.when(slot == 0)
    def _():
        def unpack(i, carry):
            for k in range(4):
                message = inbox.at[i * 4 + k]
                cols = slice(128 * k, 128 * k + 128)
                folded[pl.ds(pl.multiple_of(80 * i, 16), 64), cols] = message[...]
                last = unpack_last(lambda c: message[16 * c : 16 * c + 16])
                folded[pl.ds(pl.multiple_of(80 * i + 64, 16), 16), cols] = last.astype(BF16)
            return carry

        lax.fori_loop(0, 32, unpack, 0)
        flip, _ = flip_matrix()
        for b in range(10):
            north = folded[128 * b : 128 * b + 128].astype(F32)
            low = 1280 + 128 * (9 - b)
            south = jnp.dot(flip, folded[low : low + 128], preferred_element_type=F32)
            weight = weight_ref[128 * b : 128 * b + 128]
            for target, value in ((even, north + south), (odd, north - south)):
                part = (value * weight).astype(BF16)
                target[:, 128 * b : 128 * b + 128] = lax.dot_general(
                    pick_ref[...], part, NT, preferred_element_type=F32
                ).astype(BF16)

    rows = pl.ds(pl.multiple_of(64 * slot, 64), 64)
    table = table_ref.at[0]
    wave = waves_ref[slot]
    for parity, source in enumerate((even, odd)):
        cols = slice(384 * parity, 384 * parity + 384)
        raw = jnp.dot(source[rows], table[:, cols], preferred_element_type=F32)
        col = lax.broadcasted_iota(jnp.int32, (32, 384), 1)
        degree = wave + 2 * col + parity
        ratio = (degree * (degree + 1)).astype(F32) / float(LMAX * (LMAX + 1))
        square = ratio * ratio
        factor = 1.0 / (1.0 + rate_ref[...] * (square * square))
        factor = jnp.where(degree <= LMAX, factor, 0.0)
        coeff_ref[0, 0:32, cols] = (raw[0:32] * factor).astype(BF16)
        coeff_ref[0, 32:64, cols] = (raw[32:64] * factor).astype(BF16)


def expand_kernel(
    coeff_ref, table_ref, place_ref, recv_ref,
    north, south, wide, outbox, send_sem, recv_sem, own_sem,
):
    slot = pl.program_id(0)

    @pl.when(slot == 0)
    def _():
        greet()

    rows = pl.ds(pl.multiple_of(64 * slot, 64), 64)
    table = table_ref.at[0]
    sym = lax.dot_general(coeff_ref[0, :, 0:384], table[:, 0:384], NT, preferred_element_type=F32)
    anti = lax.dot_general(
        coeff_ref[0, :, 384:768], table[:, 384:768], NT, preferred_element_type=F32
    )
    north[rows] = (sym + anti).astype(BF16)
    south[rows] = (sym - anti).astype(BF16)

    @pl.when(slot == 5)
    def _():
        flip, same = flip_matrix()
        for b in range(10):
            cols = slice(128 * b, 128 * b + 128)
            for source, turn, low in (
                (north, same, 128 * b),
                (south, flip, 1280 + 128 * (9 - b)),
            ):
                placed = jnp.dot(
                    place_ref[...], source[:, cols], preferred_element_type=F32
                ).astype(BF16)
                wide[low : low + 128] = lax.dot_general(
                    turn, placed, NT, preferred_element_type=F32
                ).astype(BF16)
        lane16 = lax.rem(lanes(), 16)
        greeted()

        def pack(step, carry):
            group = group_at(step)
            for core in range(2):
                lat = group * 2 + core
                for k in range(4):
                    cols = slice(128 * k, 128 * k + 128)
                    to = lat * 4 + k
                    last = wide[pl.ds(pl.multiple_of(80 * lat + 64, 16), 16), cols].astype(F32)
                    for q in range(4):
                        part = wide[pl.ds(pl.multiple_of(80 * lat + 16 * q, 16), 16), cols]
                        if q < 3:
                            moved = pltpu.roll(last, 12 - 4 * q, 1)
                            part = jnp.where(lane16 >= 12, moved, part.astype(F32)).astype(BF16)
                        outbox[to, 16 * q : 16 * q + 16] = part
            send_group(group, outbox, recv_ref, send_sem, recv_sem, own_sem)
            return carry

        lax.fori_loop(0, GROUPS, pack, 0)
        wait_all(outbox, recv_ref, send_sem, recv_sem, own_sem)


def backward_kernel(inbox, angles_ref, waves_ref, modes_ref, out_ref, spread):
    @pl.when(pl.program_id(0) == 0)
    def _():
        for group in range(GROUPS):
            waves = waves_ref[group]
            for q in range(5):
                keep = waves < modes_ref[16 * q : 16 * q + 16]
                parts = []
                for d in range(8):
                    message = inbox.at[group * 8 + d]
                    if q < 4:
                        parts.append(message[16 * q : 16 * q + 16].astype(F32))
                    else:
                        parts.append(unpack_last(lambda c: message[16 * c : 16 * c + 16]))
                for f, part in enumerate(swap_blocks(parts)):
                    spread[80 * f + 16 * q : 80 * f + 16 * q + 16, 128 * group : 128 * group + 128] = (
                        jnp.where(keep, 2.0 * part, 0.0).astype(BF16)
                    )

    out_ref[...] = lax.dot_general(spread[...], angles_ref[...], NT, preferred_element_type=F32)


def trig_tables(wave_slot):
    waves = jnp.repeat(wave_slot.reshape(128, 6), 2, axis=1)
    waves = jnp.pad(waves, ((0, 0), (0, 4))).reshape(GROUPS, 1, 128)
    column = lax.broadcasted_iota(jnp.int32, (GROUPS, TRIG_ROWS, 128), 2) % 16
    row = lax.broadcasted_iota(jnp.int32, (GROUPS, TRIG_ROWS, 128), 1)
    first = row < ROW_A
    factor = jnp.where(
        first, 192 * row, jnp.where(row < ROW_A + ROW_B, 16 * (row - ROW_A), row - ROW_A - ROW_B)
    )
    turn = jnp.where(first & (column % 2 == 1), LON // 4, 0)
    index = (factor * waves + turn) % LON
    radians = index.astype(F32) * (2.0 * math.pi / LON)
    scale = jnp.where(first, jnp.where(column < 12, 1.0 / math.sqrt(LON), 0.0), 1.0)
    return jnp.cos(radians) * scale, jnp.sin(radians) * scale, waves


def pick_matrix():
    row = lax.broadcasted_iota(jnp.int32, (384, 512), 0)
    col = lax.broadcasted_iota(jnp.int32, (384, 512), 1)
    slot, part, block = row // 64, (row // 32) % 2, row % 32
    return jnp.where(col == 16 * block + 2 * slot + part, 1.0, 0.0).astype(BF16)


VMEM = pl.BlockSpec(memory_space=pltpu.VMEM)
SMEM = pl.BlockSpec(memory_space=pltpu.SMEM)
ANY = pl.BlockSpec(memory_space=pl.ANY)
INBOX = jax.ShapeDtypeStruct((128, 64, 128), BF16)
LIMIT = 60 * 1024 * 1024


def whole(shape):
    return pl.BlockSpec(shape, lambda i: (0,) * len(shape))


def body(grid_in, legendre, wave_slot, lat_modes, gauss_weight, diffusion):
    lat_index = lax.axis_index("lat")
    fld_index = lax.axis_index("fld")
    grid_rows = grid_in.reshape(640, LON)
    modes = lat_modes.reshape(80, 1)
    cosines, sines, waves = trig_tables(wave_slot)

    arrived, angles = pl.pallas_call(
        forward_kernel,
        name="forward",
        out_shape=(INBOX, jax.ShapeDtypeStruct((LON, 2048), BF16)),
        in_specs=[VMEM] * 5,
        out_specs=(ANY, ANY),
        scratch_shapes=[
            pltpu.VMEM((2, 192, 128), F32),
            pltpu.VMEM((LON, 256), BF16),
            pltpu.VMEM((640, 256), F32),
            pltpu.VMEM((8, 16, 128), F32),
            pltpu.VMEM((128, 64, 128), BF16),
            pltpu.SemaphoreType.DMA,
            pltpu.SemaphoreType.DMA,
            pltpu.SemaphoreType.DMA,
            pltpu.SemaphoreType.DMA((2,)),
        ],
        compiler_params=pltpu.CompilerParams(
            collective_id=0, has_side_effects=True, vmem_limit_bytes=LIMIT
        ),
    )(grid_rows, cosines, sines, waves, modes)

    own = lax.dynamic_slice_in_dim(wave_slot, (lat_index * 4 + fld_index) * 6, 6)
    table_spec = pl.BlockSpec((1, 1280, 768), lambda s: (s, 0, 0))
    coeff_spec = pl.BlockSpec((1, 64, 768), lambda s: (s, 0, 0))
    pick = pick_matrix()
    coeff = pl.pallas_call(
        project_kernel,
        name="project",
        grid=(6,),
        out_shape=jax.ShapeDtypeStruct((6, 64, 768), BF16),
        in_specs=[
            SMEM, whole((128, 64, 128)), table_spec, whole((1280, 1)), whole((384, 512)),
            whole((32, 1)),
        ],
        out_specs=coeff_spec,
        scratch_shapes=[
            pltpu.VMEM((2560, 512), BF16),
            pltpu.VMEM((384, 1280), BF16),
            pltpu.VMEM((384, 1280), BF16),
        ],
        compiler_params=pltpu.CompilerParams(vmem_limit_bytes=LIMIT),
        cost_estimate=pl.CostEstimate(
            flops=2 * 384 * 1280 * 768, bytes_accessed=14_000_000, transcendentals=0
        ),
    )(own, arrived, legendre, gauss_weight.reshape(1280, 1), pick, diffusion.reshape(32, 1))

    blocks = coeff.reshape(6, 2, 4, 8, 768)
    pieces = []
    for shift in range(4):
        piece = lax.dynamic_index_in_dim(blocks, (fld_index + shift) % 4, 2, keepdims=False)
        if shift:
            piece = lax.ppermute(piece, "fld", [(i, (i + shift) % 4) for i in range(4)])
        pieces.append(piece)

    returned = pl.pallas_call(
        expand_kernel,
        name="expand",
        grid=(6,),
        out_shape=INBOX,
        in_specs=[coeff_spec, table_spec, whole((512, 384))],
        out_specs=ANY,
        scratch_shapes=[
            pltpu.VMEM((384, 1280), BF16),
            pltpu.VMEM((384, 1280), BF16),
            pltpu.VMEM((2560, 512), BF16),
            pltpu.VMEM((128, 64, 128), BF16),
            pltpu.SemaphoreType.DMA,
            pltpu.SemaphoreType.DMA,
            pltpu.SemaphoreType.DMA,
        ],
        compiler_params=pltpu.CompilerParams(
            collective_id=1, has_side_effects=True, vmem_limit_bytes=LIMIT
        ),
        cost_estimate=pl.CostEstimate(
            flops=20 * 384 * 1280 * 768, bytes_accessed=14_000_000, transcendentals=0
        ),
    )(coeff, legendre, pick.T)

    grid_out = pl.pallas_call(
        backward_kernel,
        name="backward",
        grid=(7,),
        out_shape=jax.ShapeDtypeStruct((640, LON), F32),
        in_specs=[
            whole((128, 64, 128)),
            pl.BlockSpec((384, 2048), lambda i: (i, 0)),
            whole((GROUPS, 1, 128)),
            whole((80, 1)),
        ],
        out_specs=pl.BlockSpec((640, 384), lambda i: (0, i)),
        scratch_shapes=[pltpu.VMEM((640, 2048), BF16)],
        compiler_params=pltpu.CompilerParams(vmem_limit_bytes=LIMIT),
        cost_estimate=pl.CostEstimate(
            flops=2 * 640 * LON * 2048, bytes_accessed=20_000_000, transcendentals=0
        ),
    )(returned, angles, waves, modes)

    stacked = jnp.stack(pieces)
    spectra = jnp.stack(
        [
            lax.dynamic_index_in_dim(stacked, (fld_index - k) % 4, 0, keepdims=False)
            for k in range(4)
        ]
    )
    spectra = spectra.transpose(2, 0, 1, 3, 4).reshape(2, 24, 8, 768).astype(F32)
    return (grid_out.reshape(8, 80, LON), spectra)


def solution(mesh):
    return jax.shard_map(
        body,
        mesh=mesh,
        in_specs=(P("fld", "lat", None), P(("lat", "fld"), None, None), P(), P("lat"), P(), P()),
        out_specs=(P("fld", "lat", None), P(None, "lat", "fld", None)),
        check_vma=False,
    )
```

```python
import functools
import math

import jax
import jax.numpy as jnp
from jax import lax
from jax.experimental import pallas as pl
from jax.experimental.pallas import tpu as pltpu
from jax.sharding import PartitionSpec as P

LMAX = 1279
MESH = pl.DeviceIdType.MESH
F32 = jnp.float32
BF16 = jnp.bfloat16

LON = 2688
ROW_A, ROW_B, ROW_C = 14, 12, 16
GROUPS = 16
TRIG_ROWS = 48
NT = (((1,), (1,)), ((), ()))

ORDER = (
    (1, 1), (3, 3), (1, 3), (3, 1), (1, 0), (3, 0), (0, 1), (0, 3),
    (2, 1), (2, 3), (1, 2), (3, 2), (2, 0), (0, 2), (2, 2), (0, 0),
)


def position():
    lat = lax.axis_index("lat")
    return lat // 8, lax.rem(lat // 2, 4), lat, lax.axis_index("fld")


def group_at(step):
    z, x, _, _ = position()
    dz, dx = jnp.int32(0), jnp.int32(0)
    for n, (a, b) in enumerate(ORDER):
        dz = jnp.where(step == n, a, dz)
        dx = jnp.where(step == n, b, dx)
    return lax.rem(z + dz, 4) * 4 + lax.rem(x + dx, 4)


def greet():
    barrier = pltpu.get_barrier_semaphore()
    _, _, lat, fld = position()
    me = lat * 4 + fld

    def signal(n, carry):
        peer = lax.rem(me + n, 128)
        pl.semaphore_signal(
            barrier, inc=1, device_id=(peer // 4, lax.rem(peer, 4)), device_id_type=MESH
        )
        return carry

    lax.fori_loop(1, 128, signal, 0)


def greeted():
    pl.semaphore_wait(pltpu.get_barrier_semaphore(), 127)


def send_group(group, source, target, send_sem, recv_sem, own_sem):
    _, _, lat, fld = position()
    me = lat * 4 + fld

    def send(n, carry):
        to = group * 8 + n
        @pl.when(to != me)
        def _():
            pltpu.make_async_remote_copy(
                src_ref=source.at[to],
                dst_ref=target.at[me],
                send_sem=send_sem,
                recv_sem=recv_sem,
                device_id=(to // 4, lax.rem(to, 4)),
                device_id_type=MESH,
            ).start()

        @pl.when(to == me)
        def _():
            pltpu.make_async_copy(source.at[me], target.at[me], own_sem).start()

        return carry

    lax.fori_loop(0, 8, send, 0)


def wait_all(source, target, send_sem, recv_sem, own_sem):
    _, _, lat, fld = position()
    pltpu.make_async_copy(source.at[0], target.at[0], own_sem).wait()
    pltpu.make_async_remote_copy(
        src_ref=source.at[pl.ds(0, 127)],
        dst_ref=target.at[pl.ds(0, 127)],
        send_sem=send_sem,
        recv_sem=recv_sem,
        device_id=(lat, fld),
        device_id_type=MESH,
    ).wait()


def lanes(rows=16):
    return lax.broadcasted_iota(jnp.int32, (rows, 128), 1)


def aligned(start, size, unit=16):
    return pl.ds(pl.multiple_of(start, unit), size)


def swap_blocks(parts):
    block = lanes() // 16
    turned = [p if i == 0 else pltpu.roll(p, 16 * i, 1) for i, p in enumerate(parts)]
    row = [turned[(-i) % 8] for i in range(8)]
    for bit in (1, 2, 4):
        mask = (block & bit) != 0
        row = [jnp.where(mask, row[(i - bit) % 8], row[i]) for i in range(8)]
    return [p if d == 0 else pltpu.roll(p, 128 - 16 * d, 1) for d, p in enumerate(row)]


def spread_waves(slots_ref, waves):
    lane = lanes(GROUPS)
    group = lax.broadcasted_iota(jnp.int32, (GROUPS, 128), 0)
    flat = (8 * group + lane // 16) * 6 + jnp.minimum(lax.rem(lane, 16), 11) // 2
    at = lax.rem(flat, 128)
    total = jnp.zeros((GROUPS, 128), jnp.int32)
    for r in range(6):
        row = jnp.broadcast_to(slots_ref[r : r + 1], (GROUPS, 128))
        found = jnp.take_along_axis(row, at, axis=1, mode="promise_in_bounds")
        total = jnp.where(flat // 128 == r, found, total)
    waves[...] = total


def as_column(row):
    return jnp.broadcast_to(row, (128, 128)).T


def spread_modes(modes_ref, line, modes):
    line[...] = jnp.zeros((8, 128), F32)
    line[0:1, 0:80] = modes_ref[...].astype(F32)
    modes[...] = as_column(line[0:1])[0:80].astype(jnp.int32)


def fill_trig(waves, trig):
    column = lax.rem(lanes(TRIG_ROWS), 16)
    row = lax.broadcasted_iota(jnp.int32, (TRIG_ROWS, 128), 0)
    first = row < ROW_A
    factor = jnp.where(
        first, 192 * row, jnp.where(row < ROW_A + ROW_B, 16 * (row - ROW_A), row - ROW_A - ROW_B)
    )
    turn = jnp.where(first & (lax.rem(column, 2) == 1), LON // 4, 0)
    scale = jnp.where(first, jnp.where(column < 12, 1.0 / math.sqrt(LON), 0.0), 1.0)

    def one(group, carry):
        index = lax.rem(factor * waves[pl.ds(group, 1)] + turn, LON)
        radians = index.astype(F32) * (2.0 * math.pi / LON)
        trig[0, group] = jnp.cos(radians) * scale
        trig[1, group] = jnp.sin(radians) * scale
        return carry

    lax.fori_loop(0, GROUPS, one, 0)


def make_table(trig, group, half, uv, table):
    low = ROW_A + ROW_B
    cos_c = trig[0, group, low : low + ROW_C]
    sin_c = trig[1, group, low : low + ROW_C]
    for b in range(ROW_B):
        cb = trig[0, group, ROW_A + b : ROW_A + b + 1]
        sb = trig[1, group, ROW_A + b : ROW_A + b + 1]
        uv[0, 16 * b : 16 * b + 16] = cb * cos_c - sb * sin_c
        uv[1, 16 * b : 16 * b + 16] = sb * cos_c + cb * sin_c

    def rows(a, carry):
        ca, sa = trig[0, group, pl.ds(a, 1)], trig[1, group, pl.ds(a, 1)]
        table[aligned(192 * a, 192), 128 * half : 128 * half + 128] = (
            ca * uv[0] - sa * uv[1]
        ).astype(BF16)
        return carry

    lax.fori_loop(0, ROW_A, rows, 0)


def forward_kernel(
    grid_ref, slots_ref, modes_ref, recv_ref, angles_ref,
    waves, line, modes, trig, uv, table, result, last_rows, outbox,
    send_sem, recv_sem, own_sem, table_sem,
):
    greet()
    lane16 = lax.rem(lanes(), 16)
    spread_waves(slots_ref, waves)
    spread_modes(modes_ref, line, modes)
    fill_trig(waves, trig)

    def step_body(step, carry):
        groups = (group_at(2 * step), group_at(2 * step + 1))
        for half in range(2):
            make_table(trig, groups[half], half, uv, table)
        copies = [
            pltpu.make_async_copy(
                table.at[:, pl.ds(128 * half, 128)],
                angles_ref.at[:, aligned(groups[half] * 128, 128, 128)],
                table_sem.at[half],
            )
            for half in range(2)
        ]
        for copy in copies:
            copy.start()
        result[...] = jnp.dot(grid_ref[...], table[...], preferred_element_type=F32)
        for half in range(2):
            wave = waves[pl.ds(groups[half], 1)]

            def swapped(q):
                keep = wave < modes[aligned(16 * q, 16)]
                return swap_blocks([
                    jnp.where(
                        keep,
                        result[aligned(80 * f + 16 * q, 16), 128 * half : 128 * half + 128],
                        0.0,
                    )
                    for f in range(8)
                ])

            for d, part in enumerate(swapped(jnp.int32(4))):
                last_rows[d] = part

            def pack(q, carry):
                for d, part in enumerate(swapped(q)):
                    moved = pltpu.roll(last_rows[d], 12 - 4 * q, 1)
                    part = jnp.where((lane16 >= 12) & (q < 3), moved, part)
                    outbox[groups[half] * 8 + d, aligned(16 * q, 16)] = part.astype(BF16)
                return carry

            lax.fori_loop(0, 4, pack, 0)
        for copy in copies:
            copy.wait()

        @pl.when(step == 0)
        def _():
            greeted()

        for half in range(2):
            send_group(groups[half], outbox, recv_ref, send_sem, recv_sem, own_sem)
        return carry

    lax.fori_loop(0, GROUPS // 2, step_body, 0)
    wait_all(outbox, recv_ref, send_sem, recv_sem, own_sem)


def unpack_last(read):
    lane16 = lax.rem(lanes(), 16)
    last = jnp.zeros((16, 128), F32)
    for c in range(3):
        piece = pltpu.roll(read(c).astype(F32), 128 - (12 - 4 * c), 1)
        last = jnp.where((lane16 >= 4 * c) & (lane16 < 4 * c + 4), piece, last)
    return last


def turn_matrices():
    row = lax.broadcasted_iota(jnp.int32, (128, 128), 0)
    col = lax.broadcasted_iota(jnp.int32, (128, 128), 1)
    return jnp.where(row + col == 127, 1.0, 0.0).astype(BF16), jnp.where(
        row == col, 1.0, 0.0
    ).astype(BF16)


def fill_picks(pick, place):
    def rows_of(slot, carry):
        row = lax.broadcasted_iota(jnp.int32, (64, 512), 0)
        col = lax.broadcasted_iota(jnp.int32, (64, 512), 1)
        lane = 16 * lax.rem(row, 32) + row // 32 + 2 * slot
        pick[aligned(64 * slot, 64)] = jnp.where(col == lane, 1.0, 0.0).astype(BF16)
        return carry

    lax.fori_loop(0, 6, rows_of, 0)

    def lanes_of(block, carry):
        row = lax.broadcasted_iota(jnp.int32, (16, 384), 0)
        col = lax.broadcasted_iota(jnp.int32, (16, 384), 1)
        lane = (row // 2) * 64 + lax.rem(row, 2) * 32 + block
        place[aligned(16 * block, 16)] = jnp.where(
            (col == lane) & (row < 12), 1.0, 0.0
        ).astype(BF16)
        return carry

    lax.fori_loop(0, 32, lanes_of, 0)


def middle_kernel(
    slots_ref, inbox, table_ref, weight_ref, rate_ref, recv_ref, spec_ref,
    wide, even, odd, north, south, pick, place, line, rates, spec_box, outbox,
    send_sem, recv_sem, own_sem, spec_send, spec_recv, spec_own,
):
    slot = pl.program_id(0)
    _, _, lat, fld = position()

    @pl.when(slot == 0)
    def _():
        greet()
        fill_picks(pick, place)
        line[...] = jnp.zeros((8, 128), F32)
        line[0:1, 0:32] = rate_ref[...]
        rates[...] = as_column(line[0:1])[0:32]

        def unpack(i, carry):
            for k in range(4):
                message = inbox.at[i * 4 + k]
                cols = slice(128 * k, 128 * k + 128)
                wide[aligned(80 * i, 64), cols] = message[...]
                last = unpack_last(lambda c: message[16 * c : 16 * c + 16])
                wide[aligned(80 * i + 64, 16), cols] = last.astype(BF16)
            return carry

        lax.fori_loop(0, 32, unpack, 0)
        flip, _ = turn_matrices()

        def fold(b, carry):
            up = wide[aligned(128 * b, 128, 128)].astype(F32)
            low = wide[aligned(1280 + 128 * (9 - b), 128, 128)]
            down = jnp.dot(flip, low, preferred_element_type=F32)
            weight = as_column(weight_ref[pl.ds(b, 1)])[:, 0:1]
            for target, value in ((even, up + down), (odd, up - down)):
                part = (value * weight).astype(BF16)
                target[:, aligned(128 * b, 128, 128)] = lax.dot_general(
                    pick[...], part, NT, preferred_element_type=F32
                ).astype(BF16)
            return carry

        lax.fori_loop(0, 10, fold, 0)

    rows = aligned(64 * slot, 64)
    table = table_ref.at[0]
    wave = slots_ref[(lat * 4 + fld) * 6 + slot]
    sums = []
    for parity, source in enumerate((even, odd)):
        cols = slice(384 * parity, 384 * parity + 384)
        raw = jnp.dot(source[rows], table[:, cols], preferred_element_type=F32)
        col = lax.broadcasted_iota(jnp.int32, (32, 384), 1)
        degree = wave + 2 * col + parity
        ratio = (degree * (degree + 1)).astype(F32) / float(LMAX * (LMAX + 1))
        square = ratio * ratio
        factor = 1.0 / (1.0 + rates[:, 0:1] * (square * square))
        factor = jnp.where(degree <= LMAX, factor, 0.0)
        value = raw * jnp.concatenate([factor, factor], 0)
        for r in range(2):
            for k in range(4):
                spec_box[slot, r, k, :, cols] = value[32 * r + 8 * k : 32 * r + 8 * k + 8].astype(BF16)
        sums.append(
            lax.dot_general(value.astype(BF16), table[:, cols], NT, preferred_element_type=F32)
        )
    north[rows] = (sums[0] + sums[1]).astype(BF16)
    south[rows] = (sums[0] - sums[1]).astype(BF16)

    @pl.when(slot == 0)
    def _():
        greeted()

    for shift in range(4):
        to = lax.rem(fld + shift, 4)
        source, target = spec_box.at[slot, :, to], spec_ref.at[fld, slot]
        if shift:
            pltpu.make_async_remote_copy(
                src_ref=source, dst_ref=target, send_sem=spec_send, recv_sem=spec_recv,
                device_id=(lat, to), device_id_type=MESH,
            ).start()
        else:
            pltpu.make_async_copy(source, target, spec_own).start()

    @pl.when(slot == 5)
    def _():
        flip, same = turn_matrices()

        def turn(b, carry):
            cols = aligned(128 * b, 128, 128)
            for source, matrix, low in (
                (north, same, 128 * b),
                (south, flip, 1280 + 128 * (9 - b)),
            ):
                placed = jnp.dot(
                    place[...], source[:, cols], preferred_element_type=F32
                ).astype(BF16)
                wide[aligned(low, 128, 128)] = lax.dot_general(
                    matrix, placed, NT, preferred_element_type=F32
                ).astype(BF16)
            return carry

        lax.fori_loop(0, 10, turn, 0)
        lane16 = lax.rem(lanes(), 16)

        def pack(step, carry):
            group = group_at(step)
            for core in range(2):
                at = 80 * (group * 2 + core)
                for k in range(4):
                    cols = slice(128 * k, 128 * k + 128)
                    to = (group * 2 + core) * 4 + k
                    last = wide[aligned(at + 64, 16), cols].astype(F32)
                    for q in range(4):
                        part = wide[aligned(at + 16 * q, 16), cols]
                        if q < 3:
                            moved = pltpu.roll(last, 12 - 4 * q, 1)
                            part = jnp.where(lane16 >= 12, moved, part.astype(F32)).astype(BF16)
                        outbox[to, 16 * q : 16 * q + 16] = part
            send_group(group, outbox, recv_ref, send_sem, recv_sem, own_sem)
            return carry

        lax.fori_loop(0, GROUPS, pack, 0)
        pltpu.make_async_copy(spec_ref.at[0], spec_ref.at[0], spec_own).wait()
        pltpu.make_async_remote_copy(
            src_ref=spec_ref.at[pl.ds(0, 3)], dst_ref=spec_ref.at[pl.ds(0, 3)],
            send_sem=spec_send, recv_sem=spec_recv, device_id=(lat, fld), device_id_type=MESH,
        ).wait()
        wait_all(outbox, recv_ref, send_sem, recv_sem, own_sem)


def backward_kernel(inbox, angles_ref, slots_ref, modes_ref, out_ref, waves, line, modes, spread):
    @pl.when(pl.program_id(0) == 0)
    def _():
        spread_waves(slots_ref, waves)
        spread_modes(modes_ref, line, modes)

        def gather(group, carry):
            wave = waves[pl.ds(group, 1)]
            cols = aligned(128 * group, 128, 128)

            def put(q, parts):
                keep = wave < modes[aligned(16 * q, 16)]
                for f, part in enumerate(swap_blocks(parts)):
                    spread[aligned(80 * f + 16 * q, 16), cols] = jnp.where(
                        keep, 2.0 * part, 0.0
                    ).astype(BF16)

            def rows(q, carry):
                put(q, [inbox[group * 8 + d, aligned(16 * q, 16)].astype(F32) for d in range(8)])
                return carry

            lax.fori_loop(0, 4, rows, 0)
            put(
                jnp.int32(4),
                [
                    unpack_last(lambda c: inbox[group * 8 + d, 16 * c : 16 * c + 16])
                    for d in range(8)
                ],
            )
            return carry

        lax.fori_loop(0, GROUPS, gather, 0)

    out_ref[...] = lax.dot_general(spread[...], angles_ref[...], NT, preferred_element_type=F32)


VMEM = pl.BlockSpec(memory_space=pltpu.VMEM)
SMEM = pl.BlockSpec(memory_space=pltpu.SMEM)
ANY = pl.BlockSpec(memory_space=pl.ANY)
INBOX = jax.ShapeDtypeStruct((128, 64, 128), BF16)
LIMIT = 60 * 1024 * 1024


def whole(shape):
    return pl.BlockSpec(shape, lambda i: (0,) * len(shape))


def body(grid_in, legendre, wave_slot, lat_modes, gauss_weight, diffusion):
    grid_rows = grid_in.reshape(640, LON)
    modes = lat_modes.reshape(1, 80)
    slots = wave_slot.reshape(6, 128)

    arrived, angles = pl.pallas_call(
        forward_kernel,
        name="forward",
        out_shape=(INBOX, jax.ShapeDtypeStruct((LON, 2048), BF16)),
        in_specs=[VMEM] * 3,
        out_specs=(ANY, ANY),
        scratch_shapes=[
            pltpu.VMEM((GROUPS, 128), jnp.int32),
            pltpu.VMEM((8, 128), F32),
            pltpu.VMEM((80, 128), jnp.int32),
            pltpu.VMEM((2, GROUPS, TRIG_ROWS, 128), F32),
            pltpu.VMEM((2, 192, 128), F32),
            pltpu.VMEM((LON, 256), BF16),
            pltpu.VMEM((640, 256), F32),
            pltpu.VMEM((8, 16, 128), F32),
            pltpu.VMEM((128, 64, 128), BF16),
            pltpu.SemaphoreType.DMA,
            pltpu.SemaphoreType.DMA,
            pltpu.SemaphoreType.DMA,
            pltpu.SemaphoreType.DMA((2,)),
        ],
        compiler_params=pltpu.CompilerParams(
            collective_id=0, has_side_effects=True, vmem_limit_bytes=LIMIT
        ),
    )(grid_rows, slots, modes)

    returned, spectra = pl.pallas_call(
        middle_kernel,
        name="middle",
        grid=(6,),
        out_shape=(INBOX, jax.ShapeDtypeStruct((4, 6, 2, 8, 768), BF16)),
        in_specs=[
            SMEM,
            whole((128, 64, 128)),
            pl.BlockSpec((1, 1280, 768), lambda s: (s, 0, 0)),
            whole((10, 128)),
            whole((1, 32)),
        ],
        out_specs=(ANY, ANY),
        scratch_shapes=[
            pltpu.VMEM((2560, 512), BF16),
            pltpu.VMEM((384, 1280), BF16),
            pltpu.VMEM((384, 1280), BF16),
            pltpu.VMEM((384, 1280), BF16),
            pltpu.VMEM((384, 1280), BF16),
            pltpu.VMEM((384, 512), BF16),
            pltpu.VMEM((512, 384), BF16),
            pltpu.VMEM((8, 128), F32),
            pltpu.VMEM((32, 128), F32),
            pltpu.VMEM((6, 2, 4, 8, 768), BF16),
            pltpu.VMEM((128, 64, 128), BF16),
        ]
        + [pltpu.SemaphoreType.DMA] * 6,
        compiler_params=pltpu.CompilerParams(
            collective_id=1, has_side_effects=True, vmem_limit_bytes=LIMIT
        ),
    )(wave_slot, arrived, legendre, gauss_weight.reshape(10, 128), diffusion.reshape(1, 32))

    grid_out = pl.pallas_call(
        backward_kernel,
        name="backward",
        grid=(7,),
        out_shape=jax.ShapeDtypeStruct((640, LON), F32),
        in_specs=[
            whole((128, 64, 128)),
            pl.BlockSpec((384, 2048), lambda i: (i, 0)),
            whole((6, 128)),
            whole((1, 80)),
        ],
        out_specs=pl.BlockSpec((640, 384), lambda i: (0, i)),
        scratch_shapes=[
            pltpu.VMEM((GROUPS, 128), jnp.int32),
            pltpu.VMEM((8, 128), F32),
            pltpu.VMEM((80, 128), jnp.int32),
            pltpu.VMEM((640, 2048), BF16),
        ],
        compiler_params=pltpu.CompilerParams(vmem_limit_bytes=LIMIT),
    )(returned, angles, slots, modes)

    spectra = spectra.transpose(2, 0, 1, 3, 4).reshape(2, 24, 8, 768).astype(F32)
    return (grid_out.reshape(8, 80, LON), spectra)


def solution(mesh):
    return jax.shard_map(
        body,
        mesh=mesh,
        in_specs=(P("fld", "lat", None), P(("lat", "fld"), None, None), P(), P("lat"), P(), P()),
        out_specs=(P("fld", "lat", None), P(None, "lat", "fld", None)),
        check_vma=False,
    )
```

```python
import functools
import math

import jax
import jax.numpy as jnp
from jax import lax
from jax.experimental import pallas as pl
from jax.experimental.pallas import tpu as pltpu
from jax.sharding import PartitionSpec as P

LMAX = 1279
MESH = pl.DeviceIdType.MESH
F32 = jnp.float32
BF16 = jnp.bfloat16

LON = 2688
ROW_A, ROW_B, ROW_C = 14, 12, 16
GROUPS = 16
TRIG_ROWS = 48
NT = (((1,), (1,)), ((), ()))

ORDER = (
    (1, 1), (3, 3), (1, 3), (3, 1), (1, 0), (3, 0), (0, 1), (0, 3),
    (2, 1), (2, 3), (1, 2), (3, 2), (2, 0), (0, 2), (2, 2), (0, 0),
)


def position():
    lat = lax.axis_index("lat")
    return lat // 8, lax.rem(lat // 2, 4), lat, lax.axis_index("fld")


def group_at(step):
    z, x, _, _ = position()
    dz, dx = jnp.int32(0), jnp.int32(0)
    for n, (a, b) in enumerate(ORDER):
        dz = jnp.where(step == n, a, dz)
        dx = jnp.where(step == n, b, dx)
    return lax.rem(z + dz, 4) * 4 + lax.rem(x + dx, 4)


def greet():
    barrier = pltpu.get_barrier_semaphore()
    _, _, lat, fld = position()
    me = lat * 4 + fld

    def signal(n, carry):
        peer = lax.rem(me + n, 128)
        pl.semaphore_signal(
            barrier, inc=1, device_id=(peer // 4, lax.rem(peer, 4)), device_id_type=MESH
        )
        return carry

    lax.fori_loop(1, 128, signal, 0)


def greeted():
    pl.semaphore_wait(pltpu.get_barrier_semaphore(), 127)


def send_one(to, source, target, send_sem, recv_sem, own_sem):
    _, _, lat, fld = position()
    me = lat * 4 + fld

    @pl.when(to != me)
    def _():
        pltpu.make_async_remote_copy(
            src_ref=source, dst_ref=target, send_sem=send_sem, recv_sem=recv_sem,
            device_id=(to // 4, lax.rem(to, 4)), device_id_type=MESH,
        ).start()

    @pl.when(to == me)
    def _():
        pltpu.make_async_copy(source, target, own_sem).start()


def wait_all(one, others, send_sem, recv_sem, own_sem):
    _, _, lat, fld = position()
    pltpu.make_async_copy(one, one, own_sem).wait()
    pltpu.make_async_remote_copy(
        src_ref=others, dst_ref=others, send_sem=send_sem, recv_sem=recv_sem,
        device_id=(lat, fld), device_id_type=MESH,
    ).wait()


def lanes(rows=16):
    return lax.broadcasted_iota(jnp.int32, (rows, 128), 1)


def aligned(start, size, unit=16):
    return pl.ds(pl.multiple_of(start, unit), size)


def swap_blocks(parts):
    block = lanes() // 16
    turned = [p if i == 0 else pltpu.roll(p, 16 * i, 1) for i, p in enumerate(parts)]
    row = [turned[(-i) % 8] for i in range(8)]
    for bit in (1, 2, 4):
        mask = (block & bit) != 0
        row = [jnp.where(mask, row[(i - bit) % 8], row[i]) for i in range(8)]
    return [p if d == 0 else pltpu.roll(p, 128 - 16 * d, 1) for d, p in enumerate(row)]


def spread_waves(slots_ref, waves):
    lane = lanes(GROUPS)
    group = lax.broadcasted_iota(jnp.int32, (GROUPS, 128), 0)
    flat = (8 * group + lane // 16) * 6 + jnp.minimum(lax.rem(lane, 16), 11) // 2
    at = lax.rem(flat, 128)
    total = jnp.zeros((GROUPS, 128), jnp.int32)
    for r in range(6):
        row = jnp.broadcast_to(slots_ref[r : r + 1], (GROUPS, 128))
        found = jnp.take_along_axis(row, at, axis=1, mode="promise_in_bounds")
        total = jnp.where(flat // 128 == r, found, total)
    waves[...] = total


def as_column(row):
    return jnp.broadcast_to(row, (128, 128)).T


def spread_modes(modes_ref, line, modes):
    line[...] = jnp.zeros((8, 128), F32)
    line[0:1, 0:80] = modes_ref[...].astype(F32)
    modes[...] = as_column(line[0:1])[0:80].astype(jnp.int32)


def fill_trig(waves, trig):
    column = lax.rem(lanes(TRIG_ROWS), 16)
    row = lax.broadcasted_iota(jnp.int32, (TRIG_ROWS, 128), 0)
    first = row < ROW_A
    factor = jnp.where(
        first, 192 * row, jnp.where(row < ROW_A + ROW_B, 16 * (row - ROW_A), row - ROW_A - ROW_B)
    )
    turn = jnp.where(first & (lax.rem(column, 2) == 1), LON // 4, 0)
    scale = jnp.where(first, jnp.where(column < 12, 1.0 / math.sqrt(LON), 0.0), 1.0)

    def one(group, carry):
        index = lax.rem(factor * waves[pl.ds(group, 1)] + turn, LON)
        radians = index.astype(F32) * (2.0 * math.pi / LON)
        trig[0, group] = jnp.cos(radians) * scale
        trig[1, group] = jnp.sin(radians) * scale
        return carry

    lax.fori_loop(0, GROUPS, one, 0)


def make_table(trig, group, half, uv, table):
    low = ROW_A + ROW_B
    cos_c = trig[0, group, low : low + ROW_C]
    sin_c = trig[1, group, low : low + ROW_C]
    for b in range(ROW_B):
        cb = trig[0, group, ROW_A + b : ROW_A + b + 1]
        sb = trig[1, group, ROW_A + b : ROW_A + b + 1]
        uv[0, 16 * b : 16 * b + 16] = cb * cos_c - sb * sin_c
        uv[1, 16 * b : 16 * b + 16] = sb * cos_c + cb * sin_c

    def rows(a, carry):
        ca, sa = trig[0, group, pl.ds(a, 1)], trig[1, group, pl.ds(a, 1)]
        table[aligned(192 * a, 192), 128 * half : 128 * half + 128] = (
            ca * uv[0] - sa * uv[1]
        ).astype(BF16)
        return carry

    lax.fori_loop(0, ROW_A, rows, 0)


def forward_kernel(
    grid_ref, slots_ref, modes_ref, recv_ref, angles_ref,
    waves, line, modes, trig, uv, table, result, outbox,
    send_sem, recv_sem, own_sem, table_sem,
):
    greet()
    lane16 = lax.rem(lanes(), 16)
    spread_waves(slots_ref, waves)
    spread_modes(modes_ref, line, modes)
    fill_trig(waves, trig)

    def step_body(step, carry):
        groups = (group_at(2 * step), group_at(2 * step + 1))
        for half in range(2):
            make_table(trig, groups[half], half, uv, table)
        copies = [
            pltpu.make_async_copy(
                table.at[:, pl.ds(128 * half, 128)],
                angles_ref.at[:, aligned(groups[half] * 128, 128, 128)],
                table_sem.at[half],
            )
            for half in range(2)
        ]
        for copy in copies:
            copy.start()
        result[...] = jnp.dot(grid_ref[...], table[...], preferred_element_type=F32)
        for half in range(2):
            wave = waves[pl.ds(groups[half], 1)]

            def swapped(q):
                keep = wave < modes[16 * q : 16 * q + 16]
                return swap_blocks([
                    jnp.where(
                        keep,
                        result[80 * f + 16 * q : 80 * f + 16 * q + 16, 128 * half : 128 * half + 128],
                        0.0,
                    )
                    for f in range(8)
                ])

            last = swapped(4)
            for q in range(4):
                for d, part in enumerate(swapped(q)):
                    if q < 3:
                        part = jnp.where(lane16 >= 12, pltpu.roll(last[d], 12 - 4 * q, 1), part)
                    outbox[groups[half] * 8 + d, 16 * q : 16 * q + 16] = part.astype(BF16)
        for copy in copies:
            copy.wait()

        @pl.when(step == 0)
        def _():
            greeted()

        _, _, lat, fld = position()
        landing = recv_ref.at[aligned(80 * lat, 64), aligned(128 * fld, 128, 128)]
        for half in range(2):
            def send(n, carry):
                to = groups[half] * 8 + n
                send_one(to, outbox.at[to], landing, send_sem, recv_sem, own_sem)
                return carry

            lax.fori_loop(0, 8, send, 0)
        return carry

    lax.fori_loop(0, GROUPS // 2, step_body, 0)
    wait_all(
        outbox.at[0], recv_ref.at[pl.ds(0, 2032)], send_sem, recv_sem, own_sem
    )


def unpack_last(read):
    lane16 = lax.rem(lanes(), 16)
    last = jnp.zeros((16, 128), F32)
    for c in range(3):
        piece = pltpu.roll(read(c).astype(F32), 128 - (12 - 4 * c), 1)
        last = jnp.where((lane16 >= 4 * c) & (lane16 < 4 * c + 4), piece, last)
    return last


def flip_matrix(size):
    row = lax.broadcasted_iota(jnp.int32, (size, size), 0)
    col = lax.broadcasted_iota(jnp.int32, (size, size), 1)
    return jnp.where(row + col == size - 1, 1.0, 0.0).astype(BF16)


def fill_picks(pick, place):
    def rows_of(slot, carry):
        row = lax.broadcasted_iota(jnp.int32, (64, 512), 0)
        col = lax.broadcasted_iota(jnp.int32, (64, 512), 1)
        lane = 16 * lax.rem(row, 32) + row // 32 + 2 * slot
        pick[aligned(64 * slot, 64)] = jnp.where(col == lane, 1.0, 0.0).astype(BF16)
        return carry

    lax.fori_loop(0, 6, rows_of, 0)

    def lanes_of(chunk, carry):
        row = lax.broadcasted_iota(jnp.int32, (64, 384), 0)
        col = lax.broadcasted_iota(jnp.int32, (64, 384), 1)
        block, inner = 4 * chunk + row // 16, lax.rem(row, 16)
        lane = (inner // 2) * 64 + lax.rem(inner, 2) * 32 + block
        place[aligned(64 * chunk, 64)] = jnp.where(
            (col == lane) & (inner < 12), 1.0, 0.0
        ).astype(BF16)
        return carry

    lax.fori_loop(0, 8, lanes_of, 0)


def middle_kernel(
    slots_ref, arrived_ref, tables_ref, weight_ref, rate_ref, recv_ref, spec_ref,
    wide, tables, even, odd, north, south, pick, place, line, rates, coeff, spec_box,
    send_sem, recv_sem, own_sem, spec_send, spec_recv, spec_own, wide_sem, table_sem,
):
    z, x, lat, fld = position()
    me = lat * 4 + fld
    load = pltpu.make_async_copy(arrived_ref, wide, wide_sem)
    load.start()
    table_loads = [
        pltpu.make_async_copy(tables_ref.at[s], tables.at[s], table_sem.at[s]) for s in range(6)
    ]
    for copy in table_loads:
        copy.start()
    greet()
    fill_picks(pick, place)
    line[...] = jnp.zeros((8, 128), F32)
    line[0:1, 0:32] = rate_ref[...]
    rates[...] = as_column(line[0:1])[0:32]
    load.wait()

    def unpack(n, carry):
        for i in range(2):
            at = 80 * (2 * n + i)
            for k in range(4):
                cols = slice(128 * k, 128 * k + 128)
                last = unpack_last(lambda c: wide[aligned(at + 16 * c, 16), cols])
                wide[aligned(at + 64, 16), cols] = last.astype(BF16)
        return carry

    lax.fori_loop(0, 16, unpack, 0)
    flip = flip_matrix(256)
    for b in range(5):
        up = wide[256 * b : 256 * b + 256].astype(F32)
        low = 1280 + 256 * (4 - b)
        down = jnp.dot(flip, wide[low : low + 256], preferred_element_type=F32)
        weight = jnp.concatenate(
            [as_column(weight_ref[2 * b + u : 2 * b + u + 1])[:, 0:1] for u in range(2)], 0
        )
        for target, value in ((even, up + down), (odd, up - down)):
            target[:, 256 * b : 256 * b + 256] = lax.dot_general(
                pick[...], (value * weight).astype(BF16), NT, preferred_element_type=F32
            ).astype(BF16)

    col = lax.broadcasted_iota(jnp.int32, (32, 384), 1)
    for slot in range(6):
        table_loads[slot].wait()
        wave = slots_ref[me * 6 + slot]
        for parity, source in enumerate((even, odd)):
            cols = slice(384 * parity, 384 * parity + 384)
            raw = jnp.dot(
                source[64 * slot : 64 * slot + 64], tables[slot, :, cols],
                preferred_element_type=F32,
            )
            degree = wave + 2 * col + parity
            ratio = (degree * (degree + 1)).astype(F32) / float(LMAX * (LMAX + 1))
            square = ratio * ratio
            factor = 1.0 / (1.0 + rates[:, 0:1] * (square * square))
            factor = jnp.where(degree <= LMAX, factor, 0.0)
            value = raw * jnp.concatenate([factor, factor], 0)
            for r in range(2):
                for k in range(4):
                    low = 32 * r + 8 * k
                    spec_box[slot, r, k, :, cols] = value[low : low + 8].astype(BF16)
            coeff[slot, :, cols] = value.astype(BF16)
        if slot == 0:
            greeted()
        for shift in range(4):
            to = lax.rem(fld + shift, 4)
            source, target = spec_box.at[slot, :, to], spec_ref.at[fld, slot]
            if shift:
                pltpu.make_async_remote_copy(
                    src_ref=source, dst_ref=target, send_sem=spec_send, recv_sem=spec_recv,
                    device_id=(lat, to), device_id_type=MESH,
                ).start()
            else:
                pltpu.make_async_copy(source, target, spec_own).start()

    turn = flip_matrix(320)
    lane16 = lax.rem(lanes(), 16)

    def part_of(step, carry):
        b = lax.rem(step + 2 * lax.rem(z, 2) + x // 2, 4)
        for slot in range(6):
            sums = [
                lax.dot_general(
                    tables[slot, aligned(320 * b, 320, 64), 384 * p : 384 * p + 384],
                    coeff[slot, :, 384 * p : 384 * p + 384],
                    NT,
                    preferred_element_type=F32,
                )
                for p in range(2)
            ]
            north[:, 64 * slot : 64 * slot + 64] = (sums[0] + sums[1]).astype(BF16)
            south[:, 64 * slot : 64 * slot + 64] = (sums[0] - sums[1]).astype(BF16)
        wide[aligned(320 * b, 320, 64)] = lax.dot_general(
            north[...], place[...], NT, preferred_element_type=F32
        ).astype(BF16)
        mirrored = jnp.dot(turn, south[...], preferred_element_type=F32).astype(BF16)
        wide[aligned(1280 + 320 * (3 - b), 320, 64)] = lax.dot_general(
            mirrored, place[...], NT, preferred_element_type=F32
        ).astype(BF16)

        def pack(n, carry):
            for i in (4 * b + n, 31 - 4 * b - n):
                at = 80 * i
                for k in range(4):
                    cols = slice(128 * k, 128 * k + 128)
                    last = wide[aligned(at + 64, 16), cols].astype(F32)
                    for q in range(3):
                        rows = aligned(at + 16 * q, 16)
                        moved = pltpu.roll(last, 12 - 4 * q, 1)
                        wide[rows, cols] = jnp.where(
                            lane16 >= 12, moved, wide[rows, cols].astype(F32)
                        ).astype(BF16)
            return carry

        lax.fori_loop(0, 4, pack, 0)

        def send(n, carry):
            for i in (4 * b + n, 31 - 4 * b - n):
                for k in range(4):
                    send_one(
                        i * 4 + k, wide.at[aligned(80 * i, 64), 128 * k : 128 * k + 128],
                        recv_ref.at[me], send_sem, recv_sem, own_sem,
                    )
            return carry

        lax.fori_loop(0, 4, send, 0)
        return carry

    lax.fori_loop(0, 4, part_of, 0)
    pltpu.make_async_copy(spec_ref.at[0], spec_ref.at[0], spec_own).wait()
    pltpu.make_async_remote_copy(
        src_ref=spec_ref.at[pl.ds(0, 3)], dst_ref=spec_ref.at[pl.ds(0, 3)],
        send_sem=spec_send, recv_sem=spec_recv, device_id=(lat, fld), device_id_type=MESH,
    ).wait()
    wait_all(recv_ref.at[0], recv_ref.at[pl.ds(0, 127)], send_sem, recv_sem, own_sem)


def backward_kernel(inbox, angles_ref, slots_ref, modes_ref, out_ref, waves, line, modes, spread):
    @pl.when(pl.program_id(0) == 0)
    def _():
        spread_waves(slots_ref, waves)
        spread_modes(modes_ref, line, modes)

        def gather(group, carry):
            wave = waves[pl.ds(group, 1)]
            cols = aligned(128 * group, 128, 128)

            for q in range(5):
                keep = wave < modes[16 * q : 16 * q + 16]
                if q < 4:
                    parts = [inbox[group * 8 + d, 16 * q : 16 * q + 16].astype(F32) for d in range(8)]
                else:
                    parts = [
                        unpack_last(lambda c: inbox[group * 8 + d, 16 * c : 16 * c + 16])
                        for d in range(8)
                    ]
                for f, part in enumerate(swap_blocks(parts)):
                    spread[80 * f + 16 * q : 80 * f + 16 * q + 16, cols] = jnp.where(
                        keep, 2.0 * part, 0.0
                    ).astype(BF16)
            return carry

        lax.fori_loop(0, GROUPS, gather, 0)

    out_ref[...] = lax.dot_general(spread[...], angles_ref[...], NT, preferred_element_type=F32)


VMEM = pl.BlockSpec(memory_space=pltpu.VMEM)
SMEM = pl.BlockSpec(memory_space=pltpu.SMEM)
ANY = pl.BlockSpec(memory_space=pl.ANY)
INBOX = jax.ShapeDtypeStruct((128, 64, 128), BF16)
LIMIT = 60 * 1024 * 1024


def whole(shape):
    return pl.BlockSpec(shape, lambda i: (0,) * len(shape))


def body(grid_in, legendre, wave_slot, lat_modes, gauss_weight, diffusion):
    grid_rows = grid_in.reshape(640, LON)
    modes = lat_modes.reshape(1, 80)
    slots = wave_slot.reshape(6, 128)

    arrived, angles = pl.pallas_call(
        forward_kernel,
        name="forward",
        out_shape=(
            jax.ShapeDtypeStruct((2560, 512), BF16),
            jax.ShapeDtypeStruct((LON, 2048), BF16),
        ),
        in_specs=[VMEM] * 3,
        out_specs=(ANY, ANY),
        scratch_shapes=[
            pltpu.VMEM((GROUPS, 128), jnp.int32),
            pltpu.VMEM((8, 128), F32),
            pltpu.VMEM((80, 128), jnp.int32),
            pltpu.VMEM((2, GROUPS, TRIG_ROWS, 128), F32),
            pltpu.VMEM((2, 192, 128), F32),
            pltpu.VMEM((LON, 256), BF16),
            pltpu.VMEM((640, 256), F32),
            pltpu.VMEM((128, 64, 128), BF16),
            pltpu.SemaphoreType.DMA,
            pltpu.SemaphoreType.DMA,
            pltpu.SemaphoreType.DMA,
            pltpu.SemaphoreType.DMA((2,)),
        ],
        compiler_params=pltpu.CompilerParams(
            collective_id=0, has_side_effects=True, vmem_limit_bytes=LIMIT
        ),
    )(grid_rows, slots, modes)

    returned, spectra = pl.pallas_call(
        middle_kernel,
        name="middle",
        out_shape=(INBOX, jax.ShapeDtypeStruct((4, 6, 2, 8, 768), BF16)),
        in_specs=[SMEM, ANY, ANY, VMEM, VMEM],
        out_specs=(ANY, ANY),
        scratch_shapes=[
            pltpu.VMEM((2560, 512), BF16),
            pltpu.VMEM((6, 1280, 768), BF16),
            pltpu.VMEM((384, 1280), BF16),
            pltpu.VMEM((384, 1280), BF16),
            pltpu.VMEM((320, 384), BF16),
            pltpu.VMEM((320, 384), BF16),
            pltpu.VMEM((384, 512), BF16),
            pltpu.VMEM((512, 384), BF16),
            pltpu.VMEM((8, 128), F32),
            pltpu.VMEM((32, 128), F32),
            pltpu.VMEM((6, 64, 768), BF16),
            pltpu.VMEM((6, 2, 4, 8, 768), BF16),
        ]
        + [pltpu.SemaphoreType.DMA] * 7
        + [pltpu.SemaphoreType.DMA((6,))],
        compiler_params=pltpu.CompilerParams(
            collective_id=1, has_side_effects=True, vmem_limit_bytes=LIMIT
        ),
    )(wave_slot, arrived, legendre, gauss_weight.reshape(10, 128), diffusion.reshape(1, 32))

    grid_out = pl.pallas_call(
        backward_kernel,
        name="backward",
        grid=(7,),
        out_shape=jax.ShapeDtypeStruct((640, LON), F32),
        in_specs=[
            whole((128, 64, 128)),
            pl.BlockSpec((384, 2048), lambda i: (i, 0)),
            whole((6, 128)),
            whole((1, 80)),
        ],
        out_specs=pl.BlockSpec((640, 384), lambda i: (0, i)),
        scratch_shapes=[
            pltpu.VMEM((GROUPS, 128), jnp.int32),
            pltpu.VMEM((8, 128), F32),
            pltpu.VMEM((80, 128), jnp.int32),
            pltpu.VMEM((640, 2048), BF16),
        ],
        compiler_params=pltpu.CompilerParams(vmem_limit_bytes=LIMIT),
    )(returned, angles, slots, modes)

    spectra = spectra.transpose(2, 0, 1, 3, 4).reshape(2, 24, 8, 768).astype(F32)
    return (grid_out.reshape(8, 80, LON), spectra)


def solution(mesh):
    return jax.shard_map(
        body,
        mesh=mesh,
        in_specs=(P("fld", "lat", None), P(("lat", "fld"), None, None), P(), P("lat"), P(), P()),
        out_specs=(P("fld", "lat", None), P(None, "lat", "fld", None)),
        check_vma=False,
    )
```

```python
import functools
import math

import jax
import jax.numpy as jnp
from jax import lax
from jax.experimental import pallas as pl
from jax.experimental.pallas import tpu as pltpu
from jax.sharding import PartitionSpec as P

LMAX = 1279
MESH = pl.DeviceIdType.MESH
F32 = jnp.float32
BF16 = jnp.bfloat16

LON = 2688
ROW_A, ROW_B, ROW_C = 14, 12, 16
GROUPS = 16
TRIG_ROWS = 48
NT = (((1,), (1,)), ((), ()))

ORDER = (
    (1, 1), (3, 3), (1, 2), (3, 0), (2, 1), (0, 3), (1, 3), (3, 1),
    (3, 2), (1, 0), (2, 3), (0, 1), (2, 0), (0, 2), (2, 2), (0, 0),
)


def position():
    lat = lax.axis_index("lat")
    return lat // 8, lax.rem(lat // 2, 4), lat, lax.axis_index("fld")


def group_at(step):
    z, x, _, _ = position()
    dz, dx = jnp.int32(0), jnp.int32(0)
    for n, (a, b) in enumerate(ORDER):
        dz = jnp.where(step == n, a, dz)
        dx = jnp.where(step == n, b, dx)
    return lax.rem(z + dz, 4) * 4 + lax.rem(x + dx, 4)


def greet():
    barrier = pltpu.get_barrier_semaphore()
    _, _, lat, fld = position()
    me = lat * 4 + fld

    def signal(n, carry):
        peer = lax.rem(me + n, 128)
        pl.semaphore_signal(
            barrier, inc=1, device_id=(peer // 4, lax.rem(peer, 4)), device_id_type=MESH
        )
        return carry

    lax.fori_loop(1, 128, signal, 0)


def greeted():
    pl.semaphore_wait(pltpu.get_barrier_semaphore(), 127)


def send_one(to, source, target, send_sem, recv_sem, own_sem):
    _, _, lat, fld = position()
    me = lat * 4 + fld

    @pl.when(to != me)
    def _():
        pltpu.make_async_remote_copy(
            src_ref=source, dst_ref=target, send_sem=send_sem, recv_sem=recv_sem,
            device_id=(to // 4, lax.rem(to, 4)), device_id_type=MESH,
        ).start()

    @pl.when(to == me)
    def _():
        pltpu.make_async_copy(source, target, own_sem).start()


def wait_all(one, others, send_sem, recv_sem, own_sem):
    _, _, lat, fld = position()
    pltpu.make_async_copy(one, one, own_sem).wait()
    pltpu.make_async_remote_copy(
        src_ref=others, dst_ref=others, send_sem=send_sem, recv_sem=recv_sem,
        device_id=(lat, fld), device_id_type=MESH,
    ).wait()


def lanes(rows=16):
    return lax.broadcasted_iota(jnp.int32, (rows, 128), 1)


def aligned(start, size, unit=16):
    return pl.ds(pl.multiple_of(start, unit), size)


def swap_blocks(parts):
    block = lanes() // 16
    turned = [p if i == 0 else pltpu.roll(p, 16 * i, 1) for i, p in enumerate(parts)]
    row = [turned[(-i) % 8] for i in range(8)]
    for bit in (1, 2, 4):
        mask = (block & bit) != 0
        row = [jnp.where(mask, row[(i - bit) % 8], row[i]) for i in range(8)]
    return [p if d == 0 else pltpu.roll(p, 128 - 16 * d, 1) for d, p in enumerate(row)]


def spread_waves(slots_ref, waves):
    lane = lanes(GROUPS)
    group = lax.broadcasted_iota(jnp.int32, (GROUPS, 128), 0)
    flat = (8 * group + lane // 16) * 6 + jnp.minimum(lax.rem(lane, 16), 11) // 2
    at = lax.rem(flat, 128)
    total = jnp.zeros((GROUPS, 128), jnp.int32)
    for r in range(6):
        row = jnp.broadcast_to(slots_ref[r : r + 1], (GROUPS, 128))
        found = jnp.take_along_axis(row, at, axis=1, mode="promise_in_bounds")
        total = jnp.where(flat // 128 == r, found, total)
    waves[...] = total


def as_column(row):
    return jnp.broadcast_to(row, (128, 128)).T


def spread_modes(modes_ref, line, modes):
    line[...] = jnp.zeros((8, 128), F32)
    line[0:1, 0:80] = modes_ref[...].astype(F32)
    modes[...] = as_column(line[0:1])[0:80].astype(jnp.int32)


def fill_trig(waves, trig):
    column = lax.rem(lanes(TRIG_ROWS), 16)
    row = lax.broadcasted_iota(jnp.int32, (TRIG_ROWS, 128), 0)
    first = row < ROW_A
    factor = jnp.where(
        first, 192 * row, jnp.where(row < ROW_A + ROW_B, 16 * (row - ROW_A), row - ROW_A - ROW_B)
    )
    turn = jnp.where(first & (lax.rem(column, 2) == 1), LON // 4, 0)
    scale = jnp.where(first, jnp.where(column < 12, 1.0 / math.sqrt(LON), 0.0), 1.0)

    def one(group, carry):
        index = lax.rem(factor * waves[pl.ds(group, 1)] + turn, LON)
        radians = index.astype(F32) * (2.0 * math.pi / LON)
        trig[0, group] = jnp.cos(radians) * scale
        trig[1, group] = jnp.sin(radians) * scale
        return carry

    lax.fori_loop(0, GROUPS, one, 0)


def make_table(trig, group, half, uv, table):
    low = ROW_A + ROW_B
    cos_c = trig[0, group, low : low + ROW_C]
    sin_c = trig[1, group, low : low + ROW_C]
    for b in range(ROW_B):
        cb = trig[0, group, ROW_A + b : ROW_A + b + 1]
        sb = trig[1, group, ROW_A + b : ROW_A + b + 1]
        uv[0, 16 * b : 16 * b + 16] = cb * cos_c - sb * sin_c
        uv[1, 16 * b : 16 * b + 16] = sb * cos_c + cb * sin_c

    def rows(a, carry):
        ca, sa = trig[0, group, pl.ds(a, 1)], trig[1, group, pl.ds(a, 1)]
        table[aligned(192 * a, 192), 128 * half : 128 * half + 128] = (
            ca * uv[0] - sa * uv[1]
        ).astype(BF16)
        return carry

    lax.fori_loop(0, ROW_A, rows, 0)


def forward_kernel(
    grid_ref, slots_ref, modes_ref, recv_ref, angles_ref,
    waves, line, modes, trig, uv, table, result, outbox,
    send_sem, recv_sem, own_sem, table_sem,
):
    greet()
    lane16 = lax.rem(lanes(), 16)
    spread_waves(slots_ref, waves)
    spread_modes(modes_ref, line, modes)
    fill_trig(waves, trig)

    def step_body(step, carry):
        groups = (group_at(2 * step), group_at(2 * step + 1))
        for half in range(2):
            make_table(trig, groups[half], half, uv, table)
        copies = [
            pltpu.make_async_copy(
                table.at[:, pl.ds(128 * half, 128)],
                angles_ref.at[:, aligned(groups[half] * 128, 128, 128)],
                table_sem.at[half],
            )
            for half in range(2)
        ]
        for copy in copies:
            copy.start()
        result[...] = jnp.dot(grid_ref[...], table[...], preferred_element_type=F32)
        for half in range(2):
            wave = waves[pl.ds(groups[half], 1)]

            def swapped(q):
                keep = wave < modes[16 * q : 16 * q + 16]
                return swap_blocks([
                    jnp.where(
                        keep,
                        result[80 * f + 16 * q : 80 * f + 16 * q + 16, 128 * half : 128 * half + 128],
                        0.0,
                    )
                    for f in range(8)
                ])

            last = swapped(4)
            for q in range(4):
                for d, part in enumerate(swapped(q)):
                    if q < 3:
                        part = jnp.where(lane16 >= 12, pltpu.roll(last[d], 12 - 4 * q, 1), part)
                    outbox[groups[half] * 8 + d, 16 * q : 16 * q + 16] = part.astype(BF16)
        for copy in copies:
            copy.wait()

        @pl.when(step == 0)
        def _():
            greeted()

        _, _, lat, fld = position()
        landing = recv_ref.at[aligned(80 * lat, 64), aligned(128 * fld, 128, 128)]
        for half in range(2):
            def send(n, carry):
                to = groups[half] * 8 + n
                send_one(to, outbox.at[to], landing, send_sem, recv_sem, own_sem)
                return carry

            lax.fori_loop(0, 8, send, 0)
        return carry

    lax.fori_loop(0, GROUPS // 2, step_body, 0)
    wait_all(
        outbox.at[0], recv_ref.at[pl.ds(0, 2032)], send_sem, recv_sem, own_sem
    )


def unpack_last(read):
    lane16 = lax.rem(lanes(), 16)
    last = jnp.zeros((16, 128), F32)
    for c in range(3):
        piece = pltpu.roll(read(c).astype(F32), 128 - (12 - 4 * c), 1)
        last = jnp.where((lane16 >= 4 * c) & (lane16 < 4 * c + 4), piece, last)
    return last


def flip_matrix(size):
    row = lax.broadcasted_iota(jnp.int32, (size, size), 0)
    col = lax.broadcasted_iota(jnp.int32, (size, size), 1)
    return jnp.where(row + col == size - 1, 1.0, 0.0).astype(BF16)


def fill_picks(pick, place):
    def rows_of(slot, carry):
        row = lax.broadcasted_iota(jnp.int32, (64, 512), 0)
        col = lax.broadcasted_iota(jnp.int32, (64, 512), 1)
        lane = 16 * lax.rem(row, 32) + row // 32 + 2 * slot
        pick[aligned(64 * slot, 64)] = jnp.where(col == lane, 1.0, 0.0).astype(BF16)
        return carry

    lax.fori_loop(0, 6, rows_of, 0)

    def lanes_of(chunk, carry):
        row = lax.broadcasted_iota(jnp.int32, (64, 384), 0)
        col = lax.broadcasted_iota(jnp.int32, (64, 384), 1)
        block, inner = 4 * chunk + row // 16, lax.rem(row, 16)
        lane = (inner // 2) * 64 + lax.rem(inner, 2) * 32 + block
        place[aligned(64 * chunk, 64)] = jnp.where(
            (col == lane) & (inner < 12), 1.0, 0.0
        ).astype(BF16)
        return carry

    lax.fori_loop(0, 8, lanes_of, 0)


def middle_kernel(
    slots_ref, arrived_ref, tables_ref, weight_ref, rate_ref, recv_ref, spec_ref,
    wide, tables, even, odd, north, south, pick, place, line, rates, coeff, spec_box,
    send_sem, recv_sem, own_sem, spec_send, spec_recv, spec_own, wide_sem, table_sem,
):
    z, x, lat, fld = position()
    me = lat * 4 + fld
    load = pltpu.make_async_copy(arrived_ref, wide, wide_sem)
    load.start()
    table_loads = [
        pltpu.make_async_copy(tables_ref.at[s], tables.at[s], table_sem.at[s]) for s in range(6)
    ]
    for copy in table_loads:
        copy.start()
    greet()
    fill_picks(pick, place)
    line[...] = jnp.zeros((8, 128), F32)
    line[0:1, 0:32] = rate_ref[...]
    rates[...] = as_column(line[0:1])[0:32]
    load.wait()

    def unpack(n, carry):
        done = []
        for i in range(4):
            at = 80 * (4 * n + i)
            for k in range(4):
                cols = slice(128 * k, 128 * k + 128)
                last = unpack_last(lambda c: wide[aligned(at + 16 * c, 16), cols])
                done.append((at, cols, last.astype(BF16)))
        for at, cols, last in done:
            wide[aligned(at + 64, 16), cols] = last
        return carry

    lax.fori_loop(0, 8, unpack, 0)
    flip = flip_matrix(256)
    for b in range(5):
        up = wide[256 * b : 256 * b + 256].astype(F32)
        low = 1280 + 256 * (4 - b)
        down = jnp.dot(flip, wide[low : low + 256], preferred_element_type=F32)
        weight = jnp.concatenate(
            [as_column(weight_ref[2 * b + u : 2 * b + u + 1])[:, 0:1] for u in range(2)], 0
        )
        for target, value in ((even, up + down), (odd, up - down)):
            target[:, 256 * b : 256 * b + 256] = lax.dot_general(
                pick[...], (value * weight).astype(BF16), NT, preferred_element_type=F32
            ).astype(BF16)

    col = lax.broadcasted_iota(jnp.int32, (32, 384), 1)
    for slot in range(6):
        table_loads[slot].wait()
        wave = slots_ref[me * 6 + slot]
        for parity, source in enumerate((even, odd)):
            cols = slice(384 * parity, 384 * parity + 384)
            raw = jnp.dot(
                source[64 * slot : 64 * slot + 64], tables[slot, :, cols],
                preferred_element_type=F32,
            )
            degree = wave + 2 * col + parity
            ratio = (degree * (degree + 1)).astype(F32) / float(LMAX * (LMAX + 1))
            square = ratio * ratio
            factor = 1.0 / (1.0 + rates[:, 0:1] * (square * square))
            factor = jnp.where(degree <= LMAX, factor, 0.0)
            value = raw * jnp.concatenate([factor, factor], 0)
            for r in range(2):
                for k in range(4):
                    low = 32 * r + 8 * k
                    spec_box[slot, r, k, :, cols] = value[low : low + 8].astype(BF16)
            coeff[slot, :, cols] = value.astype(BF16)
        if slot == 0:
            greeted()
        for shift in range(4):
            to = lax.rem(fld + shift, 4)
            source, target = spec_box.at[slot, :, to], spec_ref.at[fld, slot]
            if shift:
                pltpu.make_async_remote_copy(
                    src_ref=source, dst_ref=target, send_sem=spec_send, recv_sem=spec_recv,
                    device_id=(lat, to), device_id_type=MESH,
                ).start()
            else:
                pltpu.make_async_copy(source, target, spec_own).start()

    turn = flip_matrix(320)
    lane16 = lax.rem(lanes(), 16)

    def part_of(step, carry):
        b = lax.rem(step + 2 * lax.rem(z, 2) + x // 2, 4)
        for slot in range(6):
            sums = [
                lax.dot_general(
                    tables[slot, aligned(320 * b, 320, 64), 384 * p : 384 * p + 384],
                    coeff[slot, :, 384 * p : 384 * p + 384],
                    NT,
                    preferred_element_type=F32,
                )
                for p in range(2)
            ]
            north[:, 64 * slot : 64 * slot + 64] = (sums[0] + sums[1]).astype(BF16)
            south[:, 64 * slot : 64 * slot + 64] = (sums[0] - sums[1]).astype(BF16)
        wide[aligned(320 * b, 320, 64)] = lax.dot_general(
            north[...], place[...], NT, preferred_element_type=F32
        ).astype(BF16)
        mirrored = jnp.dot(turn, south[...], preferred_element_type=F32).astype(BF16)
        wide[aligned(1280 + 320 * (3 - b), 320, 64)] = lax.dot_general(
            mirrored, place[...], NT, preferred_element_type=F32
        ).astype(BF16)

        def pack(n, carry):
            done = []
            for i in (4 * b + n, 31 - 4 * b - n):
                at = 80 * i
                for k in range(4):
                    cols = slice(128 * k, 128 * k + 128)
                    last = wide[aligned(at + 64, 16), cols].astype(F32)
                    for q in range(3):
                        rows = aligned(at + 16 * q, 16)
                        moved = pltpu.roll(last, 12 - 4 * q, 1)
                        part = jnp.where(lane16 >= 12, moved, wide[rows, cols].astype(F32))
                        done.append((rows, cols, part.astype(BF16)))
            for rows, cols, part in done:
                wide[rows, cols] = part
            return carry

        lax.fori_loop(0, 4, pack, 0)

        def send(n, carry):
            for i in (4 * b + n, 31 - 4 * b - n):
                for k in range(4):
                    send_one(
                        i * 4 + k, wide.at[aligned(80 * i, 64), 128 * k : 128 * k + 128],
                        recv_ref.at[me], send_sem, recv_sem, own_sem,
                    )
            return carry

        lax.fori_loop(0, 4, send, 0)
        return carry

    lax.fori_loop(0, 4, part_of, 0)
    pltpu.make_async_copy(spec_ref.at[0], spec_ref.at[0], spec_own).wait()
    pltpu.make_async_remote_copy(
        src_ref=spec_ref.at[pl.ds(0, 3)], dst_ref=spec_ref.at[pl.ds(0, 3)],
        send_sem=spec_send, recv_sem=spec_recv, device_id=(lat, fld), device_id_type=MESH,
    ).wait()
    wait_all(recv_ref.at[0], recv_ref.at[pl.ds(0, 127)], send_sem, recv_sem, own_sem)


def backward_kernel(inbox, angles_ref, slots_ref, modes_ref, out_ref, waves, line, modes, spread):
    @pl.when(pl.program_id(0) == 0)
    def _():
        spread_waves(slots_ref, waves)
        spread_modes(modes_ref, line, modes)

        def gather(group, carry):
            wave = waves[pl.ds(group, 1)]
            cols = aligned(128 * group, 128, 128)

            for q in range(5):
                keep = wave < modes[16 * q : 16 * q + 16]
                if q < 4:
                    parts = [inbox[group * 8 + d, 16 * q : 16 * q + 16].astype(F32) for d in range(8)]
                else:
                    parts = [
                        unpack_last(lambda c: inbox[group * 8 + d, 16 * c : 16 * c + 16])
                        for d in range(8)
                    ]
                for f, part in enumerate(swap_blocks(parts)):
                    spread[80 * f + 16 * q : 80 * f + 16 * q + 16, cols] = jnp.where(
                        keep, 2.0 * part, 0.0
                    ).astype(BF16)
            return carry

        lax.fori_loop(0, GROUPS, gather, 0)

    out_ref[...] = lax.dot_general(spread[...], angles_ref[...], NT, preferred_element_type=F32)


VMEM = pl.BlockSpec(memory_space=pltpu.VMEM)
SMEM = pl.BlockSpec(memory_space=pltpu.SMEM)
ANY = pl.BlockSpec(memory_space=pl.ANY)
INBOX = jax.ShapeDtypeStruct((128, 64, 128), BF16)
LIMIT = 60 * 1024 * 1024


def whole(shape):
    return pl.BlockSpec(shape, lambda i: (0,) * len(shape))


def body(grid_in, legendre, wave_slot, lat_modes, gauss_weight, diffusion):
    grid_rows = grid_in.reshape(640, LON)
    modes = lat_modes.reshape(1, 80)
    slots = wave_slot.reshape(6, 128)

    arrived, angles = pl.pallas_call(
        forward_kernel,
        name="forward",
        out_shape=(
            jax.ShapeDtypeStruct((2560, 512), BF16),
            jax.ShapeDtypeStruct((LON, 2048), BF16),
        ),
        in_specs=[VMEM] * 3,
        out_specs=(ANY, ANY),
        scratch_shapes=[
            pltpu.VMEM((GROUPS, 128), jnp.int32),
            pltpu.VMEM((8, 128), F32),
            pltpu.VMEM((80, 128), jnp.int32),
            pltpu.VMEM((2, GROUPS, TRIG_ROWS, 128), F32),
            pltpu.VMEM((2, 192, 128), F32),
            pltpu.VMEM((LON, 256), BF16),
            pltpu.VMEM((640, 256), F32),
            pltpu.VMEM((128, 64, 128), BF16),
            pltpu.SemaphoreType.DMA,
            pltpu.SemaphoreType.DMA,
            pltpu.SemaphoreType.DMA,
            pltpu.SemaphoreType.DMA((2,)),
        ],
        compiler_params=pltpu.CompilerParams(
            collective_id=0, has_side_effects=True, vmem_limit_bytes=LIMIT
        ),
    )(grid_rows, slots, modes)

    returned, spectra = pl.pallas_call(
        middle_kernel,
        name="middle",
        out_shape=(INBOX, jax.ShapeDtypeStruct((4, 6, 2, 8, 768), BF16)),
        in_specs=[SMEM, ANY, ANY, VMEM, VMEM],
        out_specs=(ANY, ANY),
        scratch_shapes=[
            pltpu.VMEM((2560, 512), BF16),
            pltpu.VMEM((6, 1280, 768), BF16),
            pltpu.VMEM((384, 1280), BF16),
            pltpu.VMEM((384, 1280), BF16),
            pltpu.VMEM((320, 384), BF16),
            pltpu.VMEM((320, 384), BF16),
            pltpu.VMEM((384, 512), BF16),
            pltpu.VMEM((512, 384), BF16),
            pltpu.VMEM((8, 128), F32),
            pltpu.VMEM((32, 128), F32),
            pltpu.VMEM((6, 64, 768), BF16),
            pltpu.VMEM((6, 2, 4, 8, 768), BF16),
        ]
        + [pltpu.SemaphoreType.DMA] * 7
        + [pltpu.SemaphoreType.DMA((6,))],
        compiler_params=pltpu.CompilerParams(
            collective_id=1, has_side_effects=True, vmem_limit_bytes=LIMIT
        ),
    )(wave_slot, arrived, legendre, gauss_weight.reshape(10, 128), diffusion.reshape(1, 32))

    grid_out = pl.pallas_call(
        backward_kernel,
        name="backward",
        grid=(7,),
        out_shape=jax.ShapeDtypeStruct((640, LON), F32),
        in_specs=[
            whole((128, 64, 128)),
            pl.BlockSpec((384, 2048), lambda i: (i, 0)),
            whole((6, 128)),
            whole((1, 80)),
        ],
        out_specs=pl.BlockSpec((640, 384), lambda i: (0, i)),
        scratch_shapes=[
            pltpu.VMEM((GROUPS, 128), jnp.int32),
            pltpu.VMEM((8, 128), F32),
            pltpu.VMEM((80, 128), jnp.int32),
            pltpu.VMEM((640, 2048), BF16),
        ],
        compiler_params=pltpu.CompilerParams(vmem_limit_bytes=LIMIT),
    )(returned, angles, slots, modes)

    spectra = spectra.transpose(2, 0, 1, 3, 4).reshape(2, 24, 8, 768).astype(F32)
    return (grid_out.reshape(8, 80, LON), spectra)


def solution(mesh):
    return jax.shard_map(
        body,
        mesh=mesh,
        in_specs=(P("fld", "lat", None), P(("lat", "fld"), None, None), P(), P("lat"), P(), P()),
        out_specs=(P("fld", "lat", None), P(None, "lat", "fld", None)),
        check_vma=False,
    )
```

```python
import functools
import math

import jax
import jax.numpy as jnp
from jax import lax
from jax.experimental import pallas as pl
from jax.experimental.pallas import tpu as pltpu
from jax.sharding import PartitionSpec as P

LMAX = 1279
MESH = pl.DeviceIdType.MESH
F32 = jnp.float32
BF16 = jnp.bfloat16

LON = 2688
ROW_A, ROW_B, ROW_C = 14, 12, 16
GROUPS = 16
TRIG_ROWS = 48
NT = (((1,), (1,)), ((), ()))

ORDER = (
    (1, 1), (3, 3), (1, 2), (3, 0), (2, 1), (0, 3), (1, 3), (3, 1),
    (3, 2), (1, 0), (2, 3), (0, 1), (2, 0), (0, 2), (2, 2), (0, 0),
)


def position():
    lat = lax.axis_index("lat")
    return lat // 8, lax.rem(lat // 2, 4), lat, lax.axis_index("fld")


def group_at(step):
    z, x, _, _ = position()
    dz, dx = jnp.int32(0), jnp.int32(0)
    for n, (a, b) in enumerate(ORDER):
        dz = jnp.where(step == n, a, dz)
        dx = jnp.where(step == n, b, dx)
    return lax.rem(z + dz, 4) * 4 + lax.rem(x + dx, 4)


def greet():
    barrier = pltpu.get_barrier_semaphore()
    _, _, lat, fld = position()
    me = lat * 4 + fld

    def signal(n, carry):
        peer = lax.rem(me + n, 128)
        pl.semaphore_signal(
            barrier, inc=1, device_id=(peer // 4, lax.rem(peer, 4)), device_id_type=MESH
        )
        return carry

    lax.fori_loop(1, 128, signal, 0)


def greeted():
    pl.semaphore_wait(pltpu.get_barrier_semaphore(), 127)


def send_one(to, source, target, send_sem, recv_sem, own_sem):
    _, _, lat, fld = position()
    me = lat * 4 + fld

    @pl.when(to != me)
    def _():
        pltpu.make_async_remote_copy(
            src_ref=source, dst_ref=target, send_sem=send_sem, recv_sem=recv_sem,
            device_id=(to // 4, lax.rem(to, 4)), device_id_type=MESH,
        ).start()

    @pl.when(to == me)
    def _():
        pltpu.make_async_copy(source, target, own_sem).start()


def wait_all(one, others, send_sem, recv_sem, own_sem):
    _, _, lat, fld = position()
    pltpu.make_async_copy(one, one, own_sem).wait()
    pltpu.make_async_remote_copy(
        src_ref=others, dst_ref=others, send_sem=send_sem, recv_sem=recv_sem,
        device_id=(lat, fld), device_id_type=MESH,
    ).wait()


def lanes(rows=16):
    return lax.broadcasted_iota(jnp.int32, (rows, 128), 1)


def aligned(start, size, unit=16):
    return pl.ds(pl.multiple_of(start, unit), size)


def swap_blocks(parts):
    block = lanes() // 16
    turned = [p if i == 0 else pltpu.roll(p, 16 * i, 1) for i, p in enumerate(parts)]
    row = [turned[(-i) % 8] for i in range(8)]
    for bit in (1, 2, 4):
        mask = (block & bit) != 0
        row = [jnp.where(mask, row[(i - bit) % 8], row[i]) for i in range(8)]
    return [p if d == 0 else pltpu.roll(p, 128 - 16 * d, 1) for d, p in enumerate(row)]


def spread_waves(slots_ref, waves):
    lane = lanes(GROUPS)
    group = lax.broadcasted_iota(jnp.int32, (GROUPS, 128), 0)
    flat = (8 * group + lane // 16) * 6 + jnp.minimum(lax.rem(lane, 16), 11) // 2
    at = lax.rem(flat, 128)
    total = jnp.zeros((GROUPS, 128), jnp.int32)
    for r in range(6):
        row = jnp.broadcast_to(slots_ref[r : r + 1], (GROUPS, 128))
        found = jnp.take_along_axis(row, at, axis=1, mode="promise_in_bounds")
        total = jnp.where(flat // 128 == r, found, total)
    waves[...] = total


def as_column(row):
    return jnp.broadcast_to(row, (128, 128)).T


def spread_modes(modes_ref, line, modes):
    line[...] = jnp.zeros((8, 128), F32)
    line[0:1, 0:80] = modes_ref[...].astype(F32)
    modes[...] = as_column(line[0:1])[0:80].astype(jnp.int32)


def fill_trig(waves, trig):
    column = lax.rem(lanes(TRIG_ROWS), 16)
    row = lax.broadcasted_iota(jnp.int32, (TRIG_ROWS, 128), 0)
    first = row < ROW_A
    factor = jnp.where(
        first, 192 * row, jnp.where(row < ROW_A + ROW_B, 16 * (row - ROW_A), row - ROW_A - ROW_B)
    )
    turn = jnp.where(first & (lax.rem(column, 2) == 1), LON // 4, 0)
    scale = jnp.where(first, jnp.where(column < 12, 1.0 / math.sqrt(LON), 0.0), 1.0)

    def one(group, carry):
        index = lax.rem(factor * waves[pl.ds(group, 1)] + turn, LON)
        radians = index.astype(F32) * (2.0 * math.pi / LON)
        trig[0, group] = jnp.cos(radians) * scale
        trig[1, group] = jnp.sin(radians) * scale
        return carry

    lax.fori_loop(0, GROUPS, one, 0)


def make_table(trig, group, half, uv, table):
    low = ROW_A + ROW_B
    cos_c = trig[0, group, low : low + ROW_C]
    sin_c = trig[1, group, low : low + ROW_C]
    for b in range(ROW_B):
        cb = trig[0, group, ROW_A + b : ROW_A + b + 1]
        sb = trig[1, group, ROW_A + b : ROW_A + b + 1]
        uv[0, 16 * b : 16 * b + 16] = cb * cos_c - sb * sin_c
        uv[1, 16 * b : 16 * b + 16] = sb * cos_c + cb * sin_c

    def rows(a, carry):
        ca, sa = trig[0, group, pl.ds(a, 1)], trig[1, group, pl.ds(a, 1)]
        table[aligned(192 * a, 192), 128 * half : 128 * half + 128] = (
            ca * uv[0] - sa * uv[1]
        ).astype(BF16)
        return carry

    lax.fori_loop(0, ROW_A, rows, 0)


def forward_kernel(
    grid_ref, slots_ref, modes_ref, recv_ref, angles_ref,
    waves, line, modes, trig, uv, table, result, outbox,
    send_sem, recv_sem, own_sem, table_sem,
):
    greet()
    lane16 = lax.rem(lanes(), 16)
    spread_waves(slots_ref, waves)
    spread_modes(modes_ref, line, modes)
    fill_trig(waves, trig)

    def step_body(step, carry):
        groups = (group_at(2 * step), group_at(2 * step + 1))
        for half in range(2):
            make_table(trig, groups[half], half, uv, table)
        copies = [
            pltpu.make_async_copy(
                table.at[:, pl.ds(128 * half, 128)],
                angles_ref.at[:, aligned(groups[half] * 128, 128, 128)],
                table_sem.at[half],
            )
            for half in range(2)
        ]
        for copy in copies:
            copy.start()
        result[...] = jnp.dot(grid_ref[...], table[...], preferred_element_type=F32)
        for half in range(2):
            wave = waves[pl.ds(groups[half], 1)]

            def swapped(q):
                keep = wave < modes[16 * q : 16 * q + 16]
                return swap_blocks([
                    jnp.where(
                        keep,
                        result[80 * f + 16 * q : 80 * f + 16 * q + 16, 128 * half : 128 * half + 128],
                        0.0,
                    )
                    for f in range(8)
                ])

            last = swapped(4)
            for q in range(4):
                for d, part in enumerate(swapped(q)):
                    if q < 3:
                        part = jnp.where(lane16 >= 12, pltpu.roll(last[d], 12 - 4 * q, 1), part)
                    outbox[groups[half] * 8 + d, 16 * q : 16 * q + 16] = part.astype(BF16)
        for copy in copies:
            copy.wait()

        @pl.when(step == 0)
        def _():
            greeted()

        _, _, lat, fld = position()
        landing = recv_ref.at[aligned(80 * lat, 64), aligned(128 * fld, 128, 128)]
        for half in range(2):
            def send(n, carry):
                to = groups[half] * 8 + n
                send_one(to, outbox.at[to], landing, send_sem, recv_sem, own_sem)
                return carry

            lax.fori_loop(0, 8, send, 0)
        return carry

    lax.fori_loop(0, GROUPS // 2, step_body, 0)
    wait_all(
        outbox.at[0], recv_ref.at[pl.ds(0, 2032)], send_sem, recv_sem, own_sem
    )


def unpack_last(read):
    lane16 = lax.rem(lanes(), 16)
    last = jnp.zeros((16, 128), F32)
    for c in range(3):
        piece = pltpu.roll(read(c).astype(F32), 128 - (12 - 4 * c), 1)
        last = jnp.where((lane16 >= 4 * c) & (lane16 < 4 * c + 4), piece, last)
    return last


def flip_matrix(size):
    row = lax.broadcasted_iota(jnp.int32, (size, size), 0)
    col = lax.broadcasted_iota(jnp.int32, (size, size), 1)
    return jnp.where(row + col == size - 1, 1.0, 0.0).astype(BF16)


def fill_picks(pick, place):
    def rows_of(slot, carry):
        row = lax.broadcasted_iota(jnp.int32, (64, 512), 0)
        col = lax.broadcasted_iota(jnp.int32, (64, 512), 1)
        lane = 16 * lax.rem(row, 32) + row // 32 + 2 * slot
        pick[aligned(64 * slot, 64)] = jnp.where(col == lane, 1.0, 0.0).astype(BF16)
        return carry

    lax.fori_loop(0, 6, rows_of, 0)

    def lanes_of(chunk, carry):
        row = lax.broadcasted_iota(jnp.int32, (64, 384), 0)
        col = lax.broadcasted_iota(jnp.int32, (64, 384), 1)
        block, inner = 4 * chunk + row // 16, lax.rem(row, 16)
        lane = (inner // 2) * 64 + lax.rem(inner, 2) * 32 + block
        place[aligned(64 * chunk, 64)] = jnp.where(
            (col == lane) & (inner < 12), 1.0, 0.0
        ).astype(BF16)
        return carry

    lax.fori_loop(0, 8, lanes_of, 0)


def middle_kernel(
    slots_ref, arrived_ref, tables_ref, weight_ref, rate_ref, rows_ref, modes_ref, angles_ref,
    partial_ref, rest_ref, spec_ref,
    wide, tables, even, odd, north, south, pick, place, line, rates, coeff, spec_box,
    waves, modes, angles, total, inbox, spread,
    send_sem, own_sem, spec_send, spec_recv, spec_own, wide_sem, angle_sem, out_sem, rest_sem,
    recv_sem, table_sem,
):
    z, x, lat, fld = position()
    me = lat * 4 + fld
    load = pltpu.make_async_copy(arrived_ref, wide, wide_sem)
    load.start()
    table_loads = [
        pltpu.make_async_copy(tables_ref.at[s], tables.at[s], table_sem.at[s]) for s in range(6)
    ]
    for copy in table_loads:
        copy.start()
    greet()
    fill_picks(pick, place)
    line[...] = jnp.zeros((8, 128), F32)
    line[0:1, 0:32] = rate_ref[...]
    rates[...] = as_column(line[0:1])[0:32]
    spread_waves(rows_ref, waves)
    spread_modes(modes_ref, line, modes)
    load.wait()

    def unpack(n, carry):
        done = []
        for i in range(4):
            at = 80 * (4 * n + i)
            for k in range(4):
                cols = slice(128 * k, 128 * k + 128)
                last = unpack_last(lambda c: wide[aligned(at + 16 * c, 16), cols])
                done.append((at, cols, last.astype(BF16)))
        for at, cols, last in done:
            wide[aligned(at + 64, 16), cols] = last
        return carry

    lax.fori_loop(0, 8, unpack, 0)
    flip = flip_matrix(256)
    for b in range(5):
        up = wide[256 * b : 256 * b + 256].astype(F32)
        low = 1280 + 256 * (4 - b)
        down = jnp.dot(flip, wide[low : low + 256], preferred_element_type=F32)
        weight = jnp.concatenate(
            [as_column(weight_ref[2 * b + u : 2 * b + u + 1])[:, 0:1] for u in range(2)], 0
        )
        for target, value in ((even, up + down), (odd, up - down)):
            target[:, 256 * b : 256 * b + 256] = lax.dot_general(
                pick[...], (value * weight).astype(BF16), NT, preferred_element_type=F32
            ).astype(BF16)

    col = lax.broadcasted_iota(jnp.int32, (32, 384), 1)
    for slot in range(6):
        table_loads[slot].wait()
        wave = slots_ref[me * 6 + slot]
        for parity, source in enumerate((even, odd)):
            cols = slice(384 * parity, 384 * parity + 384)
            raw = jnp.dot(
                source[64 * slot : 64 * slot + 64], tables[slot, :, cols],
                preferred_element_type=F32,
            )
            degree = wave + 2 * col + parity
            ratio = (degree * (degree + 1)).astype(F32) / float(LMAX * (LMAX + 1))
            square = ratio * ratio
            factor = 1.0 / (1.0 + rates[:, 0:1] * (square * square))
            factor = jnp.where(degree <= LMAX, factor, 0.0)
            value = raw * jnp.concatenate([factor, factor], 0)
            for r in range(2):
                for k in range(4):
                    low = 32 * r + 8 * k
                    spec_box[slot, r, k, :, cols] = value[low : low + 8].astype(BF16)
            coeff[slot, :, cols] = value.astype(BF16)
        if slot == 0:
            greeted()
        if slot == 5:
            angle_load = pltpu.make_async_copy(angles_ref, angles, angle_sem)
            angle_load.start()
        for shift in range(4):
            to = lax.rem(fld + shift, 4)
            source, target = spec_box.at[slot, :, to], spec_ref.at[fld, slot]
            if shift:
                pltpu.make_async_remote_copy(
                    src_ref=source, dst_ref=target, send_sem=spec_send, recv_sem=spec_recv,
                    device_id=(lat, to), device_id_type=MESH,
                ).start()
            else:
                pltpu.make_async_copy(source, target, spec_own).start()

    mine = 2 * lax.rem(z, 2) + x // 2
    turn = flip_matrix(320)
    lane16 = lax.rem(lanes(), 16)

    def part_of(step, carry):
        b = lax.rem(step + mine, 4)
        for slot in range(6):
            sums = [
                lax.dot_general(
                    tables[slot, aligned(320 * b, 320, 64), 384 * p : 384 * p + 384],
                    coeff[slot, :, 384 * p : 384 * p + 384],
                    NT,
                    preferred_element_type=F32,
                )
                for p in range(2)
            ]
            north[:, 64 * slot : 64 * slot + 64] = (sums[0] + sums[1]).astype(BF16)
            south[:, 64 * slot : 64 * slot + 64] = (sums[0] - sums[1]).astype(BF16)
        wide[aligned(320 * b, 320, 64)] = lax.dot_general(
            north[...], place[...], NT, preferred_element_type=F32
        ).astype(BF16)
        mirrored = jnp.dot(turn, south[...], preferred_element_type=F32).astype(BF16)
        wide[aligned(1280 + 320 * (3 - b), 320, 64)] = lax.dot_general(
            mirrored, place[...], NT, preferred_element_type=F32
        ).astype(BF16)

        def pack(n, carry):
            done = []
            for i in (4 * b + n, 31 - 4 * b - n):
                at = 80 * i
                for k in range(4):
                    cols = slice(128 * k, 128 * k + 128)
                    last = wide[aligned(at + 64, 16), cols].astype(F32)
                    for q in range(3):
                        rows = aligned(at + 16 * q, 16)
                        moved = pltpu.roll(last, 12 - 4 * q, 1)
                        part = jnp.where(lane16 >= 12, moved, wide[rows, cols].astype(F32))
                        done.append((rows, cols, part.astype(BF16)))
            for rows, cols, part in done:
                wide[rows, cols] = part
            return carry

        lax.fori_loop(0, 4, pack, 0)

        def send(n, carry):
            for i in (4 * b + n, 31 - 4 * b - n):
                for k in range(4):
                    send_one(
                        i * 4 + k, wide.at[aligned(80 * i, 64), 128 * k : 128 * k + 128],
                        inbox.at[me], send_sem, recv_sem.at[mine], own_sem,
                    )
            return carry

        lax.fori_loop(0, 4, send, 0)
        return carry

    lax.fori_loop(0, 4, part_of, 0)
    angle_load.wait()
    here = jnp.where(lat < 16, lat // 4, (31 - lat) // 4)

    def arrived(count, kind):
        refs = inbox.at[pl.ds(0, count)]
        pltpu.make_async_remote_copy(
            src_ref=refs, dst_ref=refs, send_sem=send_sem, recv_sem=recv_sem.at[kind],
            device_id=(lat, fld), device_id_type=MESH,
        ).wait_recv()

    for stage in range(4):
        kind = lax.rem(here + 4 - stage, 4)

        @pl.when(kind == mine)
        def _():
            pltpu.make_async_copy(inbox.at[0], inbox.at[0], own_sem).wait()
            arrived(31, kind)

        @pl.when(kind != mine)
        def _():
            arrived(32, kind)

        first = (kind // 2) * 4 + 2 * lax.rem(kind, 2)

        def gather(n, carry):
            group = first + 8 * (n // 2) + lax.rem(n, 2)
            wave = waves[pl.ds(group, 1)]
            cols = aligned(128 * n, 128, 128)
            for q in range(5):
                keep = wave < modes[16 * q : 16 * q + 16]
                if q < 4:
                    parts = [inbox[group * 8 + d, 16 * q : 16 * q + 16].astype(F32) for d in range(8)]
                else:
                    parts = [
                        unpack_last(lambda c: inbox[group * 8 + d, 16 * c : 16 * c + 16])
                        for d in range(8)
                    ]
                for f, part in enumerate(swap_blocks(parts)):
                    spread[80 * f + 16 * q : 80 * f + 16 * q + 16, cols] = jnp.where(
                        keep, 2.0 * part, 0.0
                    ).astype(BF16)
            return carry

        lax.fori_loop(0, 4, gather, 0)
        if stage == 3:
            rest_copy = pltpu.make_async_copy(spread, rest_ref, rest_sem)
            rest_copy.start()
            break

        def add(n, carry):
            rows = aligned(384 * n, 384, 128)
            part = None
            for half in range(2):
                cols = aligned(128 * first + 1024 * half, 256, 256)
                term = lax.dot_general(
                    spread[:, 256 * half : 256 * half + 256], angles[rows, cols], NT,
                    preferred_element_type=F32,
                )
                part = term if part is None else part + term
            total[:, rows] = part if stage == 0 else total[:, rows] + part
            if stage == 2:
                pltpu.make_async_copy(total.at[:, rows], partial_ref.at[:, rows], out_sem).start()
            return carry

        lax.fori_loop(0, 7, add, 0)

    pltpu.make_async_copy(total, partial_ref, out_sem).wait()
    rest_copy.wait()
    pltpu.make_async_copy(spec_ref.at[0], spec_ref.at[0], spec_own).wait()
    pltpu.make_async_remote_copy(
        src_ref=spec_ref.at[pl.ds(0, 3)], dst_ref=spec_ref.at[pl.ds(0, 3)],
        send_sem=spec_send, recv_sem=spec_recv, device_id=(lat, fld), device_id_type=MESH,
    ).wait()
    others = inbox.at[pl.ds(0, 127)]
    pltpu.make_async_remote_copy(
        src_ref=others, dst_ref=others, send_sem=send_sem, recv_sem=recv_sem.at[0],
        device_id=(lat, fld), device_id_type=MESH,
    ).wait_send()


def finish_kernel(first_ref, rest_ref, low_ref, high_ref, partial_ref, out_ref):
    del first_ref
    out_ref[...] = (
        partial_ref[...]
        + lax.dot_general(rest_ref[:, 0:256], low_ref[...], NT, preferred_element_type=F32)
        + lax.dot_general(rest_ref[:, 256:512], high_ref[...], NT, preferred_element_type=F32)
    )


VMEM = pl.BlockSpec(memory_space=pltpu.VMEM)
SMEM = pl.BlockSpec(memory_space=pltpu.SMEM)
ANY = pl.BlockSpec(memory_space=pl.ANY)
LIMIT = 60 * 1024 * 1024


def body(grid_in, legendre, wave_slot, lat_modes, gauss_weight, diffusion):
    lat_index = lax.axis_index("lat")
    grid_rows = grid_in.reshape(640, LON)
    modes = lat_modes.reshape(1, 80)
    slots = wave_slot.reshape(6, 128)

    arrived, angles = pl.pallas_call(
        forward_kernel,
        name="forward",
        out_shape=(
            jax.ShapeDtypeStruct((2560, 512), BF16),
            jax.ShapeDtypeStruct((LON, 2048), BF16),
        ),
        in_specs=[VMEM] * 3,
        out_specs=(ANY, ANY),
        scratch_shapes=[
            pltpu.VMEM((GROUPS, 128), jnp.int32),
            pltpu.VMEM((8, 128), F32),
            pltpu.VMEM((80, 128), jnp.int32),
            pltpu.VMEM((2, GROUPS, TRIG_ROWS, 128), F32),
            pltpu.VMEM((2, 192, 128), F32),
            pltpu.VMEM((LON, 256), BF16),
            pltpu.VMEM((640, 256), F32),
            pltpu.VMEM((128, 64, 128), BF16),
            pltpu.SemaphoreType.DMA,
            pltpu.SemaphoreType.DMA,
            pltpu.SemaphoreType.DMA,
            pltpu.SemaphoreType.DMA((2,)),
        ],
        compiler_params=pltpu.CompilerParams(
            collective_id=0, has_side_effects=True, vmem_limit_bytes=LIMIT
        ),
    )(grid_rows, slots, modes)

    partial, rest, spectra = pl.pallas_call(
        middle_kernel,
        name="middle",
        out_shape=(
            jax.ShapeDtypeStruct((640, LON), F32),
            jax.ShapeDtypeStruct((640, 512), BF16),
            jax.ShapeDtypeStruct((4, 6, 2, 8, 768), BF16),
        ),
        in_specs=[SMEM, ANY, ANY, VMEM, VMEM, VMEM, VMEM, ANY],
        out_specs=(ANY, ANY, ANY),
        scratch_shapes=[
            pltpu.VMEM((2560, 512), BF16),
            pltpu.VMEM((6, 1280, 768), BF16),
            pltpu.VMEM((384, 1280), BF16),
            pltpu.VMEM((384, 1280), BF16),
            pltpu.VMEM((320, 384), BF16),
            pltpu.VMEM((320, 384), BF16),
            pltpu.VMEM((384, 512), BF16),
            pltpu.VMEM((512, 384), BF16),
            pltpu.VMEM((8, 128), F32),
            pltpu.VMEM((32, 128), F32),
            pltpu.VMEM((6, 64, 768), BF16),
            pltpu.VMEM((6, 2, 4, 8, 768), BF16),
            pltpu.VMEM((GROUPS, 128), jnp.int32),
            pltpu.VMEM((80, 128), jnp.int32),
            pltpu.VMEM((LON, 2048), BF16),
            pltpu.VMEM((640, LON), F32),
            pltpu.VMEM((128, 64, 128), BF16),
            pltpu.VMEM((640, 512), BF16),
        ]
        + [pltpu.SemaphoreType.DMA] * 9
        + [pltpu.SemaphoreType.DMA((4,)), pltpu.SemaphoreType.DMA((6,))],
        compiler_params=pltpu.CompilerParams(
            collective_id=1, has_side_effects=True, vmem_limit_bytes=LIMIT
        ),
    )(
        wave_slot, arrived, legendre, gauss_weight.reshape(10, 128), diffusion.reshape(1, 32),
        slots, modes, angles,
    )

    last = lax.rem(jnp.where(lat_index < 16, lat_index // 4, (31 - lat_index) // 4) + 1, 4)
    first = ((last // 2) * 2 + lax.rem(last, 2)).reshape(1)
    grid_out = pl.pallas_call(
        finish_kernel,
        name="finish",
        grid_spec=pltpu.PrefetchScalarGridSpec(
            num_scalar_prefetch=1,
            grid=(7,),
            in_specs=[
                pl.BlockSpec((640, 512), lambda i, c: (0, 0)),
                pl.BlockSpec((384, 256), lambda i, c: (i, c[0])),
                pl.BlockSpec((384, 256), lambda i, c: (i, c[0] + 4)),
                pl.BlockSpec((640, 384), lambda i, c: (0, i)),
            ],
            out_specs=pl.BlockSpec((640, 384), lambda i, c: (0, i)),
        ),
        out_shape=jax.ShapeDtypeStruct((640, LON), F32),
        compiler_params=pltpu.CompilerParams(vmem_limit_bytes=LIMIT),
    )(first, rest, angles, angles, partial)

    spectra = spectra.transpose(2, 0, 1, 3, 4).reshape(2, 24, 8, 768).astype(F32)
    return (grid_out.reshape(8, 80, LON), spectra)


def solution(mesh):
    return jax.shard_map(
        body,
        mesh=mesh,
        in_specs=(P("fld", "lat", None), P(("lat", "fld"), None, None), P(), P("lat"), P(), P()),
        out_specs=(P("fld", "lat", None), P(None, "lat", "fld", None)),
        check_vma=False,
    )
```

```python
import functools
import math

import jax
import jax.numpy as jnp
from jax import lax
from jax.experimental import pallas as pl
from jax.experimental.pallas import tpu as pltpu
from jax.sharding import PartitionSpec as P

LMAX = 1279
MESH = pl.DeviceIdType.MESH
F32 = jnp.float32
BF16 = jnp.bfloat16

LON = 2688
ROW_A, ROW_B, ROW_C = 14, 12, 16
GROUPS = 16
TRIG_ROWS = 48
NT = (((1,), (1,)), ((), ()))

ORDER = (
    (1, 1), (3, 3), (1, 2), (3, 0), (2, 1), (0, 3), (1, 3), (3, 1),
    (3, 2), (1, 0), (2, 3), (0, 1), (2, 0), (0, 2), (2, 2), (0, 0),
)


def position():
    lat = lax.axis_index("lat")
    return lat // 8, lax.rem(lat // 2, 4), lat, lax.axis_index("fld")


def group_at(step):
    z, x, _, _ = position()
    dz, dx = jnp.int32(0), jnp.int32(0)
    for n, (a, b) in enumerate(ORDER):
        dz = jnp.where(step == n, a, dz)
        dx = jnp.where(step == n, b, dx)
    return lax.rem(z + dz, 4) * 4 + lax.rem(x + dx, 4)


def greet():
    barrier = pltpu.get_barrier_semaphore()
    _, _, lat, fld = position()
    me = lat * 4 + fld

    def signal(n, carry):
        peer = lax.rem(me + n, 128)
        pl.semaphore_signal(
            barrier, inc=1, device_id=(peer // 4, lax.rem(peer, 4)), device_id_type=MESH
        )
        return carry

    lax.fori_loop(1, 128, signal, 0)


def greeted():
    pl.semaphore_wait(pltpu.get_barrier_semaphore(), 127)


def send_one(to, source, target, send_sem, recv_sem, own_sem):
    _, _, lat, fld = position()
    me = lat * 4 + fld

    @pl.when(to != me)
    def _():
        pltpu.make_async_remote_copy(
            src_ref=source, dst_ref=target, send_sem=send_sem, recv_sem=recv_sem,
            device_id=(to // 4, lax.rem(to, 4)), device_id_type=MESH,
        ).start()

    @pl.when(to == me)
    def _():
        pltpu.make_async_copy(source, target, own_sem).start()


def wait_all(one, others, send_sem, recv_sem, own_sem):
    _, _, lat, fld = position()
    pltpu.make_async_copy(one, one, own_sem).wait()
    pltpu.make_async_remote_copy(
        src_ref=others, dst_ref=others, send_sem=send_sem, recv_sem=recv_sem,
        device_id=(lat, fld), device_id_type=MESH,
    ).wait()


def lanes(rows=16):
    return lax.broadcasted_iota(jnp.int32, (rows, 128), 1)


def aligned(start, size, unit=16):
    return pl.ds(pl.multiple_of(start, unit), size)


def swap_blocks(parts):
    block = lanes() // 16
    turned = [p if i == 0 else pltpu.roll(p, 16 * i, 1) for i, p in enumerate(parts)]
    row = [turned[(-i) % 8] for i in range(8)]
    for bit in (1, 2, 4):
        mask = (block & bit) != 0
        row = [jnp.where(mask, row[(i - bit) % 8], row[i]) for i in range(8)]
    return [p if d == 0 else pltpu.roll(p, 128 - 16 * d, 1) for d, p in enumerate(row)]


def spread_waves(slots_ref, waves):
    lane = lanes(GROUPS)
    group = lax.broadcasted_iota(jnp.int32, (GROUPS, 128), 0)
    flat = (8 * group + lane // 16) * 6 + jnp.minimum(lax.rem(lane, 16), 11) // 2
    at = lax.rem(flat, 128)
    total = jnp.zeros((GROUPS, 128), jnp.int32)
    for r in range(6):
        row = jnp.broadcast_to(slots_ref[r : r + 1], (GROUPS, 128))
        found = jnp.take_along_axis(row, at, axis=1, mode="promise_in_bounds")
        total = jnp.where(flat // 128 == r, found, total)
    waves[...] = total


def as_column(row):
    return jnp.broadcast_to(row, (128, 128)).T


def spread_modes(modes_ref, line, modes):
    line[...] = jnp.zeros((8, 128), F32)
    line[0:1, 0:80] = modes_ref[...].astype(F32)
    modes[...] = as_column(line[0:1])[0:80].astype(jnp.int32)


def fill_trig(waves, trig):
    column = lax.rem(lanes(TRIG_ROWS), 16)
    row = lax.broadcasted_iota(jnp.int32, (TRIG_ROWS, 128), 0)
    first = row < ROW_A
    factor = jnp.where(
        first, 192 * row, jnp.where(row < ROW_A + ROW_B, 16 * (row - ROW_A), row - ROW_A - ROW_B)
    )
    turn = jnp.where(first & (lax.rem(column, 2) == 1), LON // 4, 0)
    scale = jnp.where(first, jnp.where(column < 12, 1.0 / math.sqrt(LON), 0.0), 1.0)

    def one(group, carry):
        index = lax.rem(factor * waves[pl.ds(group, 1)] + turn, LON)
        radians = index.astype(F32) * (2.0 * math.pi / LON)
        trig[0, group] = jnp.cos(radians) * scale
        trig[1, group] = jnp.sin(radians) * scale
        return carry

    lax.fori_loop(0, GROUPS, one, 0)


def make_table(trig, group, half, uv, table):
    low = ROW_A + ROW_B
    cos_c = trig[0, group, low : low + ROW_C]
    sin_c = trig[1, group, low : low + ROW_C]
    for b in range(ROW_B):
        cb = trig[0, group, ROW_A + b : ROW_A + b + 1]
        sb = trig[1, group, ROW_A + b : ROW_A + b + 1]
        uv[0, 16 * b : 16 * b + 16] = cb * cos_c - sb * sin_c
        uv[1, 16 * b : 16 * b + 16] = sb * cos_c + cb * sin_c

    def rows(a, carry):
        ca, sa = trig[0, group, pl.ds(a, 1)], trig[1, group, pl.ds(a, 1)]
        table[aligned(192 * a, 192), 128 * half : 128 * half + 128] = (
            ca * uv[0] - sa * uv[1]
        ).astype(BF16)
        return carry

    lax.fori_loop(0, ROW_A, rows, 0)


def forward_kernel(
    grid_ref, slots_ref, modes_ref, recv_ref, angles_ref,
    waves, line, modes, trig, uv, table, result, outbox,
    send_sem, recv_sem, own_sem, table_sem,
):
    greet()
    lane16 = lax.rem(lanes(), 16)
    spread_waves(slots_ref, waves)
    spread_modes(modes_ref, line, modes)
    fill_trig(waves, trig)

    def step_body(step, carry):
        groups = (group_at(2 * step), group_at(2 * step + 1))
        for half in range(2):
            make_table(trig, groups[half], half, uv, table)
        copies = [
            pltpu.make_async_copy(
                table.at[:, pl.ds(128 * half, 128)],
                angles_ref.at[:, aligned(groups[half] * 128, 128, 128)],
                table_sem.at[half],
            )
            for half in range(2)
        ]
        for copy in copies:
            copy.start()
        result[...] = jnp.dot(grid_ref[...], table[...], preferred_element_type=F32)
        for half in range(2):
            wave = waves[pl.ds(groups[half], 1)]

            def swapped(q):
                keep = wave < modes[16 * q : 16 * q + 16]
                return swap_blocks([
                    jnp.where(
                        keep,
                        result[80 * f + 16 * q : 80 * f + 16 * q + 16, 128 * half : 128 * half + 128],
                        0.0,
                    )
                    for f in range(8)
                ])

            last = swapped(4)
            for q in range(4):
                for d, part in enumerate(swapped(q)):
                    if q < 3:
                        part = jnp.where(lane16 >= 12, pltpu.roll(last[d], 12 - 4 * q, 1), part)
                    outbox[groups[half] * 8 + d, 16 * q : 16 * q + 16] = part.astype(BF16)
        for copy in copies:
            copy.wait()

        @pl.when(step == 0)
        def _():
            greeted()

        _, _, lat, fld = position()
        landing = recv_ref.at[aligned(80 * lat, 64), aligned(128 * fld, 128, 128)]
        for half in range(2):
            def send(n, carry):
                to = groups[half] * 8 + n
                send_one(to, outbox.at[to], landing, send_sem, recv_sem, own_sem)
                return carry

            lax.fori_loop(0, 8, send, 0)
        return carry

    lax.fori_loop(0, GROUPS // 2, step_body, 0)
    wait_all(
        outbox.at[0], recv_ref.at[pl.ds(0, 2032)], send_sem, recv_sem, own_sem
    )


def unpack_last(read):
    lane16 = lax.rem(lanes(), 16)
    last = jnp.zeros((16, 128), F32)
    for c in range(3):
        piece = pltpu.roll(read(c).astype(F32), 128 - (12 - 4 * c), 1)
        last = jnp.where((lane16 >= 4 * c) & (lane16 < 4 * c + 4), piece, last)
    return last


def flip_matrix(size):
    row = lax.broadcasted_iota(jnp.int32, (size, size), 0)
    col = lax.broadcasted_iota(jnp.int32, (size, size), 1)
    return jnp.where(row + col == size - 1, 1.0, 0.0).astype(BF16)


def fill_picks(pick, place):
    def rows_of(slot, carry):
        row = lax.broadcasted_iota(jnp.int32, (64, 512), 0)
        col = lax.broadcasted_iota(jnp.int32, (64, 512), 1)
        lane = 16 * lax.rem(row, 32) + row // 32 + 2 * slot
        pick[aligned(64 * slot, 64)] = jnp.where(col == lane, 1.0, 0.0).astype(BF16)
        return carry

    lax.fori_loop(0, 6, rows_of, 0)

    def lanes_of(chunk, carry):
        row = lax.broadcasted_iota(jnp.int32, (64, 384), 0)
        col = lax.broadcasted_iota(jnp.int32, (64, 384), 1)
        block, inner = 4 * chunk + row // 16, lax.rem(row, 16)
        lane = (inner // 2) * 64 + lax.rem(inner, 2) * 32 + block
        place[aligned(64 * chunk, 64)] = jnp.where(
            (col == lane) & (inner < 12), 1.0, 0.0
        ).astype(BF16)
        return carry

    lax.fori_loop(0, 8, lanes_of, 0)


def middle_kernel(
    slots_ref, arrived_ref, tables_ref, weight_ref, rate_ref, rows_ref, modes_ref,
    spread_ref, spec_ref,
    wide, tables, even, odd, north, south, pick, place, line, rates, coeff, spec_box,
    waves, modes, inbox, spread,
    send_sem, own_sem, spec_send, spec_recv, spec_own, wide_sem, out_sem,
    recv_sem, table_sem,
):
    z, x, lat, fld = position()
    me = lat * 4 + fld
    load = pltpu.make_async_copy(arrived_ref, wide, wide_sem)
    load.start()
    table_loads = [
        pltpu.make_async_copy(tables_ref.at[s], tables.at[s], table_sem.at[s]) for s in range(6)
    ]
    for copy in table_loads:
        copy.start()
    greet()
    fill_picks(pick, place)
    line[...] = jnp.zeros((8, 128), F32)
    line[0:1, 0:32] = rate_ref[...]
    rates[...] = as_column(line[0:1])[0:32]
    spread_waves(rows_ref, waves)
    spread_modes(modes_ref, line, modes)
    load.wait()

    def unpack(n, carry):
        done = []
        for i in range(4):
            at = 80 * (4 * n + i)
            for k in range(4):
                cols = slice(128 * k, 128 * k + 128)
                last = unpack_last(lambda c: wide[aligned(at + 16 * c, 16), cols])
                done.append((at, cols, last.astype(BF16)))
        for at, cols, last in done:
            wide[aligned(at + 64, 16), cols] = last
        return carry

    lax.fori_loop(0, 8, unpack, 0)
    flip = flip_matrix(256)
    downs = [
        jnp.dot(flip, wide[2304 - 256 * b : 2560 - 256 * b], preferred_element_type=F32)
        for b in range(5)
    ]
    for b in range(5):
        up = wide[256 * b : 256 * b + 256].astype(F32)
        weight = jnp.concatenate(
            [as_column(weight_ref[2 * b + u : 2 * b + u + 1])[:, 0:1] for u in range(2)], 0
        )
        for target, value in ((even, up + downs[b]), (odd, up - downs[b])):
            target[:, 256 * b : 256 * b + 256] = lax.dot_general(
                pick[...], (value * weight).astype(BF16), NT, preferred_element_type=F32
            ).astype(BF16)

    for slot in range(6):
        used = 256 if slot % 2 else 384
        col = lax.broadcasted_iota(jnp.int32, (32, used), 1)
        table_loads[slot].wait()
        wave = slots_ref[me * 6 + slot]
        for parity, source in enumerate((even, odd)):
            cols = slice(384 * parity, 384 * parity + used)
            raw = jnp.dot(
                source[64 * slot : 64 * slot + 64], tables[slot, :, cols],
                preferred_element_type=F32,
            )
            degree = wave + 2 * col + parity
            ratio = (degree * (degree + 1)).astype(F32) / float(LMAX * (LMAX + 1))
            square = ratio * ratio
            factor = 1.0 / (1.0 + rates[:, 0:1] * (square * square))
            factor = jnp.where(degree <= LMAX, factor, 0.0)
            value = raw * jnp.concatenate([factor, factor], 0)
            for r in range(2):
                for k in range(4):
                    low = 32 * r + 8 * k
                    spec_box[slot, r, k, :, cols] = value[low : low + 8].astype(BF16)
            coeff[slot, :, cols] = value.astype(BF16)
            if used < 384:
                spec_box[slot, :, :, :, 384 * parity + used : 384 * parity + 384] = jnp.zeros(
                    (2, 4, 8, 384 - used), BF16
                )
        if slot == 0:
            greeted()
        for shift in range(4):
            to = lax.rem(fld + shift, 4)
            source, target = spec_box.at[slot, :, to], spec_ref.at[fld, slot]
            if shift:
                pltpu.make_async_remote_copy(
                    src_ref=source, dst_ref=target, send_sem=spec_send, recv_sem=spec_recv,
                    device_id=(lat, to), device_id_type=MESH,
                ).start()
            else:
                pltpu.make_async_copy(source, target, spec_own).start()

    mine = 2 * lax.rem(z, 2) + x // 2
    turn = flip_matrix(320)
    lane16 = lax.rem(lanes(), 16)

    def part_of(step, carry):
        b = lax.rem(step + mine, 4)
        for slot in range(6):
            used = 256 if slot % 2 else 384
            sums = [
                lax.dot_general(
                    tables[slot, aligned(320 * b, 320, 64), 384 * p : 384 * p + used],
                    coeff[slot, :, 384 * p : 384 * p + used],
                    NT,
                    preferred_element_type=F32,
                )
                for p in range(2)
            ]
            north[:, 64 * slot : 64 * slot + 64] = (sums[0] + sums[1]).astype(BF16)
            south[:, 64 * slot : 64 * slot + 64] = (sums[0] - sums[1]).astype(BF16)
        wide[aligned(320 * b, 320, 64)] = lax.dot_general(
            north[...], place[...], NT, preferred_element_type=F32
        ).astype(BF16)
        mirrored = jnp.dot(turn, south[...], preferred_element_type=F32).astype(BF16)
        wide[aligned(1280 + 320 * (3 - b), 320, 64)] = lax.dot_general(
            mirrored, place[...], NT, preferred_element_type=F32
        ).astype(BF16)

        def pack(n, carry):
            done = []
            for i in (4 * b + n, 31 - 4 * b - n):
                at = 80 * i
                for k in range(4):
                    cols = slice(128 * k, 128 * k + 128)
                    last = wide[aligned(at + 64, 16), cols].astype(F32)
                    for q in range(3):
                        rows = aligned(at + 16 * q, 16)
                        moved = pltpu.roll(last, 12 - 4 * q, 1)
                        part = jnp.where(lane16 >= 12, moved, wide[rows, cols].astype(F32))
                        done.append((rows, cols, part.astype(BF16)))
            for rows, cols, part in done:
                wide[rows, cols] = part
            return carry

        lax.fori_loop(0, 4, pack, 0)

        def send(n, carry):
            for i in (4 * b + n, 31 - 4 * b - n):
                for k in range(4):
                    send_one(
                        i * 4 + k, wide.at[aligned(80 * i, 64), 128 * k : 128 * k + 128],
                        inbox.at[me], send_sem, recv_sem.at[mine], own_sem,
                    )
            return carry

        lax.fori_loop(0, 4, send, 0)
        return carry

    lax.fori_loop(0, 4, part_of, 0)
    here = jnp.where(lat < 16, lat // 4, (31 - lat) // 4)

    def arrived(count, kind):
        refs = inbox.at[pl.ds(0, count)]
        pltpu.make_async_remote_copy(
            src_ref=refs, dst_ref=refs, send_sem=send_sem, recv_sem=recv_sem.at[kind],
            device_id=(lat, fld), device_id_type=MESH,
        ).wait_recv()

    for stage in range(4):
        kind = lax.rem(here + 4 - stage, 4)

        @pl.when(kind == mine)
        def _():
            pltpu.make_async_copy(inbox.at[0], inbox.at[0], own_sem).wait()
            arrived(31, kind)

        @pl.when(kind != mine)
        def _():
            arrived(32, kind)

        first = (kind // 2) * 4 + 2 * lax.rem(kind, 2)

        def gather(n, carry):
            group = first + 8 * (n // 2) + lax.rem(n, 2)
            wave = waves[pl.ds(group, 1)]
            cols = aligned(128 * group, 128, 128)
            for q in range(5):
                keep = wave < modes[16 * q : 16 * q + 16]
                if q < 4:
                    parts = [inbox[group * 8 + d, 16 * q : 16 * q + 16].astype(F32) for d in range(8)]
                else:
                    parts = [
                        unpack_last(lambda c: inbox[group * 8 + d, 16 * c : 16 * c + 16])
                        for d in range(8)
                    ]
                for f, part in enumerate(swap_blocks(parts)):
                    spread[80 * f + 16 * q : 80 * f + 16 * q + 16, cols] = jnp.where(
                        keep, 2.0 * part, 0.0
                    ).astype(BF16)
            return carry

        lax.fori_loop(0, 4, gather, 0)
        for half in range(2):
            cols = aligned(128 * first + 1024 * half, 256, 256)
            pltpu.make_async_copy(spread.at[:, cols], spread_ref.at[:, cols], out_sem).start()

    pltpu.make_async_copy(spread, spread_ref, out_sem).wait()
    pltpu.make_async_copy(spec_ref.at[0], spec_ref.at[0], spec_own).wait()
    pltpu.make_async_remote_copy(
        src_ref=spec_ref.at[pl.ds(0, 3)], dst_ref=spec_ref.at[pl.ds(0, 3)],
        send_sem=spec_send, recv_sem=spec_recv, device_id=(lat, fld), device_id_type=MESH,
    ).wait()
    others = inbox.at[pl.ds(0, 127)]
    pltpu.make_async_remote_copy(
        src_ref=others, dst_ref=others, send_sem=send_sem, recv_sem=recv_sem.at[0],
        device_id=(lat, fld), device_id_type=MESH,
    ).wait_send()


VMEM = pl.BlockSpec(memory_space=pltpu.VMEM)
SMEM = pl.BlockSpec(memory_space=pltpu.SMEM)
ANY = pl.BlockSpec(memory_space=pl.ANY)
LIMIT = 60 * 1024 * 1024


def body(grid_in, legendre, wave_slot, lat_modes, gauss_weight, diffusion):
    grid_rows = grid_in.reshape(640, LON)
    modes = lat_modes.reshape(1, 80)
    slots = wave_slot.reshape(6, 128)

    arrived, angles = pl.pallas_call(
        forward_kernel,
        name="forward",
        out_shape=(
            jax.ShapeDtypeStruct((2560, 512), BF16),
            jax.ShapeDtypeStruct((LON, 2048), BF16),
        ),
        in_specs=[VMEM] * 3,
        out_specs=(ANY, ANY),
        scratch_shapes=[
            pltpu.VMEM((GROUPS, 128), jnp.int32),
            pltpu.VMEM((8, 128), F32),
            pltpu.VMEM((80, 128), jnp.int32),
            pltpu.VMEM((2, GROUPS, TRIG_ROWS, 128), F32),
            pltpu.VMEM((2, 192, 128), F32),
            pltpu.VMEM((LON, 256), BF16),
            pltpu.VMEM((640, 256), F32),
            pltpu.VMEM((128, 64, 128), BF16),
            pltpu.SemaphoreType.DMA,
            pltpu.SemaphoreType.DMA,
            pltpu.SemaphoreType.DMA,
            pltpu.SemaphoreType.DMA((2,)),
        ],
        compiler_params=pltpu.CompilerParams(
            collective_id=0, has_side_effects=True, vmem_limit_bytes=LIMIT
        ),
    )(grid_rows, slots, modes)

    spread, spectra = pl.pallas_call(
        middle_kernel,
        name="middle",
        out_shape=(
            jax.ShapeDtypeStruct((640, 2048), BF16),
            jax.ShapeDtypeStruct((4, 6, 2, 8, 768), BF16),
        ),
        in_specs=[SMEM, ANY, ANY, VMEM, VMEM, VMEM, VMEM],
        out_specs=(ANY, ANY),
        scratch_shapes=[
            pltpu.VMEM((2560, 512), BF16),
            pltpu.VMEM((6, 1280, 768), BF16),
            pltpu.VMEM((384, 1280), BF16),
            pltpu.VMEM((384, 1280), BF16),
            pltpu.VMEM((320, 384), BF16),
            pltpu.VMEM((320, 384), BF16),
            pltpu.VMEM((384, 512), BF16),
            pltpu.VMEM((512, 384), BF16),
            pltpu.VMEM((8, 128), F32),
            pltpu.VMEM((32, 128), F32),
            pltpu.VMEM((6, 64, 768), BF16),
            pltpu.VMEM((6, 2, 4, 8, 768), BF16),
            pltpu.VMEM((GROUPS, 128), jnp.int32),
            pltpu.VMEM((80, 128), jnp.int32),
            pltpu.VMEM((128, 64, 128), BF16),
            pltpu.VMEM((640, 2048), BF16),
        ]
        + [pltpu.SemaphoreType.DMA] * 7
        + [pltpu.SemaphoreType.DMA((4,)), pltpu.SemaphoreType.DMA((6,))],
        compiler_params=pltpu.CompilerParams(
            collective_id=1, has_side_effects=True, vmem_limit_bytes=LIMIT
        ),
    )(
        wave_slot, arrived, legendre, gauss_weight.reshape(10, 128), diffusion.reshape(1, 32),
        slots, modes,
    )

    grid_out = lax.dot_general(spread, angles, NT, preferred_element_type=F32)

    spectra = spectra.transpose(2, 0, 1, 3, 4).reshape(2, 24, 8, 768).astype(F32)
    return (grid_out.reshape(8, 80, LON), spectra)


def solution(mesh):
    return jax.shard_map(
        body,
        mesh=mesh,
        in_specs=(P("fld", "lat", None), P(("lat", "fld"), None, None), P(), P("lat"), P(), P()),
        out_specs=(P("fld", "lat", None), P(None, "lat", "fld", None)),
        check_vma=False,
    )
```

```python
import functools
import math

import jax
import jax.numpy as jnp
from jax import lax
from jax.experimental import pallas as pl
from jax.experimental.pallas import tpu as pltpu
from jax.sharding import PartitionSpec as P

LMAX = 1279
MESH = pl.DeviceIdType.MESH
F32 = jnp.float32
BF16 = jnp.bfloat16

LON = 2688
ROW_A, ROW_B, ROW_C = 14, 12, 16
GROUPS = 16
TRIG_ROWS = 48
NT = (((1,), (1,)), ((), ()))

ORDER = (
    (1, 1), (3, 3), (1, 2), (3, 0), (2, 1), (0, 3), (1, 3), (3, 1),
    (3, 2), (1, 0), (2, 3), (0, 1), (2, 0), (0, 2), (2, 2), (0, 0),
)


def position():
    lat = lax.axis_index("lat")
    return lat // 8, lax.rem(lat // 2, 4), lat, lax.axis_index("fld")


def group_at(step):
    z, x, _, _ = position()
    dz, dx = jnp.int32(0), jnp.int32(0)
    for n, (a, b) in enumerate(ORDER):
        dz = jnp.where(step == n, a, dz)
        dx = jnp.where(step == n, b, dx)
    return lax.rem(z + dz, 4) * 4 + lax.rem(x + dx, 4)


def greet():
    barrier = pltpu.get_barrier_semaphore()
    _, _, lat, fld = position()
    me = lat * 4 + fld

    def signal(n, carry):
        peer = lax.rem(me + n, 128)
        pl.semaphore_signal(
            barrier, inc=1, device_id=(peer // 4, lax.rem(peer, 4)), device_id_type=MESH
        )
        return carry

    lax.fori_loop(1, 128, signal, 0)


def greeted():
    pl.semaphore_wait(pltpu.get_barrier_semaphore(), 127)


def send_one(to, source, target, send_sem, recv_sem, own_sem):
    _, _, lat, fld = position()
    me = lat * 4 + fld

    @pl.when(to != me)
    def _():
        pltpu.make_async_remote_copy(
            src_ref=source, dst_ref=target, send_sem=send_sem, recv_sem=recv_sem,
            device_id=(to // 4, lax.rem(to, 4)), device_id_type=MESH,
        ).start()

    @pl.when(to == me)
    def _():
        pltpu.make_async_copy(source, target, own_sem).start()


def wait_all(one, others, send_sem, recv_sem, own_sem):
    _, _, lat, fld = position()
    pltpu.make_async_copy(one, one, own_sem).wait()
    pltpu.make_async_remote_copy(
        src_ref=others, dst_ref=others, send_sem=send_sem, recv_sem=recv_sem,
        device_id=(lat, fld), device_id_type=MESH,
    ).wait()


def lanes(rows=16):
    return lax.broadcasted_iota(jnp.int32, (rows, 128), 1)


def aligned(start, size, unit=16):
    return pl.ds(pl.multiple_of(start, unit), size)


def swap_blocks(parts):
    block = lanes() // 16
    turned = [p if i == 0 else pltpu.roll(p, 16 * i, 1) for i, p in enumerate(parts)]
    row = [turned[(-i) % 8] for i in range(8)]
    for bit in (1, 2, 4):
        mask = (block & bit) != 0
        row = [jnp.where(mask, row[(i - bit) % 8], row[i]) for i in range(8)]
    return [p if d == 0 else pltpu.roll(p, 128 - 16 * d, 1) for d, p in enumerate(row)]


def spread_waves(slots_ref, waves):
    lane = lanes(GROUPS)
    group = lax.broadcasted_iota(jnp.int32, (GROUPS, 128), 0)
    flat = (8 * group + lane // 16) * 6 + jnp.minimum(lax.rem(lane, 16), 11) // 2
    at = lax.rem(flat, 128)
    total = jnp.zeros((GROUPS, 128), jnp.int32)
    for r in range(6):
        row = jnp.broadcast_to(slots_ref[r : r + 1], (GROUPS, 128))
        found = jnp.take_along_axis(row, at, axis=1, mode="promise_in_bounds")
        total = jnp.where(flat // 128 == r, found, total)
    waves[...] = total


def as_column(row):
    return jnp.broadcast_to(row, (128, 128)).T


def spread_modes(modes_ref, line, modes):
    line[...] = jnp.zeros((8, 128), F32)
    line[0:1, 0:80] = modes_ref[...].astype(F32)
    modes[...] = as_column(line[0:1])[0:80].astype(jnp.int32)


def fill_trig(waves, trig):
    column = lax.rem(lanes(TRIG_ROWS), 16)
    row = lax.broadcasted_iota(jnp.int32, (TRIG_ROWS, 128), 0)
    first = row < ROW_A
    factor = jnp.where(
        first, 192 * row, jnp.where(row < ROW_A + ROW_B, 16 * (row - ROW_A), row - ROW_A - ROW_B)
    )
    turn = jnp.where(first & (lax.rem(column, 2) == 1), LON // 4, 0)
    scale = jnp.where(first, jnp.where(column < 12, 1.0 / math.sqrt(LON), 0.0), 1.0)

    def one(group, carry):
        index = lax.rem(factor * waves[pl.ds(group, 1)] + turn, LON)
        radians = index.astype(F32) * (2.0 * math.pi / LON)
        trig[0, group] = jnp.cos(radians) * scale
        trig[1, group] = jnp.sin(radians) * scale
        return carry

    lax.fori_loop(0, GROUPS, one, 0)


def make_table(trig, group, half, uv, table):
    low = ROW_A + ROW_B
    cos_c = trig[0, group, low : low + ROW_C]
    sin_c = trig[1, group, low : low + ROW_C]
    for b in range(ROW_B):
        cb = trig[0, group, ROW_A + b : ROW_A + b + 1]
        sb = trig[1, group, ROW_A + b : ROW_A + b + 1]
        uv[0, 16 * b : 16 * b + 16] = cb * cos_c - sb * sin_c
        uv[1, 16 * b : 16 * b + 16] = sb * cos_c + cb * sin_c

    def rows(a, carry):
        ca, sa = trig[0, group, pl.ds(a, 1)], trig[1, group, pl.ds(a, 1)]
        table[aligned(192 * a, 192), 128 * half : 128 * half + 128] = (
            ca * uv[0] - sa * uv[1]
        ).astype(BF16)
        return carry

    lax.fori_loop(0, ROW_A, rows, 0)


def forward_part(
    grid_ref, slots_ref, modes_ref, landing_ref, angles_ref,
    waves, line, modes, trig, uv, table, result, outbox,
    send_sem, recv_sem, own_sem, table_sem,
):
    lane16 = lax.rem(lanes(), 16)
    spread_waves(slots_ref, waves)
    spread_modes(modes_ref, line, modes)
    fill_trig(waves, trig)

    def step_body(step, carry):
        groups = (group_at(2 * step), group_at(2 * step + 1))
        for half in range(2):
            make_table(trig, groups[half], half, uv, table)
        copies = [
            pltpu.make_async_copy(
                table.at[:, pl.ds(128 * half, 128)],
                angles_ref.at[:, aligned(groups[half] * 128, 128, 128)],
                table_sem.at[half],
            )
            for half in range(2)
        ]
        for copy in copies:
            copy.start()
        result[...] = jnp.dot(grid_ref[...], table[...], preferred_element_type=F32)
        for half in range(2):
            wave = waves[pl.ds(groups[half], 1)]

            def swapped(q):
                keep = wave < modes[16 * q : 16 * q + 16]
                return swap_blocks([
                    jnp.where(
                        keep,
                        result[80 * f + 16 * q : 80 * f + 16 * q + 16, 128 * half : 128 * half + 128],
                        0.0,
                    )
                    for f in range(8)
                ])

            last = swapped(4)
            for q in range(4):
                for d, part in enumerate(swapped(q)):
                    if q < 3:
                        part = jnp.where(lane16 >= 12, pltpu.roll(last[d], 12 - 4 * q, 1), part)
                    outbox[groups[half] * 8 + d, 16 * q : 16 * q + 16] = part.astype(BF16)
        for copy in copies:
            copy.wait()

        @pl.when(step == 0)
        def _():
            greeted()

        _, _, lat, fld = position()
        landing = landing_ref.at[aligned(80 * lat, 64), aligned(128 * fld, 128, 128)]
        for half in range(2):
            def send(n, carry):
                to = groups[half] * 8 + n
                send_one(to, outbox.at[to], landing, send_sem, recv_sem, own_sem)
                return carry

            lax.fori_loop(0, 8, send, 0)
        return carry

    lax.fori_loop(0, GROUPS // 2, step_body, 0)


def unpack_last(read):
    lane16 = lax.rem(lanes(), 16)
    last = jnp.zeros((16, 128), F32)
    for c in range(3):
        piece = pltpu.roll(read(c).astype(F32), 128 - (12 - 4 * c), 1)
        last = jnp.where((lane16 >= 4 * c) & (lane16 < 4 * c + 4), piece, last)
    return last


def flip_matrix(size):
    row = lax.broadcasted_iota(jnp.int32, (size, size), 0)
    col = lax.broadcasted_iota(jnp.int32, (size, size), 1)
    return jnp.where(row + col == size - 1, 1.0, 0.0).astype(BF16)


def fill_picks(pick, place):
    def rows_of(slot, carry):
        row = lax.broadcasted_iota(jnp.int32, (64, 512), 0)
        col = lax.broadcasted_iota(jnp.int32, (64, 512), 1)
        lane = 16 * lax.rem(row, 32) + row // 32 + 2 * slot
        pick[aligned(64 * slot, 64)] = jnp.where(col == lane, 1.0, 0.0).astype(BF16)
        return carry

    lax.fori_loop(0, 6, rows_of, 0)

    def lanes_of(chunk, carry):
        row = lax.broadcasted_iota(jnp.int32, (64, 384), 0)
        col = lax.broadcasted_iota(jnp.int32, (64, 384), 1)
        block, inner = 4 * chunk + row // 16, lax.rem(row, 16)
        lane = (inner // 2) * 64 + lax.rem(inner, 2) * 32 + block
        place[aligned(64 * chunk, 64)] = jnp.where(
            (col == lane) & (inner < 12), 1.0, 0.0
        ).astype(BF16)
        return carry

    lax.fori_loop(0, 8, lanes_of, 0)


def exchange_kernel(
    wave_ref, grid_ref, tables_ref, weight_ref, rate_ref, rows_ref, modes_ref,
    angles_ref, spread_ref, spec_ref,
    trig, uv, table, result, outbox,
    wide, tables, even, odd, north, south, pick, place, line, rates, coeff, spec_box,
    waves, modes, inbox, spread,
    first_send, first_recv, first_own, send_sem, own_sem, spec_send, spec_recv, spec_own, out_sem,
    angle_sem, recv_sem, table_sem,
):
    z, x, lat, fld = position()
    me = lat * 4 + fld
    greet()
    table_loads = [
        pltpu.make_async_copy(tables_ref.at[s], tables.at[s], table_sem.at[s]) for s in range(6)
    ]
    for copy in table_loads:
        copy.start()
    forward_part(
        grid_ref, rows_ref, modes_ref, wide, angles_ref,
        waves, line, modes, trig, uv, table, result, outbox,
        first_send, first_recv, first_own, angle_sem,
    )
    fill_picks(pick, place)
    line[...] = jnp.zeros((8, 128), F32)
    line[0:1, 0:32] = rate_ref[...]
    rates[...] = as_column(line[0:1])[0:32]
    for copy in table_loads:
        copy.wait()
    wait_all(outbox.at[0], wide.at[pl.ds(0, 2032)], first_send, first_recv, first_own)

    def unpack(n, carry):
        done = []
        for i in range(4):
            at = 80 * (4 * n + i)
            for k in range(4):
                cols = slice(128 * k, 128 * k + 128)
                last = unpack_last(lambda c: wide[aligned(at + 16 * c, 16), cols])
                done.append((at, cols, last.astype(BF16)))
        for at, cols, last in done:
            wide[aligned(at + 64, 16), cols] = last
        return carry

    lax.fori_loop(0, 8, unpack, 0)
    flip = flip_matrix(256)
    downs = [
        jnp.dot(flip, wide[2304 - 256 * b : 2560 - 256 * b], preferred_element_type=F32)
        for b in range(5)
    ]
    for b in range(5):
        up = wide[256 * b : 256 * b + 256].astype(F32)
        weight = jnp.concatenate(
            [as_column(weight_ref[2 * b + u : 2 * b + u + 1])[:, 0:1] for u in range(2)], 0
        )
        for target, value in ((even, up + downs[b]), (odd, up - downs[b])):
            target[:, 256 * b : 256 * b + 256] = lax.dot_general(
                pick[...], (value * weight).astype(BF16), NT, preferred_element_type=F32
            ).astype(BF16)

    for slot in range(6):
        used = 256 if slot % 2 else 384
        col = lax.broadcasted_iota(jnp.int32, (32, used), 1)
        wave = wave_ref[me * 6 + slot]
        for parity, source in enumerate((even, odd)):
            cols = slice(384 * parity, 384 * parity + used)
            raw = jnp.dot(
                source[64 * slot : 64 * slot + 64], tables[slot, :, cols],
                preferred_element_type=F32,
            )
            degree = wave + 2 * col + parity
            ratio = (degree * (degree + 1)).astype(F32) / float(LMAX * (LMAX + 1))
            square = ratio * ratio
            factor = 1.0 / (1.0 + rates[:, 0:1] * (square * square))
            factor = jnp.where(degree <= LMAX, factor, 0.0)
            value = raw * jnp.concatenate([factor, factor], 0)
            for r in range(2):
                for k in range(4):
                    low = 32 * r + 8 * k
                    spec_box[slot, r, k, :, cols] = value[low : low + 8].astype(BF16)
            coeff[slot, :, cols] = value.astype(BF16)
            if used < 384:
                spec_box[slot, :, :, :, 384 * parity + used : 384 * parity + 384] = jnp.zeros(
                    (2, 4, 8, 384 - used), BF16
                )
        for shift in range(4):
            to = lax.rem(fld + shift, 4)
            source, target = spec_box.at[slot, :, to], spec_ref.at[fld, slot]
            if shift:
                pltpu.make_async_remote_copy(
                    src_ref=source, dst_ref=target, send_sem=spec_send, recv_sem=spec_recv,
                    device_id=(lat, to), device_id_type=MESH,
                ).start()
            else:
                pltpu.make_async_copy(source, target, spec_own).start()

    mine = 2 * lax.rem(z, 2) + x // 2
    turn = flip_matrix(320)
    lane16 = lax.rem(lanes(), 16)

    def part_of(step, carry):
        b = lax.rem(step + mine, 4)
        for slot in range(6):
            used = 256 if slot % 2 else 384
            sums = [
                lax.dot_general(
                    tables[slot, aligned(320 * b, 320, 64), 384 * p : 384 * p + used],
                    coeff[slot, :, 384 * p : 384 * p + used],
                    NT,
                    preferred_element_type=F32,
                )
                for p in range(2)
            ]
            north[:, 64 * slot : 64 * slot + 64] = (sums[0] + sums[1]).astype(BF16)
            south[:, 64 * slot : 64 * slot + 64] = (sums[0] - sums[1]).astype(BF16)
        wide[aligned(320 * b, 320, 64)] = lax.dot_general(
            north[...], place[...], NT, preferred_element_type=F32
        ).astype(BF16)
        mirrored = jnp.dot(turn, south[...], preferred_element_type=F32).astype(BF16)
        wide[aligned(1280 + 320 * (3 - b), 320, 64)] = lax.dot_general(
            mirrored, place[...], NT, preferred_element_type=F32
        ).astype(BF16)

        def pack(n, carry):
            done = []
            for i in (4 * b + n, 31 - 4 * b - n):
                at = 80 * i
                for k in range(4):
                    cols = slice(128 * k, 128 * k + 128)
                    last = wide[aligned(at + 64, 16), cols].astype(F32)
                    for q in range(3):
                        rows = aligned(at + 16 * q, 16)
                        moved = pltpu.roll(last, 12 - 4 * q, 1)
                        part = jnp.where(lane16 >= 12, moved, wide[rows, cols].astype(F32))
                        done.append((rows, cols, part.astype(BF16)))
            for rows, cols, part in done:
                wide[rows, cols] = part
            return carry

        lax.fori_loop(0, 4, pack, 0)

        def send(n, carry):
            for i in (4 * b + n, 31 - 4 * b - n):
                for k in range(4):
                    send_one(
                        i * 4 + k, wide.at[aligned(80 * i, 64), 128 * k : 128 * k + 128],
                        inbox.at[me], send_sem, recv_sem.at[mine], own_sem,
                    )
            return carry

        lax.fori_loop(0, 4, send, 0)
        return carry

    lax.fori_loop(0, 4, part_of, 0)
    here = jnp.where(lat < 16, lat // 4, (31 - lat) // 4)

    def arrived(count, kind):
        refs = inbox.at[pl.ds(0, count)]
        pltpu.make_async_remote_copy(
            src_ref=refs, dst_ref=refs, send_sem=send_sem, recv_sem=recv_sem.at[kind],
            device_id=(lat, fld), device_id_type=MESH,
        ).wait_recv()

    for stage in range(4):
        kind = lax.rem(here + 4 - stage, 4)

        @pl.when(kind == mine)
        def _():
            pltpu.make_async_copy(inbox.at[0], inbox.at[0], own_sem).wait()
            arrived(31, kind)

        @pl.when(kind != mine)
        def _():
            arrived(32, kind)

        first = (kind // 2) * 4 + 2 * lax.rem(kind, 2)

        def gather(n, carry):
            group = first + 8 * (n // 2) + lax.rem(n, 2)
            wave = waves[pl.ds(group, 1)]
            cols = aligned(128 * group, 128, 128)
            for q in range(5):
                keep = wave < modes[16 * q : 16 * q + 16]
                if q < 4:
                    parts = [inbox[group * 8 + d, 16 * q : 16 * q + 16].astype(F32) for d in range(8)]
                else:
                    parts = [
                        unpack_last(lambda c: inbox[group * 8 + d, 16 * c : 16 * c + 16])
                        for d in range(8)
                    ]
                for f, part in enumerate(swap_blocks(parts)):
                    spread[80 * f + 16 * q : 80 * f + 16 * q + 16, cols] = jnp.where(
                        keep, 2.0 * part, 0.0
                    ).astype(BF16)
            return carry

        lax.fori_loop(0, 4, gather, 0)
        for half in range(2):
            cols = aligned(128 * first + 1024 * half, 256, 256)
            pltpu.make_async_copy(spread.at[:, cols], spread_ref.at[:, cols], out_sem).start()

    pltpu.make_async_copy(spread, spread_ref, out_sem).wait()
    pltpu.make_async_copy(spec_ref.at[0], spec_ref.at[0], spec_own).wait()
    pltpu.make_async_remote_copy(
        src_ref=spec_ref.at[pl.ds(0, 3)], dst_ref=spec_ref.at[pl.ds(0, 3)],
        send_sem=spec_send, recv_sem=spec_recv, device_id=(lat, fld), device_id_type=MESH,
    ).wait()
    others = inbox.at[pl.ds(0, 127)]
    pltpu.make_async_remote_copy(
        src_ref=others, dst_ref=others, send_sem=send_sem, recv_sem=recv_sem.at[0],
        device_id=(lat, fld), device_id_type=MESH,
    ).wait_send()


def backward_kernel(spread_ref, angles_ref, spec_ref, out_ref, spectra_ref):
    out_ref[...] = lax.dot_general(spread_ref[...], angles_ref[...], NT, preferred_element_type=F32)

    @pl.when(pl.program_id(0) == 0)
    def _():
        for k in range(4):
            for slot in range(6):
                for r in range(2):
                    spectra_ref[r, 6 * k + slot] = spec_ref[k, slot, r].astype(F32)


VMEM = pl.BlockSpec(memory_space=pltpu.VMEM)
SMEM = pl.BlockSpec(memory_space=pltpu.SMEM)
ANY = pl.BlockSpec(memory_space=pl.ANY)
LIMIT = 60 * 1024 * 1024


def body(grid_in, legendre, wave_slot, lat_modes, gauss_weight, diffusion):
    grid_rows = grid_in.reshape(640, LON)
    modes = lat_modes.reshape(1, 80)
    slots = wave_slot.reshape(6, 128)

    angles, spread, spectra = pl.pallas_call(
        exchange_kernel,
        name="exchange",
        out_shape=(
            jax.ShapeDtypeStruct((LON, 2048), BF16),
            jax.ShapeDtypeStruct((640, 2048), BF16),
            jax.ShapeDtypeStruct((4, 6, 2, 8, 768), BF16),
        ),
        in_specs=[SMEM, VMEM, ANY, VMEM, VMEM, VMEM, VMEM],
        out_specs=(ANY, ANY, ANY),
        scratch_shapes=[
            pltpu.VMEM((2, GROUPS, TRIG_ROWS, 128), F32),
            pltpu.VMEM((2, 192, 128), F32),
            pltpu.VMEM((LON, 256), BF16),
            pltpu.VMEM((640, 256), F32),
            pltpu.VMEM((128, 64, 128), BF16),
            pltpu.VMEM((2560, 512), BF16),
            pltpu.VMEM((6, 1280, 768), BF16),
            pltpu.VMEM((384, 1280), BF16),
            pltpu.VMEM((384, 1280), BF16),
            pltpu.VMEM((320, 384), BF16),
            pltpu.VMEM((320, 384), BF16),
            pltpu.VMEM((384, 512), BF16),
            pltpu.VMEM((512, 384), BF16),
            pltpu.VMEM((8, 128), F32),
            pltpu.VMEM((32, 128), F32),
            pltpu.VMEM((6, 64, 768), BF16),
            pltpu.VMEM((6, 2, 4, 8, 768), BF16),
            pltpu.VMEM((GROUPS, 128), jnp.int32),
            pltpu.VMEM((80, 128), jnp.int32),
            pltpu.VMEM((128, 64, 128), BF16),
            pltpu.VMEM((640, 2048), BF16),
        ]
        + [pltpu.SemaphoreType.DMA] * 9
        + [
            pltpu.SemaphoreType.DMA((2,)),
            pltpu.SemaphoreType.DMA((4,)),
            pltpu.SemaphoreType.DMA((6,)),
        ],
        compiler_params=pltpu.CompilerParams(
            collective_id=0, has_side_effects=True, vmem_limit_bytes=LIMIT
        ),
    )(
        wave_slot, grid_rows, legendre, gauss_weight.reshape(10, 128), diffusion.reshape(1, 32),
        slots, modes,
    )

    grid_out, spectra = pl.pallas_call(
        backward_kernel,
        name="backward",
        grid=(3,),
        out_shape=(
            jax.ShapeDtypeStruct((640, LON), F32),
            jax.ShapeDtypeStruct((2, 24, 8, 768), F32),
        ),
        in_specs=[
            pl.BlockSpec((640, 2048), lambda i: (0, 0)),
            pl.BlockSpec((896, 2048), lambda i: (i, 0)),
            pl.BlockSpec((4, 6, 2, 8, 768), lambda i: (0, 0, 0, 0, 0)),
        ],
        out_specs=(
            pl.BlockSpec((640, 896), lambda i: (0, i)),
            pl.BlockSpec((2, 24, 8, 768), lambda i: (0, 0, 0, 0)),
        ),
        compiler_params=pltpu.CompilerParams(vmem_limit_bytes=LIMIT),
    )(spread, angles, spectra)

    return (grid_out.reshape(8, 80, LON), spectra)


def solution(mesh):
    return jax.shard_map(
        body,
        mesh=mesh,
        in_specs=(P("fld", "lat", None), P(("lat", "fld"), None, None), P(), P("lat"), P(), P()),
        out_specs=(P("fld", "lat", None), P(None, "lat", "fld", None)),
        check_vma=False,
    )
```

```python
import functools
import math

import jax
import jax.numpy as jnp
from jax import lax
from jax.experimental import pallas as pl
from jax.experimental.pallas import tpu as pltpu
from jax.sharding import PartitionSpec as P

LMAX = 1279
MESH = pl.DeviceIdType.MESH
F32 = jnp.float32
BF16 = jnp.bfloat16

LON = 2688
ROW_A, ROW_B, ROW_C = 14, 12, 16
GROUPS = 16
TRIG_ROWS = 48
NT = (((1,), (1,)), ((), ()))

ORDER = (
    (1, 1), (3, 3), (1, 2), (3, 0), (2, 1), (0, 3), (1, 3), (3, 1),
    (3, 2), (1, 0), (2, 3), (0, 1), (2, 0), (0, 2), (2, 2), (0, 0),
)


def position():
    lat = lax.axis_index("lat")
    return lat // 8, lax.rem(lat // 2, 4), lat, lax.axis_index("fld")


def group_at(step):
    z, x, _, _ = position()
    dz, dx = jnp.int32(0), jnp.int32(0)
    for n, (a, b) in enumerate(ORDER):
        dz = jnp.where(step == n, a, dz)
        dx = jnp.where(step == n, b, dx)
    return lax.rem(z + dz, 4) * 4 + lax.rem(x + dx, 4)


def greet():
    barrier = pltpu.get_barrier_semaphore()
    _, _, lat, fld = position()
    me = lat * 4 + fld

    def signal(n, carry):
        peer = lax.rem(me + n, 128)
        pl.semaphore_signal(
            barrier, inc=1, device_id=(peer // 4, lax.rem(peer, 4)), device_id_type=MESH
        )
        return carry

    lax.fori_loop(1, 128, signal, 0)


def greeted():
    pl.semaphore_wait(pltpu.get_barrier_semaphore(), 127)


def send_one(to, source, target, send_sem, recv_sem, own_sem):
    _, _, lat, fld = position()
    me = lat * 4 + fld

    @pl.when(to != me)
    def _():
        pltpu.make_async_remote_copy(
            src_ref=source, dst_ref=target, send_sem=send_sem, recv_sem=recv_sem,
            device_id=(to // 4, lax.rem(to, 4)), device_id_type=MESH,
        ).start()

    @pl.when(to == me)
    def _():
        pltpu.make_async_copy(source, target, own_sem).start()


def wait_all(one, others, send_sem, recv_sem, own_sem):
    _, _, lat, fld = position()
    pltpu.make_async_copy(one, one, own_sem).wait()
    pltpu.make_async_remote_copy(
        src_ref=others, dst_ref=others, send_sem=send_sem, recv_sem=recv_sem,
        device_id=(lat, fld), device_id_type=MESH,
    ).wait()


def lanes(rows=16):
    return lax.broadcasted_iota(jnp.int32, (rows, 128), 1)


def aligned(start, size, unit=16):
    return pl.ds(pl.multiple_of(start, unit), size)


def swap_blocks(parts):
    block = lanes() // 16
    turned = [p if i == 0 else pltpu.roll(p, 16 * i, 1) for i, p in enumerate(parts)]
    row = [turned[(-i) % 8] for i in range(8)]
    for bit in (1, 2, 4):
        mask = (block & bit) != 0
        row = [jnp.where(mask, row[(i - bit) % 8], row[i]) for i in range(8)]
    return [p if d == 0 else pltpu.roll(p, 128 - 16 * d, 1) for d, p in enumerate(row)]


def spread_waves(slots_ref, waves):
    lane = lanes(GROUPS)
    group = lax.broadcasted_iota(jnp.int32, (GROUPS, 128), 0)
    flat = (8 * group + lane // 16) * 6 + jnp.minimum(lax.rem(lane, 16), 11) // 2
    at = lax.rem(flat, 128)
    total = jnp.zeros((GROUPS, 128), jnp.int32)
    for r in range(6):
        row = jnp.broadcast_to(slots_ref[r : r + 1], (GROUPS, 128))
        found = jnp.take_along_axis(row, at, axis=1, mode="promise_in_bounds")
        total = jnp.where(flat // 128 == r, found, total)
    waves[...] = total


def as_column(row):
    return jnp.broadcast_to(row, (128, 128)).T


def spread_modes(modes_ref, line, modes):
    line[...] = jnp.zeros((8, 128), F32)
    line[0:1, 0:80] = modes_ref[...].astype(F32)
    modes[...] = as_column(line[0:1])[0:80].astype(jnp.int32)


def fill_trig(waves, trig):
    column = lax.rem(lanes(TRIG_ROWS), 16)
    row = lax.broadcasted_iota(jnp.int32, (TRIG_ROWS, 128), 0)
    first = row < ROW_A
    factor = jnp.where(
        first, 192 * row, jnp.where(row < ROW_A + ROW_B, 16 * (row - ROW_A), row - ROW_A - ROW_B)
    )
    turn = jnp.where(first & (lax.rem(column, 2) == 1), LON // 4, 0)
    scale = jnp.where(first, jnp.where(column < 12, 1.0 / math.sqrt(LON), 0.0), 1.0)

    def one(group, carry):
        index = lax.rem(factor * waves[pl.ds(group, 1)] + turn, LON)
        radians = index.astype(F32) * (2.0 * math.pi / LON)
        trig[0, group] = jnp.cos(radians) * scale
        trig[1, group] = jnp.sin(radians) * scale
        return carry

    lax.fori_loop(0, GROUPS, one, 0)


def make_table(trig, group, half, uv, table):
    low = ROW_A + ROW_B
    cos_c = trig[0, group, low : low + ROW_C]
    sin_c = trig[1, group, low : low + ROW_C]
    for b in range(ROW_B):
        cb = trig[0, group, ROW_A + b : ROW_A + b + 1]
        sb = trig[1, group, ROW_A + b : ROW_A + b + 1]
        uv[0, 16 * b : 16 * b + 16] = cb * cos_c - sb * sin_c
        uv[1, 16 * b : 16 * b + 16] = sb * cos_c + cb * sin_c

    def rows(a, carry):
        ca, sa = trig[0, group, pl.ds(a, 1)], trig[1, group, pl.ds(a, 1)]
        table[aligned(192 * a, 192), 128 * half : 128 * half + 128] = (
            ca * uv[0] - sa * uv[1]
        ).astype(BF16)
        return carry

    lax.fori_loop(0, ROW_A, rows, 0)


def forward_part(
    grid_ref, slots_ref, modes_ref, landing_ref, angles_ref,
    waves, line, modes, trig, uv, table, result, outbox,
    send_sem, recv_sem, own_sem, table_sem,
):
    lane16 = lax.rem(lanes(), 16)
    spread_waves(slots_ref, waves)
    spread_modes(modes_ref, line, modes)
    fill_trig(waves, trig)

    def step_body(step, carry):
        groups = (group_at(2 * step), group_at(2 * step + 1))
        for half in range(2):
            make_table(trig, groups[half], half, uv, table)
        copies = [
            pltpu.make_async_copy(
                table.at[:, pl.ds(128 * half, 128)],
                angles_ref.at[:, aligned(groups[half] * 128, 128, 128)],
                table_sem.at[half],
            )
            for half in range(2)
        ]
        for copy in copies:
            copy.start()
        result[...] = jnp.dot(grid_ref[...], table[...], preferred_element_type=F32)
        for half in range(2):
            wave = waves[pl.ds(groups[half], 1)]

            def swapped(q):
                keep = wave < modes[16 * q : 16 * q + 16]
                return swap_blocks([
                    jnp.where(
                        keep,
                        result[80 * f + 16 * q : 80 * f + 16 * q + 16, 128 * half : 128 * half + 128],
                        0.0,
                    )
                    for f in range(8)
                ])

            last = swapped(4)
            for q in range(4):
                for d, part in enumerate(swapped(q)):
                    if q < 3:
                        part = jnp.where(lane16 >= 12, pltpu.roll(last[d], 12 - 4 * q, 1), part)
                    outbox[groups[half] * 8 + d, 16 * q : 16 * q + 16] = part.astype(BF16)
        for copy in copies:
            copy.wait()

        @pl.when(step == 0)
        def _():
            greeted()

        _, _, lat, fld = position()
        landing = landing_ref.at[aligned(80 * lat, 64), aligned(128 * fld, 128, 128)]
        for half in range(2):
            def send(n, carry):
                to = groups[half] * 8 + n
                send_one(to, outbox.at[to], landing, send_sem, recv_sem, own_sem)
                return carry

            lax.fori_loop(0, 8, send, 0)
        return carry

    lax.fori_loop(0, GROUPS // 2, step_body, 0)


def unpack_last(read):
    lane16 = lax.rem(lanes(), 16)
    last = jnp.zeros((16, 128), F32)
    for c in range(3):
        piece = pltpu.roll(read(c).astype(F32), 128 - (12 - 4 * c), 1)
        last = jnp.where((lane16 >= 4 * c) & (lane16 < 4 * c + 4), piece, last)
    return last


def flip_matrix(size):
    row = lax.broadcasted_iota(jnp.int32, (size, size), 0)
    col = lax.broadcasted_iota(jnp.int32, (size, size), 1)
    return jnp.where(row + col == size - 1, 1.0, 0.0).astype(BF16)


def fill_picks(pick, place):
    def rows_of(slot, carry):
        row = lax.broadcasted_iota(jnp.int32, (64, 512), 0)
        col = lax.broadcasted_iota(jnp.int32, (64, 512), 1)
        lane = 16 * lax.rem(row, 32) + row // 32 + 2 * slot
        pick[aligned(64 * slot, 64)] = jnp.where(col == lane, 1.0, 0.0).astype(BF16)
        return carry

    lax.fori_loop(0, 6, rows_of, 0)

    def lanes_of(chunk, carry):
        row = lax.broadcasted_iota(jnp.int32, (64, 384), 0)
        col = lax.broadcasted_iota(jnp.int32, (64, 384), 1)
        block, inner = 4 * chunk + row // 16, lax.rem(row, 16)
        lane = (inner // 2) * 64 + lax.rem(inner, 2) * 32 + block
        place[aligned(64 * chunk, 64)] = jnp.where(
            (col == lane) & (inner < 12), 1.0, 0.0
        ).astype(BF16)
        return carry

    lax.fori_loop(0, 8, lanes_of, 0)


def exchange_kernel(
    wave_ref, grid_ref, tables_ref, weight_ref, rate_ref, rows_ref, modes_ref,
    angles_ref, partial_ref, rest_ref, spec_ref,
    trig, uv, table, result, outbox,
    wide, tables, even, odd, north, south, pick, place, line, rates, coeff, spec_box,
    waves, modes, inbox, spread, early, total,
    first_send, first_recv, first_own, send_sem, own_sem, spec_send, spec_recv, spec_own, out_sem, rest_sem, early_sem,
    angle_sem, recv_sem, table_sem,
):
    z, x, lat, fld = position()
    me = lat * 4 + fld
    greet()
    table_loads = [
        pltpu.make_async_copy(tables_ref.at[s], tables.at[s], table_sem.at[s]) for s in range(6)
    ]
    for copy in table_loads:
        copy.start()
    forward_part(
        grid_ref, rows_ref, modes_ref, wide, angles_ref,
        waves, line, modes, trig, uv, table, result, outbox,
        first_send, first_recv, first_own, angle_sem,
    )
    fill_picks(pick, place)
    line[...] = jnp.zeros((8, 128), F32)
    line[0:1, 0:32] = rate_ref[...]
    rates[...] = as_column(line[0:1])[0:32]
    for copy in table_loads:
        copy.wait()
    wait_all(outbox.at[0], wide.at[pl.ds(0, 2032)], first_send, first_recv, first_own)
    mine = 2 * lax.rem(z, 2) + x // 2
    here = jnp.where(lat < 16, lat // 4, (31 - lat) // 4)
    kinds = [lax.rem(here + 4 - stage, 4) for stage in range(4)]
    firsts = [(kind // 2) * 4 + 2 * lax.rem(kind, 2) for kind in kinds]
    for stage in range(2):
        for half in range(2):
            low = 512 * stage + 256 * half
            pltpu.make_async_copy(
                angles_ref.at[:, aligned(128 * firsts[stage] + 1024 * half, 256, 256)],
                early.at[:, low : low + 256],
                early_sem,
            ).start()

    def unpack(n, carry):
        done = []
        for i in range(4):
            at = 80 * (4 * n + i)
            for k in range(4):
                cols = slice(128 * k, 128 * k + 128)
                last = unpack_last(lambda c: wide[aligned(at + 16 * c, 16), cols])
                done.append((at, cols, last.astype(BF16)))
        for at, cols, last in done:
            wide[aligned(at + 64, 16), cols] = last
        return carry

    lax.fori_loop(0, 8, unpack, 0)
    flip = flip_matrix(256)
    downs = [
        jnp.dot(flip, wide[2304 - 256 * b : 2560 - 256 * b], preferred_element_type=F32)
        for b in range(5)
    ]
    for b in range(5):
        up = wide[256 * b : 256 * b + 256].astype(F32)
        weight = jnp.concatenate(
            [as_column(weight_ref[2 * b + u : 2 * b + u + 1])[:, 0:1] for u in range(2)], 0
        )
        for target, value in ((even, up + downs[b]), (odd, up - downs[b])):
            target[:, 256 * b : 256 * b + 256] = lax.dot_general(
                pick[...], (value * weight).astype(BF16), NT, preferred_element_type=F32
            ).astype(BF16)

    for slot in range(6):
        used = 256 if slot % 2 else 384
        col = lax.broadcasted_iota(jnp.int32, (32, used), 1)
        wave = wave_ref[me * 6 + slot]
        for parity, source in enumerate((even, odd)):
            cols = slice(384 * parity, 384 * parity + used)
            raw = jnp.dot(
                source[64 * slot : 64 * slot + 64], tables[slot, :, cols],
                preferred_element_type=F32,
            )
            degree = wave + 2 * col + parity
            ratio = (degree * (degree + 1)).astype(F32) / float(LMAX * (LMAX + 1))
            square = ratio * ratio
            factor = 1.0 / (1.0 + rates[:, 0:1] * (square * square))
            factor = jnp.where(degree <= LMAX, factor, 0.0)
            value = raw * jnp.concatenate([factor, factor], 0)
            for r in range(2):
                for k in range(4):
                    low = 32 * r + 8 * k
                    spec_box[slot, r, k, :, cols] = value[low : low + 8].astype(BF16)
            coeff[slot, :, cols] = value.astype(BF16)
            if used < 384:
                spec_box[slot, :, :, :, 384 * parity + used : 384 * parity + 384] = jnp.zeros(
                    (2, 4, 8, 384 - used), BF16
                )
        for shift in range(4):
            to = lax.rem(fld + shift, 4)
            source, target = spec_box.at[slot, :, to], spec_ref.at[fld, slot]
            if shift:
                pltpu.make_async_remote_copy(
                    src_ref=source, dst_ref=target, send_sem=spec_send, recv_sem=spec_recv,
                    device_id=(lat, to), device_id_type=MESH,
                ).start()
            else:
                pltpu.make_async_copy(source, target, spec_own).start()

    turn = flip_matrix(320)
    lane16 = lax.rem(lanes(), 16)

    def part_of(step, carry):
        b = lax.rem(step + mine, 4)
        for slot in range(6):
            used = 256 if slot % 2 else 384
            sums = [
                lax.dot_general(
                    tables[slot, aligned(320 * b, 320, 64), 384 * p : 384 * p + used],
                    coeff[slot, :, 384 * p : 384 * p + used],
                    NT,
                    preferred_element_type=F32,
                )
                for p in range(2)
            ]
            north[:, 64 * slot : 64 * slot + 64] = (sums[0] + sums[1]).astype(BF16)
            south[:, 64 * slot : 64 * slot + 64] = (sums[0] - sums[1]).astype(BF16)
        wide[aligned(320 * b, 320, 64)] = lax.dot_general(
            north[...], place[...], NT, preferred_element_type=F32
        ).astype(BF16)
        mirrored = jnp.dot(turn, south[...], preferred_element_type=F32).astype(BF16)
        wide[aligned(1280 + 320 * (3 - b), 320, 64)] = lax.dot_general(
            mirrored, place[...], NT, preferred_element_type=F32
        ).astype(BF16)

        def pack(n, carry):
            done = []
            for i in (4 * b + n, 31 - 4 * b - n):
                at = 80 * i
                for k in range(4):
                    cols = slice(128 * k, 128 * k + 128)
                    last = wide[aligned(at + 64, 16), cols].astype(F32)
                    for q in range(3):
                        rows = aligned(at + 16 * q, 16)
                        moved = pltpu.roll(last, 12 - 4 * q, 1)
                        part = jnp.where(lane16 >= 12, moved, wide[rows, cols].astype(F32))
                        done.append((rows, cols, part.astype(BF16)))
            for rows, cols, part in done:
                wide[rows, cols] = part
            return carry

        lax.fori_loop(0, 4, pack, 0)

        def send(n, carry):
            for i in (4 * b + n, 31 - 4 * b - n):
                for k in range(4):
                    send_one(
                        i * 4 + k, wide.at[aligned(80 * i, 64), 128 * k : 128 * k + 128],
                        inbox.at[me], send_sem, recv_sem.at[mine], own_sem,
                    )
            return carry

        lax.fori_loop(0, 4, send, 0)
        return carry

    lax.fori_loop(0, 4, part_of, 0)

    def arrived(count, kind):
        refs = inbox.at[pl.ds(0, count)]
        pltpu.make_async_remote_copy(
            src_ref=refs, dst_ref=refs, send_sem=send_sem, recv_sem=recv_sem.at[kind],
            device_id=(lat, fld), device_id_type=MESH,
        ).wait_recv()

    for stage in range(4):
        kind, first = kinds[stage], firsts[stage]

        @pl.when(kind == mine)
        def _():
            pltpu.make_async_copy(inbox.at[0], inbox.at[0], own_sem).wait()
            arrived(31, kind)

        @pl.when(kind != mine)
        def _():
            arrived(32, kind)

        def gather(n, carry):
            group = first + 8 * (n // 2) + lax.rem(n, 2)
            wave = waves[pl.ds(group, 1)]
            cols = aligned(512 * stage + 128 * n, 128, 128)
            for q in range(5):
                keep = wave < modes[16 * q : 16 * q + 16]
                if q < 4:
                    parts = [inbox[group * 8 + d, 16 * q : 16 * q + 16].astype(F32) for d in range(8)]
                else:
                    parts = [
                        unpack_last(lambda c: inbox[group * 8 + d, 16 * c : 16 * c + 16])
                        for d in range(8)
                    ]
                for f, part in enumerate(swap_blocks(parts)):
                    spread[80 * f + 16 * q : 80 * f + 16 * q + 16, cols] = jnp.where(
                        keep, 2.0 * part, 0.0
                    ).astype(BF16)
            return carry

        lax.fori_loop(0, 4, gather, 0)
        if stage == 1:
            pltpu.make_async_copy(early, early, early_sem).wait()

            def begin(n, carry):
                rows = aligned(896 * n, 896, 128)
                total[:, rows] = lax.dot_general(
                    spread[:, 0:1024], early[rows], NT, preferred_element_type=F32
                )
                pltpu.make_async_copy(total.at[:, rows], partial_ref.at[:, rows], out_sem).start()
                return carry

            lax.fori_loop(0, 3, begin, 0)
        if stage >= 2:
            low = 512 * stage
            pltpu.make_async_copy(
                spread.at[:, low : low + 512], rest_ref.at[:, low - 1024 : low - 512], rest_sem
            ).start()

    pltpu.make_async_copy(total, partial_ref, out_sem).wait()
    pltpu.make_async_copy(rest_ref, rest_ref, rest_sem).wait()
    pltpu.make_async_copy(spec_ref.at[0], spec_ref.at[0], spec_own).wait()
    pltpu.make_async_remote_copy(
        src_ref=spec_ref.at[pl.ds(0, 3)], dst_ref=spec_ref.at[pl.ds(0, 3)],
        send_sem=spec_send, recv_sem=spec_recv, device_id=(lat, fld), device_id_type=MESH,
    ).wait()
    others = inbox.at[pl.ds(0, 127)]
    pltpu.make_async_remote_copy(
        src_ref=others, dst_ref=others, send_sem=send_sem, recv_sem=recv_sem.at[0],
        device_id=(lat, fld), device_id_type=MESH,
    ).wait_send()


def backward_kernel(
    firsts_ref, rest_ref, a_ref, b_ref, c_ref, d_ref, partial_ref, spec_ref,
    out_ref, spectra_ref, late,
):
    del firsts_ref
    for n, ref in enumerate((a_ref, b_ref, c_ref, d_ref)):
        late[:, 256 * n : 256 * n + 256] = ref[...]
    out_ref[...] = partial_ref[...] + lax.dot_general(
        rest_ref[...], late[...], NT, preferred_element_type=F32
    )

    @pl.when(pl.program_id(0) == 0)
    def _():
        for k in range(4):
            for slot in range(6):
                for r in range(2):
                    spectra_ref[r, 6 * k + slot] = spec_ref[k, slot, r].astype(F32)


VMEM = pl.BlockSpec(memory_space=pltpu.VMEM)
SMEM = pl.BlockSpec(memory_space=pltpu.SMEM)
ANY = pl.BlockSpec(memory_space=pl.ANY)
LIMIT = 60 * 1024 * 1024


def body(grid_in, legendre, wave_slot, lat_modes, gauss_weight, diffusion):
    grid_rows = grid_in.reshape(640, LON)
    modes = lat_modes.reshape(1, 80)
    slots = wave_slot.reshape(6, 128)

    angles, partial, rest, spectra = pl.pallas_call(
        exchange_kernel,
        name="exchange",
        out_shape=(
            jax.ShapeDtypeStruct((LON, 2048), BF16),
            jax.ShapeDtypeStruct((640, LON), F32),
            jax.ShapeDtypeStruct((640, 1024), BF16),
            jax.ShapeDtypeStruct((4, 6, 2, 8, 768), BF16),
        ),
        in_specs=[SMEM, VMEM, ANY, VMEM, VMEM, VMEM, VMEM],
        out_specs=(ANY, ANY, ANY, ANY),
        scratch_shapes=[
            pltpu.VMEM((2, GROUPS, TRIG_ROWS, 128), F32),
            pltpu.VMEM((2, 192, 128), F32),
            pltpu.VMEM((LON, 256), BF16),
            pltpu.VMEM((640, 256), F32),
            pltpu.VMEM((128, 64, 128), BF16),
            pltpu.VMEM((2560, 512), BF16),
            pltpu.VMEM((6, 1280, 768), BF16),
            pltpu.VMEM((384, 1280), BF16),
            pltpu.VMEM((384, 1280), BF16),
            pltpu.VMEM((320, 384), BF16),
            pltpu.VMEM((320, 384), BF16),
            pltpu.VMEM((384, 512), BF16),
            pltpu.VMEM((512, 384), BF16),
            pltpu.VMEM((8, 128), F32),
            pltpu.VMEM((32, 128), F32),
            pltpu.VMEM((6, 64, 768), BF16),
            pltpu.VMEM((6, 2, 4, 8, 768), BF16),
            pltpu.VMEM((GROUPS, 128), jnp.int32),
            pltpu.VMEM((80, 128), jnp.int32),
            pltpu.VMEM((128, 64, 128), BF16),
            pltpu.VMEM((640, 2048), BF16),
            pltpu.VMEM((LON, 1024), BF16),
            pltpu.VMEM((640, LON), F32),
        ]
        + [pltpu.SemaphoreType.DMA] * 11
        + [
            pltpu.SemaphoreType.DMA((2,)),
            pltpu.SemaphoreType.DMA((4,)),
            pltpu.SemaphoreType.DMA((6,)),
        ],
        compiler_params=pltpu.CompilerParams(
            collective_id=0, has_side_effects=True, vmem_limit_bytes=LIMIT
        ),
    )(
        wave_slot, grid_rows, legendre, gauss_weight.reshape(10, 128), diffusion.reshape(1, 32),
        slots, modes,
    )

    lat = lax.axis_index("lat")
    here = jnp.where(lat < 16, lat // 4, (31 - lat) // 4)
    late = (here + jnp.array([2, 1], jnp.int32)) % 4
    firsts = (late // 2) * 2 + late % 2

    def table_block(stage, half):
        return pl.BlockSpec((896, 256), lambda i, c: (i, c[stage] + 4 * half))

    grid_out, spectra = pl.pallas_call(
        backward_kernel,
        name="backward",
        grid_spec=pltpu.PrefetchScalarGridSpec(
            num_scalar_prefetch=1,
            grid=(3,),
            in_specs=[
                pl.BlockSpec((640, 1024), lambda i, c: (0, 0)),
                table_block(0, 0),
                table_block(0, 1),
                table_block(1, 0),
                table_block(1, 1),
                pl.BlockSpec((640, 896), lambda i, c: (0, i)),
                pl.BlockSpec((4, 6, 2, 8, 768), lambda i, c: (0, 0, 0, 0, 0)),
            ],
            out_specs=(
                pl.BlockSpec((640, 896), lambda i, c: (0, i)),
                pl.BlockSpec((2, 24, 8, 768), lambda i, c: (0, 0, 0, 0)),
            ),
            scratch_shapes=[pltpu.VMEM((896, 1024), BF16)],
        ),
        out_shape=(
            jax.ShapeDtypeStruct((640, LON), F32),
            jax.ShapeDtypeStruct((2, 24, 8, 768), F32),
        ),
        compiler_params=pltpu.CompilerParams(vmem_limit_bytes=LIMIT),
    )(firsts, rest, angles, angles, angles, angles, partial, spectra)

    return (grid_out.reshape(8, 80, LON), spectra)


def solution(mesh):
    return jax.shard_map(
        body,
        mesh=mesh,
        in_specs=(P("fld", "lat", None), P(("lat", "fld"), None, None), P(), P("lat"), P(), P()),
        out_specs=(P("fld", "lat", None), P(None, "lat", "fld", None)),
        check_vma=False,
    )
```

```python
import functools
import math

import jax
import jax.numpy as jnp
from jax import lax
from jax.experimental import pallas as pl
from jax.experimental.pallas import tpu as pltpu
from jax.sharding import PartitionSpec as P

LMAX = 1279
MESH = pl.DeviceIdType.MESH
F32 = jnp.float32
BF16 = jnp.bfloat16

LON = 2688
ROW_A, ROW_B, ROW_C = 14, 12, 16
GROUPS = 16
TRIG_ROWS = 48
NT = (((1,), (1,)), ((), ()))

ORDER = (
    (1, 1), (3, 3), (1, 2), (3, 0), (2, 1), (0, 3), (1, 3), (3, 1),
    (3, 2), (1, 0), (2, 3), (0, 1), (2, 0), (0, 2), (2, 2), (0, 0),
)


def position():
    lat = lax.axis_index("lat")
    return lat // 8, lax.rem(lat // 2, 4), lat, lax.axis_index("fld")


def group_at(step):
    z, x, _, _ = position()
    dz, dx = jnp.int32(0), jnp.int32(0)
    for n, (a, b) in enumerate(ORDER):
        dz = jnp.where(step == n, a, dz)
        dx = jnp.where(step == n, b, dx)
    return lax.rem(z + dz, 4) * 4 + lax.rem(x + dx, 4)


def greet():
    barrier = pltpu.get_barrier_semaphore()
    _, _, lat, fld = position()
    me = lat * 4 + fld

    def signal(n, carry):
        peer = lax.rem(me + n, 128)
        pl.semaphore_signal(
            barrier, inc=1, device_id=(peer // 4, lax.rem(peer, 4)), device_id_type=MESH
        )
        return carry

    lax.fori_loop(1, 128, signal, 0)


def greeted():
    pl.semaphore_wait(pltpu.get_barrier_semaphore(), 127)


def send_one(to, source, target, send_sem, recv_sem, own_sem):
    _, _, lat, fld = position()
    me = lat * 4 + fld

    @pl.when(to != me)
    def _():
        pltpu.make_async_remote_copy(
            src_ref=source, dst_ref=target, send_sem=send_sem, recv_sem=recv_sem,
            device_id=(to // 4, lax.rem(to, 4)), device_id_type=MESH,
        ).start()

    @pl.when(to == me)
    def _():
        pltpu.make_async_copy(source, target, own_sem).start()


def wait_all(one, others, send_sem, recv_sem, own_sem):
    _, _, lat, fld = position()
    pltpu.make_async_copy(one, one, own_sem).wait()
    pltpu.make_async_remote_copy(
        src_ref=others, dst_ref=others, send_sem=send_sem, recv_sem=recv_sem,
        device_id=(lat, fld), device_id_type=MESH,
    ).wait()


def lanes(rows=16):
    return lax.broadcasted_iota(jnp.int32, (rows, 128), 1)


def aligned(start, size, unit=16):
    return pl.ds(pl.multiple_of(start, unit), size)


def swap_blocks(parts):
    block = lanes() // 16
    turned = [p if i == 0 else pltpu.roll(p, 16 * i, 1) for i, p in enumerate(parts)]
    row = [turned[(-i) % 8] for i in range(8)]
    for bit in (1, 2, 4):
        mask = (block & bit) != 0
        row = [jnp.where(mask, row[(i - bit) % 8], row[i]) for i in range(8)]
    return [p if d == 0 else pltpu.roll(p, 128 - 16 * d, 1) for d, p in enumerate(row)]


def spread_waves(slots_ref, waves):
    lane = lanes(GROUPS)
    group = lax.broadcasted_iota(jnp.int32, (GROUPS, 128), 0)
    flat = (8 * group + lane // 16) * 6 + jnp.minimum(lax.rem(lane, 16), 11) // 2
    at = lax.rem(flat, 128)
    total = jnp.zeros((GROUPS, 128), jnp.int32)
    for r in range(6):
        row = jnp.broadcast_to(slots_ref[r : r + 1], (GROUPS, 128))
        found = jnp.take_along_axis(row, at, axis=1, mode="promise_in_bounds")
        total = jnp.where(flat // 128 == r, found, total)
    waves[...] = total


def as_column(row):
    return jnp.broadcast_to(row, (128, 128)).T


def spread_modes(modes_ref, line, modes):
    line[...] = jnp.zeros((8, 128), F32)
    line[0:1, 0:80] = modes_ref[...].astype(F32)
    modes[...] = as_column(line[0:1])[0:80].astype(jnp.int32)


def fill_trig(waves, trig, groups):
    column = lax.rem(lanes(TRIG_ROWS), 16)
    row = lax.broadcasted_iota(jnp.int32, (TRIG_ROWS, 128), 0)
    first = row < ROW_A
    factor = jnp.where(
        first, 192 * row, jnp.where(row < ROW_A + ROW_B, 16 * (row - ROW_A), row - ROW_A - ROW_B)
    )
    turn = jnp.where(first & (lax.rem(column, 2) == 1), LON // 4, 0)
    scale = jnp.where(first, jnp.where(column < 12, 1.0 / math.sqrt(LON), 0.0), 1.0)

    for group in groups:
        index = lax.rem(factor * waves[pl.ds(group, 1)] + turn, LON)
        radians = index.astype(F32) * (2.0 * math.pi / LON)
        trig[0, group] = jnp.cos(radians) * scale
        trig[1, group] = jnp.sin(radians) * scale


def make_table(trig, group, half, uv, table):
    low = ROW_A + ROW_B
    cos_c = trig[0, group, low : low + ROW_C]
    sin_c = trig[1, group, low : low + ROW_C]
    for b in range(ROW_B):
        cb = trig[0, group, ROW_A + b : ROW_A + b + 1]
        sb = trig[1, group, ROW_A + b : ROW_A + b + 1]
        uv[0, 16 * b : 16 * b + 16] = cb * cos_c - sb * sin_c
        uv[1, 16 * b : 16 * b + 16] = sb * cos_c + cb * sin_c

    def rows(a, carry):
        ca, sa = trig[0, group, pl.ds(a, 1)], trig[1, group, pl.ds(a, 1)]
        table[aligned(192 * a, 192), 128 * half : 128 * half + 128] = (
            ca * uv[0] - sa * uv[1]
        ).astype(BF16)
        return carry

    lax.fori_loop(0, ROW_A, rows, 0)


def forward_part(
    grid_ref, slots_ref, modes_ref, landing_ref, angles_ref,
    waves, line, modes, trig, uv, table, result, outbox,
    send_sem, recv_sem, own_sem, table_sem,
):
    lane16 = lax.rem(lanes(), 16)
    spread_waves(slots_ref, waves)
    spread_modes(modes_ref, line, modes)

    def step_body(step, carry):
        groups = (group_at(2 * step), group_at(2 * step + 1))
        fill_trig(waves, trig, groups)
        for half in range(2):
            make_table(trig, groups[half], half, uv, table)
        copies = [
            pltpu.make_async_copy(
                table.at[:, pl.ds(128 * half, 128)],
                angles_ref.at[:, aligned(groups[half] * 128, 128, 128)],
                table_sem.at[half],
            )
            for half in range(2)
        ]
        for copy in copies:
            copy.start()
        result[...] = jnp.dot(grid_ref[...], table[...], preferred_element_type=F32)
        for half in range(2):
            wave = waves[pl.ds(groups[half], 1)]

            def swapped(q):
                keep = wave < modes[16 * q : 16 * q + 16]
                return swap_blocks([
                    jnp.where(
                        keep,
                        result[80 * f + 16 * q : 80 * f + 16 * q + 16, 128 * half : 128 * half + 128],
                        0.0,
                    )
                    for f in range(8)
                ])

            last = swapped(4)
            for q in range(4):
                for d, part in enumerate(swapped(q)):
                    if q < 3:
                        part = jnp.where(lane16 >= 12, pltpu.roll(last[d], 12 - 4 * q, 1), part)
                    outbox[groups[half] * 8 + d, 16 * q : 16 * q + 16] = part.astype(BF16)
        for copy in copies:
            copy.wait()

        @pl.when(step == 0)
        def _():
            greeted()

        _, _, lat, fld = position()
        landing = landing_ref.at[aligned(80 * lat, 64), aligned(128 * fld, 128, 128)]
        for half in range(2):
            def send(n, carry):
                to = groups[half] * 8 + n
                send_one(to, outbox.at[to], landing, send_sem, recv_sem, own_sem)
                return carry

            lax.fori_loop(0, 8, send, 0)
        return carry

    lax.fori_loop(0, GROUPS // 2, step_body, 0)


def unpack_last(read):
    lane16 = lax.rem(lanes(), 16)
    last = jnp.zeros((16, 128), F32)
    for c in range(3):
        piece = pltpu.roll(read(c).astype(F32), 128 - (12 - 4 * c), 1)
        last = jnp.where((lane16 >= 4 * c) & (lane16 < 4 * c + 4), piece, last)
    return last


def flip_matrix(size):
    row = lax.broadcasted_iota(jnp.int32, (size, size), 0)
    col = lax.broadcasted_iota(jnp.int32, (size, size), 1)
    return jnp.where(row + col == size - 1, 1.0, 0.0).astype(BF16)


def fill_picks(pick, place):
    def rows_of(slot, carry):
        row = lax.broadcasted_iota(jnp.int32, (64, 512), 0)
        col = lax.broadcasted_iota(jnp.int32, (64, 512), 1)
        lane = 16 * lax.rem(row, 32) + row // 32 + 2 * slot
        pick[aligned(64 * slot, 64)] = jnp.where(col == lane, 1.0, 0.0).astype(BF16)
        return carry

    lax.fori_loop(0, 6, rows_of, 0)

    def lanes_of(chunk, carry):
        row = lax.broadcasted_iota(jnp.int32, (64, 384), 0)
        col = lax.broadcasted_iota(jnp.int32, (64, 384), 1)
        block, inner = 4 * chunk + row // 16, lax.rem(row, 16)
        lane = (inner // 2) * 64 + lax.rem(inner, 2) * 32 + block
        place[aligned(64 * chunk, 64)] = jnp.where(
            (col == lane) & (inner < 12), 1.0, 0.0
        ).astype(BF16)
        return carry

    lax.fori_loop(0, 8, lanes_of, 0)


def exchange_kernel(
    wave_ref, grid_ref, tables_ref, weight_ref, rate_ref, rows_ref, modes_ref,
    angles_ref, spread_ref, spec_ref,
    trig, uv, table, result, outbox,
    wide, tables, even, odd, north, south, pick, place, line, rates, coeff, spec_box,
    waves, modes, inbox, spread,
    first_send, first_recv, first_own, send_sem, own_sem, spec_send, spec_recv, spec_own, out_sem,
    angle_sem, recv_sem, table_sem,
):
    z, x, lat, fld = position()
    me = lat * 4 + fld
    greet()
    table_loads = [
        pltpu.make_async_copy(tables_ref.at[s], tables.at[s], table_sem.at[s]) for s in range(6)
    ]
    for copy in table_loads:
        copy.start()
    forward_part(
        grid_ref, rows_ref, modes_ref, wide, angles_ref,
        waves, line, modes, trig, uv, table, result, outbox,
        first_send, first_recv, first_own, angle_sem,
    )
    fill_picks(pick, place)
    line[...] = jnp.zeros((8, 128), F32)
    line[0:1, 0:32] = rate_ref[...]
    rates[...] = as_column(line[0:1])[0:32]
    for copy in table_loads:
        copy.wait()
    wait_all(outbox.at[0], wide.at[pl.ds(0, 2032)], first_send, first_recv, first_own)

    def unpack(n, carry):
        done = []
        for i in range(4):
            at = 80 * (4 * n + i)
            for k in range(4):
                cols = slice(128 * k, 128 * k + 128)
                last = unpack_last(lambda c: wide[aligned(at + 16 * c, 16), cols])
                done.append((at, cols, last.astype(BF16)))
        for at, cols, last in done:
            wide[aligned(at + 64, 16), cols] = last
        return carry

    lax.fori_loop(0, 8, unpack, 0)
    flip = flip_matrix(256)
    downs = [
        jnp.dot(flip, wide[2304 - 256 * b : 2560 - 256 * b], preferred_element_type=F32)
        for b in range(5)
    ]
    for b in range(5):
        up = wide[256 * b : 256 * b + 256].astype(F32)
        weight = jnp.concatenate(
            [as_column(weight_ref[2 * b + u : 2 * b + u + 1])[:, 0:1] for u in range(2)], 0
        )
        for target, value in ((even, up + downs[b]), (odd, up - downs[b])):
            target[:, 256 * b : 256 * b + 256] = lax.dot_general(
                pick[...], (value * weight).astype(BF16), NT, preferred_element_type=F32
            ).astype(BF16)

    for slot in range(6):
        used = 256 if slot % 2 else 384
        col = lax.broadcasted_iota(jnp.int32, (32, used), 1)
        wave = wave_ref[me * 6 + slot]
        for parity, source in enumerate((even, odd)):
            cols = slice(384 * parity, 384 * parity + used)
            raw = jnp.dot(
                source[64 * slot : 64 * slot + 64], tables[slot, :, cols],
                preferred_element_type=F32,
            )
            degree = wave + 2 * col + parity
            ratio = (degree * (degree + 1)).astype(F32) / float(LMAX * (LMAX + 1))
            square = ratio * ratio
            factor = 1.0 / (1.0 + rates[:, 0:1] * (square * square))
            factor = jnp.where(degree <= LMAX, factor, 0.0)
            value = raw * jnp.concatenate([factor, factor], 0)
            for r in range(2):
                for k in range(4):
                    low = 32 * r + 8 * k
                    spec_box[slot, r, k, :, cols] = value[low : low + 8].astype(BF16)
            coeff[slot, :, cols] = value.astype(BF16)
            if used < 384:
                spec_box[slot, :, :, :, 384 * parity + used : 384 * parity + 384] = jnp.zeros(
                    (2, 4, 8, 384 - used), BF16
                )
        for shift in range(4):
            to = lax.rem(fld + shift, 4)
            source, target = spec_box.at[slot, :, to], spec_ref.at[fld, slot]
            if shift:
                pltpu.make_async_remote_copy(
                    src_ref=source, dst_ref=target, send_sem=spec_send, recv_sem=spec_recv,
                    device_id=(lat, to), device_id_type=MESH,
                ).start()
            else:
                pltpu.make_async_copy(source, target, spec_own).start()

    mine, column = 2 * lax.rem(z, 2) + x // 2, z * 4 + x
    turn = flip_matrix(320)
    lane16 = lax.rem(lanes(), 16)

    def part_of(step, carry):
        b = lax.rem(step + mine, 4)
        for slot in range(6):
            used = 256 if slot % 2 else 384
            sums = [
                lax.dot_general(
                    tables[slot, aligned(320 * b, 320, 64), 384 * p : 384 * p + used],
                    coeff[slot, :, 384 * p : 384 * p + used],
                    NT,
                    preferred_element_type=F32,
                )
                for p in range(2)
            ]
            north[:, 64 * slot : 64 * slot + 64] = (sums[0] + sums[1]).astype(BF16)
            south[:, 64 * slot : 64 * slot + 64] = (sums[0] - sums[1]).astype(BF16)
        wide[aligned(320 * b, 320, 64)] = lax.dot_general(
            north[...], place[...], NT, preferred_element_type=F32
        ).astype(BF16)
        mirrored = jnp.dot(turn, south[...], preferred_element_type=F32).astype(BF16)
        wide[aligned(1280 + 320 * (3 - b), 320, 64)] = lax.dot_general(
            mirrored, place[...], NT, preferred_element_type=F32
        ).astype(BF16)

        def pack(n, carry):
            done = []
            for i in (4 * b + n, 31 - 4 * b - n):
                at = 80 * i
                for k in range(4):
                    cols = slice(128 * k, 128 * k + 128)
                    last = wide[aligned(at + 64, 16), cols].astype(F32)
                    for q in range(3):
                        rows = aligned(at + 16 * q, 16)
                        moved = pltpu.roll(last, 12 - 4 * q, 1)
                        part = jnp.where(lane16 >= 12, moved, wide[rows, cols].astype(F32))
                        done.append((rows, cols, part.astype(BF16)))
            for rows, cols, part in done:
                wide[rows, cols] = part
            return carry

        lax.fori_loop(0, 4, pack, 0)

        def send(n, carry):
            for i in (4 * b + n, 31 - 4 * b - n):
                for k in range(4):
                    send_one(
                        i * 4 + k, wide.at[aligned(80 * i, 64), 128 * k : 128 * k + 128],
                        inbox.at[me], send_sem, recv_sem.at[column], own_sem,
                    )
            return carry

        lax.fori_loop(0, 4, send, 0)
        return carry

    lax.fori_loop(0, 4, part_of, 0)
    here = jnp.where(lat < 16, lat // 4, (31 - lat) // 4)

    def arrived(count, kind):
        refs = inbox.at[pl.ds(0, count)]
        pltpu.make_async_remote_copy(
            src_ref=refs, dst_ref=refs, send_sem=send_sem, recv_sem=recv_sem.at[kind],
            device_id=(lat, fld), device_id_type=MESH,
        ).wait_recv()

    for stage in range(4):
        kind = lax.rem(here + 4 - stage, 4)

        first = (kind // 2) * 4 + 2 * lax.rem(kind, 2)

        def gather(n, carry):
            group = first + 8 * (n // 2) + lax.rem(n, 2)

            @pl.when(group == column)
            def _():
                pltpu.make_async_copy(inbox.at[0], inbox.at[0], own_sem).wait()
                arrived(7, group)

            @pl.when(group != column)
            def _():
                arrived(8, group)

            wave = waves[pl.ds(group, 1)]
            cols = aligned(128 * group, 128, 128)
            for q in range(5):
                keep = wave < modes[16 * q : 16 * q + 16]
                if q < 4:
                    parts = [inbox[group * 8 + d, 16 * q : 16 * q + 16].astype(F32) for d in range(8)]
                else:
                    parts = [
                        unpack_last(lambda c: inbox[group * 8 + d, 16 * c : 16 * c + 16])
                        for d in range(8)
                    ]
                for f, part in enumerate(swap_blocks(parts)):
                    spread[80 * f + 16 * q : 80 * f + 16 * q + 16, cols] = jnp.where(
                        keep, 2.0 * part, 0.0
                    ).astype(BF16)
            pltpu.make_async_copy(spread.at[:, cols], spread_ref.at[:, cols], out_sem).start()
            return carry

        lax.fori_loop(0, 4, gather, 0)

    pltpu.make_async_copy(spread, spread_ref, out_sem).wait()
    pltpu.make_async_copy(spec_ref.at[0], spec_ref.at[0], spec_own).wait()
    pltpu.make_async_remote_copy(
        src_ref=spec_ref.at[pl.ds(0, 3)], dst_ref=spec_ref.at[pl.ds(0, 3)],
        send_sem=spec_send, recv_sem=spec_recv, device_id=(lat, fld), device_id_type=MESH,
    ).wait()
    others = inbox.at[pl.ds(0, 127)]
    pltpu.make_async_remote_copy(
        src_ref=others, dst_ref=others, send_sem=send_sem, recv_sem=recv_sem.at[0],
        device_id=(lat, fld), device_id_type=MESH,
    ).wait_send()


def backward_kernel(spread_ref, angles_ref, spec_ref, out_ref, spectra_ref):
    out_ref[...] = lax.dot_general(spread_ref[...], angles_ref[...], NT, preferred_element_type=F32)

    @pl.when(pl.program_id(0) == 0)
    def _():
        for k in range(4):
            for slot in range(6):
                for r in range(2):
                    spectra_ref[r, 6 * k + slot] = spec_ref[k, slot, r].astype(F32)


VMEM = pl.BlockSpec(memory_space=pltpu.VMEM)
SMEM = pl.BlockSpec(memory_space=pltpu.SMEM)
ANY = pl.BlockSpec(memory_space=pl.ANY)
LIMIT = 60 * 1024 * 1024


def body(grid_in, legendre, wave_slot, lat_modes, gauss_weight, diffusion):
    grid_rows = grid_in.reshape(640, LON)
    modes = lat_modes.reshape(1, 80)
    slots = wave_slot.reshape(6, 128)

    angles, spread, spectra = pl.pallas_call(
        exchange_kernel,
        name="exchange",
        out_shape=(
            jax.ShapeDtypeStruct((LON, 2048), BF16),
            jax.ShapeDtypeStruct((640, 2048), BF16),
            jax.ShapeDtypeStruct((4, 6, 2, 8, 768), BF16),
        ),
        in_specs=[SMEM, VMEM, ANY, VMEM, VMEM, VMEM, VMEM],
        out_specs=(ANY, ANY, ANY),
        scratch_shapes=[
            pltpu.VMEM((2, GROUPS, TRIG_ROWS, 128), F32),
            pltpu.VMEM((2, 192, 128), F32),
            pltpu.VMEM((LON, 256), BF16),
            pltpu.VMEM((640, 256), F32),
            pltpu.VMEM((128, 64, 128), BF16),
            pltpu.VMEM((2560, 512), BF16),
            pltpu.VMEM((6, 1280, 768), BF16),
            pltpu.VMEM((384, 1280), BF16),
            pltpu.VMEM((384, 1280), BF16),
            pltpu.VMEM((320, 384), BF16),
            pltpu.VMEM((320, 384), BF16),
            pltpu.VMEM((384, 512), BF16),
            pltpu.VMEM((512, 384), BF16),
            pltpu.VMEM((8, 128), F32),
            pltpu.VMEM((32, 128), F32),
            pltpu.VMEM((6, 64, 768), BF16),
            pltpu.VMEM((6, 2, 4, 8, 768), BF16),
            pltpu.VMEM((GROUPS, 128), jnp.int32),
            pltpu.VMEM((80, 128), jnp.int32),
            pltpu.VMEM((128, 64, 128), BF16),
            pltpu.VMEM((640, 2048), BF16),
        ]
        + [pltpu.SemaphoreType.DMA] * 9
        + [
            pltpu.SemaphoreType.DMA((2,)),
            pltpu.SemaphoreType.DMA((GROUPS,)),
            pltpu.SemaphoreType.DMA((6,)),
        ],
        compiler_params=pltpu.CompilerParams(
            collective_id=0, has_side_effects=True, vmem_limit_bytes=LIMIT
        ),
    )(
        wave_slot, grid_rows, legendre, gauss_weight.reshape(10, 128), diffusion.reshape(1, 32),
        slots, modes,
    )

    grid_out, spectra = pl.pallas_call(
        backward_kernel,
        name="backward",
        grid=(3,),
        out_shape=(
            jax.ShapeDtypeStruct((640, LON), F32),
            jax.ShapeDtypeStruct((2, 24, 8, 768), F32),
        ),
        in_specs=[
            pl.BlockSpec((640, 2048), lambda i: (0, 0)),
            pl.BlockSpec((896, 2048), lambda i: (i, 0)),
            pl.BlockSpec((4, 6, 2, 8, 768), lambda i: (0, 0, 0, 0, 0)),
        ],
        out_specs=(
            pl.BlockSpec((640, 896), lambda i: (0, i)),
            pl.BlockSpec((2, 24, 8, 768), lambda i: (0, 0, 0, 0)),
        ),
        compiler_params=pltpu.CompilerParams(vmem_limit_bytes=LIMIT),
    )(spread, angles, spectra)

    return (grid_out.reshape(8, 80, LON), spectra)


def solution(mesh):
    return jax.shard_map(
        body,
        mesh=mesh,
        in_specs=(P("fld", "lat", None), P(("lat", "fld"), None, None), P(), P("lat"), P(), P()),
        out_specs=(P("fld", "lat", None), P(None, "lat", "fld", None)),
        check_vma=False,
    )
```
